8 devices in a mesh: tp: 2 (over z, y), dp: 4 (over x, core).
Axes of the slice: x: 2, y: 2, z: 1, core: 2. Of those that a mesh axis runs over, the one named last changes fastest.
Arguments:
- x_in: bfloat16 [128, 3072], P('dp')
- w_gate: bfloat16 [3072, 8192], P('dp', 'tp')
- w_up: bfloat16 [3072, 8192], P('dp', 'tp')
- w_down: bfloat16 [8192, 3072], P('tp', 'dp')
- dy_in: bfloat16 [128, 3072], P('dp')
Outputs:
- output 1: bfloat16 [128, 3072], P('dp')
- output 2: bfloat16 [128, 3072], P('dp')
- output 3: float32 [3072, 8192], P('dp', 'tp')
- output 4: float32 [3072, 8192], P('dp', 'tp')
- output 5: float32 [8192, 3072], P('tp', 'dp')
All inputs are finite; a program needn't handle non-finite values.
Results may differ from the reference program's by a relative error of at most 0.00101.
Values are sent between devices in bfloat16 or wider.
A program may use at most 1 GiB of HBM per device.

```python
import jax
import jax.numpy as jnp
from jax import lax

MODEL_DIM = 3072
HIDDEN_DIM = 8192
SHARD_TOKENS = 32
DATA_SHARDS = 4


def setup_inputs(seed: int = 0) -> dict:
    key_list = jax.random.split(jax.random.key(seed), 5)
    row_count = DATA_SHARDS * SHARD_TOKENS
    x_vals = jax.random.normal(key_list[0], (row_count, MODEL_DIM), jnp.float32)
    gate_vals = jax.random.normal(key_list[1], (MODEL_DIM, HIDDEN_DIM), jnp.float32) * MODEL_DIM ** -0.5
    up_vals = jax.random.normal(key_list[2], (MODEL_DIM, HIDDEN_DIM), jnp.float32) * MODEL_DIM ** -0.5
    down_vals = jax.random.normal(key_list[3], (HIDDEN_DIM, MODEL_DIM), jnp.float32) * HIDDEN_DIM ** -0.5
    dy_vals = jax.random.normal(key_list[4], (row_count, MODEL_DIM), jnp.float32)
    return {
        'x_in': x_vals.astype(jnp.bfloat16),
        'w_gate': gate_vals.astype(jnp.bfloat16),
        'w_up': up_vals.astype(jnp.bfloat16),
        'w_down': down_vals.astype(jnp.bfloat16),
        'dy_in': dy_vals.astype(jnp.bfloat16),
    }


def reference(x_in, w_gate, w_up, w_down, dy_in):
    row_count = DATA_SHARDS * SHARD_TOKENS
    x_blocks = x_in.reshape(DATA_SHARDS, SHARD_TOKENS, MODEL_DIM)
    dy_blocks = dy_in.reshape(DATA_SHARDS, SHARD_TOKENS, MODEL_DIM)

    def shard_pass(carry, block):
        acc_gate, acc_up, acc_down = carry
        x_blk, dy_blk = block
        gate_pre = jnp.dot(x_blk, w_gate, preferred_element_type=jnp.float32)
        up_pre = jnp.dot(x_blk, w_up, preferred_element_type=jnp.float32)
        sig_gate = jax.nn.sigmoid(gate_pre)
        silu_gate = gate_pre * sig_gate
        hidden = (silu_gate * up_pre).astype(jnp.bfloat16)
        y_blk = (x_blk.astype(jnp.float32) + jnp.dot(hidden, w_down, preferred_element_type=jnp.float32)).astype(jnp.bfloat16)
        grad_h = jnp.dot(dy_blk, w_down.T, preferred_element_type=jnp.float32)
        d_gate = (grad_h * up_pre * sig_gate * (1.0 + gate_pre * (1.0 - sig_gate))).astype(jnp.bfloat16)
        d_up = (grad_h * silu_gate).astype(jnp.bfloat16)
        dx_blk = (dy_blk.astype(jnp.float32)
                  + jnp.dot(d_gate, w_gate.T, preferred_element_type=jnp.float32)
                  + jnp.dot(d_up, w_up.T, preferred_element_type=jnp.float32)).astype(jnp.bfloat16)
        acc_gate = acc_gate + jnp.dot(x_blk.T, d_gate, preferred_element_type=jnp.float32)
        acc_up = acc_up + jnp.dot(x_blk.T, d_up, preferred_element_type=jnp.float32)
        acc_down = acc_down + jnp.dot(hidden.T, dy_blk, preferred_element_type=jnp.float32)
        return (acc_gate, acc_up, acc_down), (y_blk, dx_blk)

    zero_acc = (jnp.zeros((MODEL_DIM, HIDDEN_DIM), jnp.float32),
                jnp.zeros((MODEL_DIM, HIDDEN_DIM), jnp.float32),
                jnp.zeros((HIDDEN_DIM, MODEL_DIM), jnp.float32))
    sums, outs = lax.scan(shard_pass, zero_acc, (x_blocks, dy_blocks))
    y_blocks, dx_blocks = outs
    return (y_blocks.reshape(row_count, MODEL_DIM), dx_blocks.reshape(row_count, MODEL_DIM), sums[0], sums[1], sums[2])
```

```python
import functools

import jax
import jax.numpy as jnp
from jax import lax
from jax.experimental import pallas as pl
from jax.experimental.pallas import tpu as pltpu
from jax.sharding import PartitionSpec as P

MESH = pl.DeviceIdType.MESH
F32 = jnp.float32
BF16 = jnp.bfloat16
CHUNK = 512
SHARDS = 4
OWN, FAR, SIB, DIAG = 0, 1, 2, 3


def _dot(lhs, rhs, lhs_dim, rhs_dim):
    return lax.dot_general(lhs, rhs, (((lhs_dim,), (rhs_dim,)), ((), ())), preferred_element_type=F32)


def exchange_kernel(chunks, x_hbm, gate_hbm, up_hbm, down_hbm, dy_hbm,
                    xc_out, dyc_out, hid_out, grad_out, y_out, dx_out,
                    x_own, dy_own, xc, dyc, gate, up, down,
                    ab_keep, ab_give, ab_got, g_keep, g_give, g_got,
                    ab_send, ab_recv, g_send, g_recv, hid, grad,
                    y_acc, dx_acc, y_peer, dx_peer, y_sum, dx_sum, y_stage, dx_stage,
                    in_sem, w_sem, tok_ss, tok_rs, core_ss, core_rs, link_ss, link_rs,
                    hid_ss, hid_rs, grad_ss, grad_rs, tp_ss, tp_rs, row_ss, row_rs, out_sem):
    tp = lax.axis_index('tp')
    dp = lax.axis_index('dp')
    sib = dp + 1 - 2 * lax.rem(dp, 2)
    far = lax.rem(dp + 2, SHARDS)
    diag = lax.rem(sib + 2, SHARDS)
    peers = {FAR: far, SIB: sib, DIAG: diag}
    width = xc.shape[-1]

    def remote(src, dst, ss, rs, **device):
        return pltpu.make_async_remote_copy(src_ref=src, dst_ref=dst, send_sem=ss, recv_sem=rs,
                                            device_id=device, device_id_type=MESH)

    def cols(i):
        return pl.ds(pl.multiple_of(i * width, width), width)

    def span(c):
        return pl.ds(pl.multiple_of(c * CHUNK, CHUNK), CHUNK)

    def load_gate(c):
        return pltpu.make_async_copy(gate_hbm.at[:, span(c)], gate.at[c], w_sem.at[0, c])

    def load_up(c):
        return pltpu.make_async_copy(up_hbm.at[:, span(c)], up.at[c], w_sem.at[1, c])

    def load_down(c):
        return pltpu.make_async_copy(down_hbm.at[span(c)], down.at[c], w_sem.at[2, c])

    tokens = ((x_hbm, x_own, xc, 0), (dy_hbm, dy_own, dyc, 1))
    stage_in = [pltpu.make_async_copy(h, v, in_sem.at[i]) for h, v, _, i in tokens]
    keep_in = [pltpu.make_async_copy(h.at[:, :, cols(dp)], s.at[OWN], in_sem.at[2 + i]) for h, _, s, i in tokens]
    for copy in stage_in + keep_in:
        copy.start()
    for c in range(chunks):
        load_gate(c).start()
        load_up(c).start()
    for c in range(chunks):
        load_down(c).start()

    barrier = pltpu.get_barrier_semaphore()
    for p in (FAR, SIB, DIAG):
        pl.semaphore_signal(barrier, inc=1, device_id={'dp': peers[p]}, device_id_type=MESH)
        pl.semaphore_signal(barrier, inc=1, device_id={'dp': peers[p], 'tp': 1 - tp}, device_id_type=MESH)
    pl.semaphore_signal(barrier, inc=1, device_id={'tp': 1 - tp}, device_id_type=MESH)
    pl.semaphore_wait(barrier, 2 * SHARDS - 1)

    token_copies = []
    for _, own, slots, i in tokens:
        stage_in[i].wait()
        for p in (FAR, DIAG, SIB):
            copy = remote(own.at[:, :, cols(peers[p])], slots.at[p], tok_ss.at[i, p], tok_rs.at[i, p], dp=peers[p])
            copy.start()
            token_copies.append(copy)
        token_copies.append(None)

    def core_ab(c):
        return remote(ab_give.at[c], ab_got.at[c], core_ss.at[0, c], core_rs.at[0, c], dp=sib)

    def core_g(c):
        return remote(g_give.at[c], g_got.at[c], core_ss.at[1, c], core_rs.at[1, c], dp=sib)

    def link_ab(c):
        return remote(ab_send.at[c], ab_recv.at[c], link_ss.at[0, c], link_rs.at[0, c], dp=far)

    def link_g(c):
        return remote(g_send.at[c], g_recv.at[c], link_ss.at[1, c], link_rs.at[1, c], dp=far)

    rows = 2 * x_own.shape[1]
    all_rows = SHARDS * rows

    def put(part, keep, give, index):
        part = part.reshape(SHARDS, rows, CHUNK)
        keep[index] = part[:2]
        give[index] = part[2:]

    def send_ab(c):
        core_ab(c).wait_recv()
        ab_send[c] = ab_keep[c, :, 1] + ab_got[c, :, 1]
        link_ab(c).start()

    def send_g(c):
        core_g(c).wait_recv()
        g_send[c] = g_keep[c, 1] + g_got[c, 1]
        link_g(c).start()

    keep_in[0].wait()
    for copy in token_copies[:3]:
        copy.wait_recv()

    def part_ab(c, carry):
        tok = xc[...].reshape(all_rows, width)
        load_gate(c).wait()
        put(_dot(tok, gate[c], 1, 0), ab_keep, ab_give, (c, 0))
        load_up(c).wait()
        put(_dot(tok, up[c], 1, 0), ab_keep, ab_give, (c, 1))
        core_ab(c).start()

        @pl.when(c > 0)
        def _():
            send_ab(c - 1)
        return carry

    lax.fori_loop(0, chunks, part_ab, 0)
    send_ab(chunks - 1)

    keep_in[1].wait()
    for copy in token_copies[4:7]:
        copy.wait_recv()

    def part_g(c, carry):
        tok = dyc[...].reshape(all_rows, width)
        load_down(c).wait()
        put(_dot(tok, down[c], 1, 1), g_keep, g_give, (c,))
        core_g(c).start()

        @pl.when(c > 0)
        def _():
            send_g(c - 1)
        return carry

    lax.fori_loop(0, chunks, part_g, 0)
    send_g(chunks - 1)

    keep_out = [pltpu.make_async_copy(xc, xc_out, out_sem.at[0]), pltpu.make_async_copy(dyc, dyc_out, out_sem.at[1])]
    for copy in keep_out:
        copy.start()

    def hid_far(c):
        return remote(hid.at[c, OWN], hid.at[c, FAR], hid_ss.at[0, c], hid_rs.at[0, c], dp=far)

    def hid_sib(c):
        return remote(hid.at[c, OWN], hid.at[c, SIB], hid_ss.at[1, c], hid_rs.at[1, c], dp=sib)

    def hid_fwd(c):
        return remote(hid.at[c, FAR], hid.at[c, DIAG], hid_ss.at[2, c], hid_rs.at[2, c], dp=sib)

    def grad_far(c):
        return remote(grad.at[c, OWN], grad.at[c, FAR], grad_ss.at[0, c], grad_rs.at[0, c], dp=far)

    def grad_sib(c):
        return remote(grad.at[c, OWN], grad.at[c, SIB], grad_ss.at[1, c], grad_rs.at[1, c], dp=sib)

    def grad_fwd(c):
        return remote(grad.at[c, FAR], grad.at[c, DIAG], grad_ss.at[2, c], grad_rs.at[2, c], dp=sib)

    def hid_save(c):
        return pltpu.make_async_copy(hid.at[c], hid_out.at[c], out_sem.at[2 + c])

    def grad_save(c):
        return pltpu.make_async_copy(grad.at[c], grad_out.at[c], out_sem.at[2 + chunks + c])

    def form_hidden(c, carry):
        link_ab(c).wait_recv()
        total = ab_keep[c, :, 0] + ab_got[c, :, 0] + ab_recv[c]
        ab_keep[c, :, 0] = total
        a, b = total[0], total[1]
        hid[c, OWN] = (a * jax.nn.sigmoid(a) * b).astype(BF16)
        hid_far(c).start()
        hid_sib(c).start()
        return carry

    lax.fori_loop(0, chunks, form_hidden, 0)

    def form_grads(c, carry):
        link_g(c).wait_recv()
        g = g_keep[c, 0] + g_got[c, 0] + g_recv[c]
        a, b = ab_keep[c, 0, 0], ab_keep[c, 1, 0]
        s = jax.nn.sigmoid(a)
        grad[c, OWN, 0] = (g * b * s * (1.0 + a * (1.0 - s))).astype(BF16)
        grad[c, OWN, 1] = (g * (a * s)).astype(BF16)
        grad_far(c).start()
        grad_sib(c).start()
        return carry

    lax.fori_loop(0, chunks, form_grads, 0)

    y_acc[...] = jnp.zeros_like(y_acc)
    dx_acc[...] = jnp.zeros_like(dx_acc)

    def use_hidden(c):
        hid_sib(c).wait_recv()
        hid_fwd(c).wait_recv()
        hid_save(c).start()
        y_acc[...] += _dot(hid[c].reshape(all_rows, CHUNK), down[c], 1, 0).reshape(y_acc.shape)

    def take_hidden(c, carry):
        hid_far(c).wait_recv()
        hid_fwd(c).start()

        @pl.when(c > 0)
        def _():
            use_hidden(c - 1)
        return carry

    lax.fori_loop(0, chunks, take_hidden, 0)
    use_hidden(chunks - 1)

    def tp_copy(acc, peer, i):
        return remote(acc.at[:, 1 - tp], peer, tp_ss.at[i], tp_rs.at[i], tp=1 - tp)

    def row_copies(total, stage, i):
        out = []
        for p in (FAR, DIAG, SIB):
            out.append(remote(total.at[p], stage.at[p, 0], row_ss.at[i, p, 0], row_rs.at[i, p, 0], dp=peers[p]))
            out.append(remote(total.at[p], stage.at[p, 1], row_ss.at[i, p, 1], row_rs.at[i, p, 1],
                              dp=peers[p], tp=1 - tp))
        out.append(remote(total.at[OWN], stage.at[OWN, 1], row_ss.at[i, OWN, 1], row_rs.at[i, OWN, 1], tp=1 - tp))
        return out

    def finish(tok, acc, peer, total, stage, i):
        tp_copy(acc, peer, i).wait()
        rows_out = (tok[:, tp].astype(F32) + (acc[:, tp] + peer[...])).astype(BF16)
        total[...] = rows_out
        stage[OWN, 0] = rows_out[OWN]
        copies = row_copies(total, stage, i)
        for copy in copies:
            copy.start()
        return copies

    tp_copy(y_acc, y_peer, 0).start()

    def use_grad(c):
        grad_sib(c).wait_recv()
        grad_fwd(c).wait_recv()
        grad_save(c).start()
        part = (_dot(grad[c, :, 0].reshape(all_rows, CHUNK), gate[c], 1, 1)
                + _dot(grad[c, :, 1].reshape(all_rows, CHUNK), up[c], 1, 1))
        dx_acc[...] += part.reshape(dx_acc.shape)

    def take_grad(c, carry):
        grad_far(c).wait_recv()
        grad_fwd(c).start()

        @pl.when(c > 0)
        def _():
            use_grad(c - 1)
        return carry

    lax.fori_loop(0, chunks, take_grad, 0)
    use_grad(chunks - 1)
    tp_copy(dx_acc, dx_peer, 1).start()
    copies = finish(xc, y_acc, y_peer, y_sum, y_stage, 0)
    copies += finish(dyc, dx_acc, dx_peer, dx_sum, dx_stage, 1)
    for copy in copies:
        copy.wait()
    last = [pltpu.make_async_copy(y_stage, y_out, in_sem.at[0]), pltpu.make_async_copy(dx_stage, dx_out, in_sem.at[1])]
    for copy in last:
        copy.start()

    for copy in token_copies:
        if copy is not None:
            copy.wait_send()
    for copy in keep_out:
        copy.wait()

    def drain(c, carry):
        for copy in (core_ab(c), core_g(c), link_ab(c), link_g(c), hid_far(c), hid_sib(c), hid_fwd(c),
                     grad_far(c), grad_sib(c), grad_fwd(c)):
            copy.wait_send()
        hid_save(c).wait()
        grad_save(c).wait()
        return carry

    lax.fori_loop(0, chunks, drain, 0)
    for copy in last:
        copy.wait()


def gradient_kernel(xc, dyc, hid, grad, y_stage, dx_stage, y_out, dx_out, dgate, dup, ddown, x_t):
    tp = lax.axis_index('tp')
    dp = lax.axis_index('dp')
    sib = dp + 1 - 2 * lax.rem(dp, 2)
    owner = {OWN: dp, FAR: lax.rem(dp + 2, SHARDS), SIB: sib, DIAG: lax.rem(sib + 2, SHARDS)}
    width = xc.shape[-1]
    all_rows = xc.shape[0] * xc.shape[1] * xc.shape[2]

    @pl.when(pl.program_id(0) == 0)
    def _():
        x_t[...] = xc[...].reshape(all_rows, width).T
        for stage, out in ((y_stage, y_out), (dx_stage, dx_out)):
            for p in range(SHARDS):
                at = pl.ds(pl.multiple_of(owner[p] * width, width), width)
                out[tp, :, at] = stage[p, 0]
                out[1 - tp, :, at] = stage[p, 1]

    dgate[...] = _dot(x_t[...], grad[0, :, 0].reshape(all_rows, CHUNK), 1, 0)
    dup[...] = _dot(x_t[...], grad[0, :, 1].reshape(all_rows, CHUNK), 1, 0)
    ddown[...] = _dot(hid[0].reshape(all_rows, CHUNK), dyc[...].reshape(all_rows, width), 0, 0)


def solution(mesh):
    def device_pass(x_rows, gate_blk, up_blk, down_blk, dy_rows):
        rows, model = x_rows.shape
        width, hidden = gate_blk.shape
        chunks = hidden // CHUNK
        half = rows // 2
        hbm = pl.BlockSpec(memory_space=pl.ANY)
        tok = (SHARDS, 2, half, width)
        sds = jax.ShapeDtypeStruct
        dma = pltpu.SemaphoreType.DMA
        xc, dyc, hid, grad, y_stage, dx_stage = pl.pallas_call(
            functools.partial(exchange_kernel, chunks),
            name='exchange',
            out_shape=(sds(tok, BF16), sds(tok, BF16), sds((chunks, SHARDS, rows, CHUNK), BF16),
                       sds((chunks, SHARDS, 2, rows, CHUNK), BF16), sds(tok, BF16), sds(tok, BF16)),
            in_specs=[hbm] * 5,
            out_specs=[hbm] * 6,
            scratch_shapes=[
                pltpu.VMEM((2, half, model), BF16), pltpu.VMEM((2, half, model), BF16),
                pltpu.VMEM(tok, BF16), pltpu.VMEM(tok, BF16),
                pltpu.VMEM((chunks, width, CHUNK), BF16), pltpu.VMEM((chunks, width, CHUNK), BF16),
                pltpu.VMEM((chunks, CHUNK, width), BF16),
                pltpu.VMEM((chunks, 2, 2, rows, CHUNK), F32), pltpu.VMEM((chunks, 2, 2, rows, CHUNK), F32),
                pltpu.VMEM((chunks, 2, 2, rows, CHUNK), F32),
                pltpu.VMEM((chunks, 2, rows, CHUNK), F32), pltpu.VMEM((chunks, 2, rows, CHUNK), F32),
                pltpu.VMEM((chunks, 2, rows, CHUNK), F32),
                pltpu.VMEM((chunks, 2, rows, CHUNK), F32), pltpu.VMEM((chunks, 2, rows, CHUNK), F32),
                pltpu.VMEM((chunks, rows, CHUNK), F32), pltpu.VMEM((chunks, rows, CHUNK), F32),
                pltpu.VMEM((chunks, SHARDS, rows, CHUNK), BF16), pltpu.VMEM((chunks, SHARDS, 2, rows, CHUNK), BF16),
                pltpu.VMEM(tok, F32), pltpu.VMEM(tok, F32),
                pltpu.VMEM((SHARDS, half, width), F32), pltpu.VMEM((SHARDS, half, width), F32),
                pltpu.VMEM((SHARDS, half, width), BF16), pltpu.VMEM((SHARDS, half, width), BF16),
                pltpu.VMEM(tok, BF16), pltpu.VMEM(tok, BF16),
                dma((4,)), dma((3, chunks)), dma((2, SHARDS)), dma((2, SHARDS)),
                dma((2, chunks)), dma((2, chunks)), dma((2, chunks)), dma((2, chunks)),
                dma((3, chunks)), dma((3, chunks)), dma((3, chunks)), dma((3, chunks)),
                dma((2,)), dma((2,)), dma((2, SHARDS, 2)), dma((2, SHARDS, 2)), dma((2 + 2 * chunks,)),
            ],
            compiler_params=pltpu.CompilerParams(collective_id=0, has_side_effects=True,
                                                 vmem_limit_bytes=60 * 1024 * 1024),
        )(x_rows.reshape(2, half, model), gate_blk, up_blk, down_blk, dy_rows.reshape(2, half, model))

        whole = lambda shape: pl.BlockSpec(shape, lambda c: (0,) * len(shape))
        y_rows, dx_rows, dw_gate, dw_up, dw_down = pl.pallas_call(
            gradient_kernel,
            name='gradients',
            grid=(chunks,),
            out_shape=(sds((2, half, model), BF16), sds((2, half, model), BF16), sds((width, hidden), F32),
                       sds((width, hidden), F32), sds((hidden, width), F32)),
            in_specs=[whole(tok), whole(tok),
                      pl.BlockSpec((1, SHARDS, rows, CHUNK), lambda c: (c, 0, 0, 0)),
                      pl.BlockSpec((1, SHARDS, 2, rows, CHUNK), lambda c: (c, 0, 0, 0, 0)),
                      whole(tok), whole(tok)],
            out_specs=[whole((2, half, model)), whole((2, half, model)),
                       pl.BlockSpec((width, CHUNK), lambda c: (0, c)), pl.BlockSpec((width, CHUNK), lambda c: (0, c)),
                       pl.BlockSpec((CHUNK, width), lambda c: (c, 0))],
            scratch_shapes=[pltpu.VMEM((width, all_rows := SHARDS * rows), BF16)],
            compiler_params=pltpu.CompilerParams(vmem_limit_bytes=48 * 1024 * 1024),
        )(xc, dyc, hid, grad, y_stage, dx_stage)
        return y_rows.reshape(rows, model), dx_rows.reshape(rows, model), dw_gate, dw_up, dw_down

    row_spec = P('dp', None)
    weight_spec = P('dp', 'tp')
    down_spec = P('tp', 'dp')
    return jax.shard_map(device_pass, mesh=mesh,
                         in_specs=(row_spec, weight_spec, weight_spec, down_spec, row_spec),
                         out_specs=(row_spec, row_spec, weight_spec, weight_spec, down_spec),
                         check_vma=False)
```

```python
import functools

import jax
import jax.numpy as jnp
from jax import lax
from jax.experimental import pallas as pl
from jax.experimental.pallas import tpu as pltpu
from jax.sharding import PartitionSpec as P

MESH = pl.DeviceIdType.MESH
F32 = jnp.float32
BF16 = jnp.bfloat16
CHUNK = 512
SHARDS = 4
OWN, SIB, FAR, DIAG = 0, 1, 2, 3


def _dot(lhs, rhs, lhs_dim, rhs_dim):
    return lax.dot_general(lhs, rhs, (((lhs_dim,), (rhs_dim,)), ((), ())), preferred_element_type=F32)


def exchange_kernel(chunks, x_hbm, gate_hbm, up_hbm, down_hbm, dy_hbm,
                    xc_out, dyc_out, hid_out, grad_out, y_out, dx_out,
                    x_own, dy_own, xc, dyc, gate, up, down,
                    ab_keep, ab_give, ab_got, g_keep, g_give, g_got, ab_recv, g_recv, hid, grad,
                    y_acc, dx_acc, y_peer, dx_peer, y_sum, dx_sum, y_stage, dx_stage,
                    in_sem, w_sem, tok_ss, tok_rs, core_ss, core_rs, link_ss, link_rs,
                    hid_ss, hid_rs, grad_ss, grad_rs, tp_ss, tp_rs, row_ss, row_rs, out_sem):
    tp = lax.axis_index('tp')
    dp = lax.axis_index('dp')
    sib = dp + 1 - 2 * lax.rem(dp, 2)
    far = lax.rem(dp + 2, SHARDS)
    diag = lax.rem(sib + 2, SHARDS)
    peers = {SIB: sib, FAR: far, DIAG: diag}
    width = xc.shape[-1]
    rows = x_own.shape[0] * x_own.shape[1]

    def remote(src, dst, ss, rs, **device):
        return pltpu.make_async_remote_copy(src_ref=src, dst_ref=dst, send_sem=ss, recv_sem=rs,
                                            device_id=device, device_id_type=MESH)

    def cols(i):
        return pl.ds(pl.multiple_of(i * width, width), width)

    def span(c):
        return pl.ds(pl.multiple_of(c * CHUNK, CHUNK), CHUNK)

    def load_gate(c):
        return pltpu.make_async_copy(gate_hbm.at[:, span(c)], gate.at[c], w_sem.at[0, c])

    def load_up(c):
        return pltpu.make_async_copy(up_hbm.at[:, span(c)], up.at[c], w_sem.at[1, c])

    def load_down(c):
        return pltpu.make_async_copy(down_hbm.at[span(c)], down.at[c], w_sem.at[2, c])

    tokens = ((x_hbm, x_own, xc, 0), (dy_hbm, dy_own, dyc, 1))
    stage_in = [pltpu.make_async_copy(h, v, in_sem.at[i]) for h, v, _, i in tokens]
    keep_in = [pltpu.make_async_copy(h.at[:, :, cols(dp)], s.at[OWN], in_sem.at[2 + i]) for h, _, s, i in tokens]
    for copy in stage_in + keep_in:
        copy.start()

    barrier = pltpu.get_barrier_semaphore()
    for p in (FAR, SIB, DIAG):
        pl.semaphore_signal(barrier, inc=1, device_id={'dp': peers[p]}, device_id_type=MESH)
        pl.semaphore_signal(barrier, inc=1, device_id={'dp': peers[p], 'tp': 1 - tp}, device_id_type=MESH)
    pl.semaphore_signal(barrier, inc=1, device_id={'tp': 1 - tp}, device_id_type=MESH)
    for copy in stage_in + keep_in:
        copy.wait()
    for c in range(chunks):
        load_gate(c).start()
        load_up(c).start()
    for c in range(chunks):
        load_down(c).start()
    pl.semaphore_wait(barrier, 2 * SHARDS - 1)

    def token(p, i):
        _, own, slots, _ = tokens[i]
        return remote(own.at[:, :, cols(peers[p])], slots.at[p], tok_ss.at[i, p], tok_rs.at[i, p], dp=peers[p])

    for i in (0, 1):
        for p in (SIB, FAR, DIAG):
            token(p, i).start()

    def core_ab(q, c):
        return remote(ab_give.at[q, c], ab_got.at[q, c], core_ss.at[q, 0, c], core_rs.at[q, 0, c], dp=sib)

    def core_g(q, c):
        return remote(g_give.at[q, c], g_got.at[q, c], core_ss.at[q, 1, c], core_rs.at[q, 1, c], dp=sib)

    def link_ab(c):
        return remote(ab_keep.at[0, c], ab_recv.at[c], link_ss.at[0, c], link_rs.at[0, c], dp=far)

    def link_g(c):
        return remote(g_keep.at[0, c], g_recv.at[c], link_ss.at[1, c], link_rs.at[1, c], dp=far)

    def send_ab(c):
        core_ab(0, c).wait_recv()
        ab_keep[0, c] += ab_got[0, c]
        link_ab(c).start()

    def send_g(c):
        core_g(0, c).wait_recv()
        g_keep[0, c] += g_got[0, c]
        link_g(c).start()

    def pair_rows(slots, q):
        return slots[2 * q:2 * q + 2].reshape(2 * rows, slots.shape[-1])

    def part_ab(q, c):
        tok = pair_rows(xc, q)
        for i, weight in enumerate((gate, up)):
            if q == 0:
                (load_gate, load_up)[i](c).wait()
            part = _dot(tok, weight[c], 1, 0)
            ab_keep[q, c, i] = part[:rows]
            ab_give[q, c, i] = part[rows:]
        core_ab(q, c).start()

    def part_g(q, c):
        if q == 0:
            load_down(c).wait()
        part = _dot(pair_rows(dyc, q), down[c], 1, 1)
        g_keep[q, c] = part[:rows]
        g_give[q, c] = part[rows:]
        core_g(q, c).start()

    def staggered(first, second, lower=0):
        def body(c, carry):
            first(c)

            @pl.when(c > 0)
            def _():
                second(c - 1)
            return carry

        lax.fori_loop(0, chunks, body, 0)
        second(chunks - 1)

    def each(body):
        lax.fori_loop(0, chunks, lambda c, carry: (body(c), carry)[1], 0)

    token(SIB, 0).wait_recv()
    staggered(functools.partial(part_ab, 0), send_ab)
    token(SIB, 1).wait_recv()
    staggered(functools.partial(part_g, 0), send_g)
    token(FAR, 0).wait_recv()
    token(DIAG, 0).wait_recv()
    each(functools.partial(part_ab, 1))
    token(FAR, 1).wait_recv()
    token(DIAG, 1).wait_recv()
    each(functools.partial(part_g, 1))

    keep_out = [pltpu.make_async_copy(xc, xc_out, out_sem.at[0]), pltpu.make_async_copy(dyc, dyc_out, out_sem.at[1])]
    for copy in keep_out:
        copy.start()

    def gathers(buf, ss, rs):
        def to_far(c):
            return remote(buf.at[c, FAR], buf.at[c, OWN], ss.at[0, c], rs.at[0, c], dp=far)

        def to_sib(c):
            return remote(buf.at[c, FAR], buf.at[c, DIAG], ss.at[1, c], rs.at[1, c], dp=sib)

        def forward(c):
            return remote(buf.at[c, OWN], buf.at[c, SIB], ss.at[2, c], rs.at[2, c], dp=sib)

        return to_far, to_sib, forward

    hid_far, hid_sib, hid_fwd = gathers(hid, hid_ss, hid_rs)
    grad_far, grad_sib, grad_fwd = gathers(grad, grad_ss, grad_rs)

    def hid_save(c):
        return pltpu.make_async_copy(hid.at[c], hid_out.at[c], out_sem.at[2 + c])

    def grad_save(c):
        return pltpu.make_async_copy(grad.at[c], grad_out.at[c], out_sem.at[2 + chunks + c])

    y_acc[...] = jnp.zeros_like(y_acc)
    dx_acc[...] = jnp.zeros_like(dx_acc)

    def add_y(q, c):
        part = _dot(hid[c, 2 * q:2 * q + 2].reshape(2 * rows, CHUNK), down[c], 1, 0)
        y_acc[q] += part.reshape(y_acc.shape[1:])

    def add_dx(q, c):
        part = (_dot(grad[c, 2 * q:2 * q + 2, 0].reshape(2 * rows, CHUNK), gate[c], 1, 1)
                + _dot(grad[c, 2 * q:2 * q + 2, 1].reshape(2 * rows, CHUNK), up[c], 1, 1))
        dx_acc[q] += part.reshape(dx_acc.shape[1:])

    def form_hidden(c):
        core_ab(1, c).wait_recv()
        link_ab(c).wait_recv()
        total = ab_keep[1, c] + ab_got[1, c] + ab_recv[c]
        ab_keep[1, c] = total
        a, b = total[0], total[1]
        hid[c, FAR] = (a * jax.nn.sigmoid(a) * b).astype(BF16)
        hid_far(c).start()
        hid_sib(c).start()

    def away_y(c):
        hid_sib(c).wait_recv()
        add_y(1, c)

    def form_grads(c):
        core_g(1, c).wait_recv()
        link_g(c).wait_recv()
        g = g_keep[1, c] + g_got[1, c] + g_recv[c]
        a, b = ab_keep[1, c, 0], ab_keep[1, c, 1]
        s = jax.nn.sigmoid(a)
        grad[c, FAR, 0] = (g * b * s * (1.0 + a * (1.0 - s))).astype(BF16)
        grad[c, FAR, 1] = (g * (a * s)).astype(BF16)
        grad_far(c).start()
        grad_sib(c).start()

    def away_dx(c):
        grad_sib(c).wait_recv()
        add_dx(1, c)

    results = ((xc, y_acc, y_peer, y_sum, y_stage), (dyc, dx_acc, dx_peer, dx_sum, dx_stage))

    def tp_copy(i, q):
        _, acc, peer, _, _ = results[i]
        return remote(acc.at[q, :, 1 - tp], peer.at[q], tp_ss.at[i, q], tp_rs.at[i, q], tp=1 - tp)

    def row_copies(i, q):
        _, _, _, total, stage = results[i]
        out = []
        for j in (0, 1):
            p = 2 * q + j
            for r in (0, 1):
                device = {} if p == OWN else {'dp': peers[p]}
                if r:
                    device['tp'] = 1 - tp
                if device:
                    out.append(remote(total.at[p], stage.at[p, r], row_ss.at[i, p, r], row_rs.at[i, p, r], **device))
        return out

    def finish(i, q):
        tok, acc, peer, total, stage = results[i]
        tp_copy(i, q).wait()
        total[2 * q:2 * q + 2] = (tok[2 * q:2 * q + 2, tp].astype(F32) + (acc[q, :, tp] + peer[q])).astype(BF16)
        if q == 0:
            stage[OWN, 0] = total[OWN]
        for copy in row_copies(i, q):
            copy.start()

    staggered(form_hidden, away_y)
    tp_copy(0, 1).start()
    staggered(form_grads, away_dx)
    tp_copy(1, 1).start()
    finish(0, 1)

    def take_hidden(c):
        hid_far(c).wait_recv()
        hid_fwd(c).start()

    def home_y(c):
        hid_fwd(c).wait_recv()
        hid_save(c).start()
        add_y(0, c)

    staggered(take_hidden, home_y)
    tp_copy(0, 0).start()
    finish(1, 1)

    def take_grad(c):
        grad_far(c).wait_recv()
        grad_fwd(c).start()

        @pl.when(c == chunks // 2)
        def _():
            finish(0, 0)

    def home_dx(c):
        grad_fwd(c).wait_recv()
        grad_save(c).start()
        add_dx(0, c)

    staggered(take_grad, home_dx)
    tp_copy(1, 0).start()
    finish(1, 0)
    for i in (0, 1):
        for q in (0, 1):
            for copy in row_copies(i, q):
                copy.wait()
    last = [pltpu.make_async_copy(y_stage, y_out, in_sem.at[0]), pltpu.make_async_copy(dx_stage, dx_out, in_sem.at[1])]
    for copy in last:
        copy.start()

    for i in (0, 1):
        for p in (SIB, FAR, DIAG):
            token(p, i).wait_send()
    for copy in keep_out:
        copy.wait()

    def drain(c):
        for copy in (core_ab(0, c), core_ab(1, c), core_g(0, c), core_g(1, c), link_ab(c), link_g(c),
                     hid_far(c), hid_sib(c), hid_fwd(c), grad_far(c), grad_sib(c), grad_fwd(c)):
            copy.wait_send()
        hid_save(c).wait()
        grad_save(c).wait()

    each(drain)
    for copy in last:
        copy.wait()


def gradient_kernel(xc, dyc, hid, grad, y_stage, dx_stage, y_out, dx_out, dgate, dup, ddown, x_t):
    tp = lax.axis_index('tp')
    dp = lax.axis_index('dp')
    sib = dp + 1 - 2 * lax.rem(dp, 2)
    owner = {OWN: dp, FAR: lax.rem(dp + 2, SHARDS), SIB: sib, DIAG: lax.rem(sib + 2, SHARDS)}
    width = xc.shape[-1]
    all_rows = xc.shape[0] * xc.shape[1] * xc.shape[2]

    @pl.when(pl.program_id(0) == 0)
    def _():
        x_t[...] = xc[...].reshape(all_rows, width).T
        for stage, out in ((y_stage, y_out), (dx_stage, dx_out)):
            for p in range(SHARDS):
                at = pl.ds(pl.multiple_of(owner[p] * width, width), width)
                out[tp, :, at] = stage[p, 0]
                out[1 - tp, :, at] = stage[p, 1]

    dgate[...] = _dot(x_t[...], grad[0, :, 0].reshape(all_rows, CHUNK), 1, 0)
    dup[...] = _dot(x_t[...], grad[0, :, 1].reshape(all_rows, CHUNK), 1, 0)
    ddown[...] = _dot(hid[0].reshape(all_rows, CHUNK), dyc[...].reshape(all_rows, width), 0, 0)


def solution(mesh):
    def device_pass(x_rows, gate_blk, up_blk, down_blk, dy_rows):
        rows, model = x_rows.shape
        width, hidden = gate_blk.shape
        chunks = hidden // CHUNK
        half = rows // 2
        hbm = pl.BlockSpec(memory_space=pl.ANY)
        tok = (SHARDS, 2, half, width)
        sds = jax.ShapeDtypeStruct
        dma = pltpu.SemaphoreType.DMA
        xc, dyc, hid, grad, y_stage, dx_stage = pl.pallas_call(
            functools.partial(exchange_kernel, chunks),
            name='exchange',
            out_shape=(sds(tok, BF16), sds(tok, BF16), sds((chunks, SHARDS, rows, CHUNK), BF16),
                       sds((chunks, SHARDS, 2, rows, CHUNK), BF16), sds(tok, BF16), sds(tok, BF16)),
            in_specs=[hbm] * 5,
            out_specs=[hbm] * 6,
            scratch_shapes=[
                pltpu.VMEM((2, half, model), BF16), pltpu.VMEM((2, half, model), BF16),
                pltpu.VMEM(tok, BF16), pltpu.VMEM(tok, BF16),
                pltpu.VMEM((chunks, width, CHUNK), BF16), pltpu.VMEM((chunks, width, CHUNK), BF16),
                pltpu.VMEM((chunks, CHUNK, width), BF16),
                pltpu.VMEM((2, chunks, 2, rows, CHUNK), F32), pltpu.VMEM((2, chunks, 2, rows, CHUNK), F32),
                pltpu.VMEM((2, chunks, 2, rows, CHUNK), F32),
                pltpu.VMEM((2, chunks, rows, CHUNK), F32), pltpu.VMEM((2, chunks, rows, CHUNK), F32),
                pltpu.VMEM((2, chunks, rows, CHUNK), F32),
                pltpu.VMEM((chunks, 2, rows, CHUNK), F32), pltpu.VMEM((chunks, rows, CHUNK), F32),
                pltpu.VMEM((chunks, SHARDS, rows, CHUNK), BF16), pltpu.VMEM((chunks, SHARDS, 2, rows, CHUNK), BF16),
                pltpu.VMEM((2, 2, 2, half, width), F32), pltpu.VMEM((2, 2, 2, half, width), F32),
                pltpu.VMEM((2, 2, half, width), F32), pltpu.VMEM((2, 2, half, width), F32),
                pltpu.VMEM((SHARDS, half, width), BF16), pltpu.VMEM((SHARDS, half, width), BF16),
                pltpu.VMEM(tok, BF16), pltpu.VMEM(tok, BF16),
                dma((4,)), dma((3, chunks)), dma((2, SHARDS)), dma((2, SHARDS)),
                dma((2, 2, chunks)), dma((2, 2, chunks)), dma((2, chunks)), dma((2, chunks)),
                dma((3, chunks)), dma((3, chunks)), dma((3, chunks)), dma((3, chunks)),
                dma((2, 2)), dma((2, 2)), dma((2, SHARDS, 2)), dma((2, SHARDS, 2)), dma((2 + 2 * chunks,)),
            ],
            compiler_params=pltpu.CompilerParams(collective_id=0, has_side_effects=True,
                                                 vmem_limit_bytes=60 * 1024 * 1024),
        )(x_rows.reshape(2, half, model), gate_blk, up_blk, down_blk, dy_rows.reshape(2, half, model))

        whole = lambda shape: pl.BlockSpec(shape, lambda c: (0,) * len(shape))
        y_rows, dx_rows, dw_gate, dw_up, dw_down = pl.pallas_call(
            gradient_kernel,
            name='gradients',
            grid=(chunks,),
            out_shape=(sds((2, half, model), BF16), sds((2, half, model), BF16), sds((width, hidden), F32),
                       sds((width, hidden), F32), sds((hidden, width), F32)),
            in_specs=[whole(tok), whole(tok),
                      pl.BlockSpec((1, SHARDS, rows, CHUNK), lambda c: (c, 0, 0, 0)),
                      pl.BlockSpec((1, SHARDS, 2, rows, CHUNK), lambda c: (c, 0, 0, 0, 0)),
                      whole(tok), whole(tok)],
            out_specs=[whole((2, half, model)), whole((2, half, model)),
                       pl.BlockSpec((width, CHUNK), lambda c: (0, c)), pl.BlockSpec((width, CHUNK), lambda c: (0, c)),
                       pl.BlockSpec((CHUNK, width), lambda c: (c, 0))],
            scratch_shapes=[pltpu.VMEM((width, all_rows := SHARDS * rows), BF16)],
            compiler_params=pltpu.CompilerParams(vmem_limit_bytes=62 * 1024 * 1024),
        )(xc, dyc, hid, grad, y_stage, dx_stage)
        return y_rows.reshape(rows, model), dx_rows.reshape(rows, model), dw_gate, dw_up, dw_down

    row_spec = P('dp', None)
    weight_spec = P('dp', 'tp')
    down_spec = P('tp', 'dp')
    return jax.shard_map(device_pass, mesh=mesh,
                         in_specs=(row_spec, weight_spec, weight_spec, down_spec, row_spec),
                         out_specs=(row_spec, row_spec, weight_spec, weight_spec, down_spec),
                         check_vma=False)
```

```python
import jax
import jax.numpy as jnp
from jax import lax
from jax.experimental import pallas as pl
from jax.experimental.pallas import tpu as pltpu
from jax.sharding import PartitionSpec as P

MESH = pl.DeviceIdType.MESH
F32 = jnp.float32
BF16 = jnp.bfloat16
SHARDS = 4
CHUNK = 512
GROUP = 2 * CHUNK
TILE = 512
RING = 3
OWN, SIB, FAR, DIAG = 0, 1, 2, 3
(S_TOK, S_TOK_FWD, S_CORE_AB, S_CORE_G, S_LINK_AB, S_LINK_G, S_HID_FAR, S_HID_SIB, S_HID_FWD, S_GRAD_FAR, S_GRAD_SIB,
 S_GRAD_FWD, S_TP, S_ROW_HOME, S_ROW_AWAY, S_ROW_FWD, S_TAIL) = (0, 2, 4, 6, 8, 9, 10, 11, 12, 13, 14, 15, 16, 19, 20, 22, 23)
SENDS = 26


def _dot(lhs, rhs, lhs_dim, rhs_dim):
    return lax.dot_general(lhs, rhs, (((lhs_dim,), (rhs_dim,)), ((), ())), preferred_element_type=F32)


def exchange_kernel(x_own, gate_hbm, up_hbm, down_hbm, dy_own,
                    x_t, dyc, hid, grad, y_rows, dx_rows,
                    xc, gate_up, down,
                    ab_keep, ab_give, ab_got, g_keep, g_give, g_got, ab_recv, g_recv,
                    y_acc, dx_away, dx_home, y_peer, dx_peer, y_sum, dx_sum, y_stage, dx_stage, here_in, near_in,
                    send, gate_up_sem, down_sem, tok_rs, core_rs, away_rs, link_rs,
                    hid_rs, grad_rs, grad_sib_rs, tp_rs, home_rs, away_row_rs, tail_rs):
    tp = lax.axis_index('tp')
    dp = lax.axis_index('dp')
    sib = dp + 1 - 2 * lax.rem(dp, 2)
    far = lax.rem(dp + 2, SHARDS)
    diag = lax.rem(sib + 2, SHARDS)
    peers = {SIB: sib, FAR: far, DIAG: diag}
    half, width = xc.shape[-2:]
    groups = hid.shape[0]

    def remote(src, dst, ss, rs, **device):
        return pltpu.make_async_remote_copy(src_ref=src, dst_ref=dst, send_sem=send.at[ss], recv_sem=rs,
                                            device_id=device, device_id_type=MESH)

    def cols(i):
        return pl.ds(pl.multiple_of(i * width, width), width)

    def chunk_of(g, s):
        return pl.ds(pl.multiple_of(g * GROUP, GROUP) + s * CHUNK, CHUNK)

    def load_gate_up(g, s):
        sem = gate_up_sem.at[2 * g + s]
        return (pltpu.make_async_copy(gate_hbm.at[:, chunk_of(g, s)], gate_up.at[g, s, 0], sem),
                pltpu.make_async_copy(up_hbm.at[:, chunk_of(g, s)], gate_up.at[g, s, 1], sem))

    def load_down(g):
        return pltpu.make_async_copy(down_hbm.at[pl.ds(pl.multiple_of(g * GROUP, GROUP), GROUP)], down.at[g], down_sem.at[g])

    tokens = ((x_own, xc), (dy_own, dyc))
    barrier = pltpu.get_barrier_semaphore()
    for p in (FAR, SIB, DIAG):
        pl.semaphore_signal(barrier, inc=1, device_id={'dp': peers[p]}, device_id_type=MESH)
        pl.semaphore_signal(barrier, inc=1, device_id={'dp': peers[p], 'tp': 1 - tp}, device_id_type=MESH)
    pl.semaphore_signal(barrier, inc=1, device_id={'tp': 1 - tp}, device_id_type=MESH)
    for g in range(groups):
        for s in (0, 1):
            for copy in load_gate_up(g, s):
                copy.start()
    for g in range(groups):
        load_down(g).start()
    for own, slots in tokens:
        slots[:, OWN] = own[:, :, cols(dp)]
    pl.semaphore_wait(barrier, 2 * SHARDS - 1)

    def token(p, i):
        own, slots = tokens[i]
        if p == SIB:
            return remote(own.at[:, :, cols(sib)], slots.at[:, SIB], S_TOK + i, tok_rs.at[i, 0], dp=sib)
        return remote(own.at[tp, :, cols(peers[p])], slots.at[tp, p], S_TOK + i, tok_rs.at[i, 1], dp=peers[p])

    def token_fwd(i):
        part = tokens[i][1].at[tp, 2:4]
        return remote(part, part, S_TOK_FWD + i, tok_rs.at[i, 2], tp=1 - tp)

    def tokens_far(i):
        part = tokens[i][1].at[tp, 2:4]
        return remote(part, part, S_TOK + i, tok_rs.at[i, 1], dp=far)

    for i in (0, 1):
        for p in (SIB, FAR, DIAG):
            token(p, i).start()

    def core_ab(q, c):
        rs = core_rs.at[0, c] if q == 0 else away_rs.at[0]
        return remote(ab_give.at[q, c], ab_got.at[q, c], S_CORE_AB + q, rs, dp=sib)

    def core_g(q, c):
        rs = core_rs.at[1, c] if q == 0 else away_rs.at[1]
        return remote(g_give.at[q, c], g_got.at[q, c], S_CORE_G + q, rs, dp=sib)

    def link_ab(c):
        return remote(ab_keep.at[0, c], ab_recv.at[c], S_LINK_AB, link_rs.at[0, c], dp=far)

    def link_g(c):
        return remote(g_keep.at[0, c], g_recv.at[c], S_LINK_G, link_rs.at[1, c], dp=far)

    def send_ab(c):
        core_ab(0, c).wait_recv()
        ab_keep[0, c] += ab_got[0, c]
        link_ab(c).start()

    def send_g(c):
        core_g(0, c).wait_recv()
        g_keep[0, c] += g_got[0, c]
        link_g(c).start()

    def pair_rows(slots, q):
        return slots[:, 2 * q:2 * q + 2].reshape(4 * half, slots.shape[-1])

    def split(part):
        part = part.reshape(2, 2, half, part.shape[-1])
        return part[:, 0], part[:, 1]

    def part_ab(q, g, s):
        c = 2 * g + s
        if q == 0:
            pltpu.make_async_copy(gate_up.at[g, s], gate_up.at[g, s], gate_up_sem.at[c]).wait()
        tok = pair_rows(xc, q)
        for i in (0, 1):
            ab_keep[q, c, i], ab_give[q, c, i] = split(_dot(tok, gate_up[g, s, i], 1, 0))
        core_ab(q, c).start()

    def part_g(q, g, s):
        c = 2 * g + s
        if q == 0 and s == 0:
            load_down(g).wait()
        g_keep[q, c], g_give[q, c] = split(_dot(pair_rows(dyc, q), down[g, s * CHUNK:(s + 1) * CHUNK], 1, 1))
        core_g(q, c).start()

    def each(body):
        lax.fori_loop(0, groups, lambda g, carry: (body(g), carry)[1], 0)

    def behind(first, second):
        def body(g):
            first(g)

            @pl.when(g > 0)
            def _():
                second(g - 1)

        each(body)
        second(groups - 1)

    def home_parts(part, send_on):
        def body(g):
            part(0, g, 0)

            @pl.when(g > 0)
            def _():
                send_on(2 * g - 1)
            part(0, g, 1)
            send_on(2 * g)

        each(body)
        send_on(2 * groups - 1)

    def away_parts(part):
        each(lambda g: (part(1, g, 0), part(1, g, 1)))

    token(SIB, 0).wait_recv()
    home_parts(part_ab, send_ab)
    for i in (0, 1):
        tokens_far(i).wait_recv()
        token_fwd(i).start()
    token(SIB, 1).wait_recv()
    home_parts(part_g, send_g)
    token_fwd(0).wait_recv()
    away_parts(part_ab)
    token_fwd(1).wait_recv()
    away_parts(part_g)
    x_t[...] = xc[...].reshape(2 * SHARDS * half, width).T

    def hid_far(g):
        return remote(hid.at[g, :, FAR], hid.at[g, :, OWN], S_HID_FAR, hid_rs.at[0, g], dp=far)

    def hid_sib(g):
        return remote(hid.at[g, :, FAR], hid.at[g, :, DIAG], S_HID_SIB, hid_rs.at[1, g], dp=sib)

    def hid_fwd(g):
        return remote(hid.at[g, :, OWN], hid.at[g, :, SIB], S_HID_FWD, hid_rs.at[2, g], dp=sib)

    def grad_far(g, h):
        return remote(grad.at[g, h, FAR], grad.at[g, h, OWN], S_GRAD_FAR, grad_rs.at[0, h, g], dp=far)

    def grad_sib(g):
        return remote(grad.at[g, :, FAR], grad.at[g, :, DIAG], S_GRAD_SIB, grad_sib_rs, dp=sib)

    def grad_fwd(g, h):
        return remote(grad.at[g, h, OWN], grad.at[g, h, SIB], S_GRAD_FWD, grad_rs.at[1, h, g], dp=sib)

    y_acc[...] = jnp.zeros_like(y_acc)
    dx_away[...] = jnp.zeros_like(dx_away)
    dx_home[...] = jnp.zeros_like(dx_home)

    def add_y(q, g):
        part = _dot(hid[g, :, 2 * q:2 * q + 2].reshape(4 * half, GROUP), down[g], 1, 0)
        y_acc[q] += part.reshape(y_acc.shape[1:])

    def dx_part(take, count, g):
        part = None
        for s in (0, 1):
            for i in (0, 1):
                lhs = take(i, s * CHUNK).reshape(count, CHUNK)
                term = _dot(lhs, gate_up[g, s, i], 1, 1)
                part = term if part is None else part + term
        return part

    def add_dx_away(g):
        part = dx_part(lambda i, at: grad[g, :, 2:4, i, :, at:at + CHUNK], 4 * half, g)
        dx_away[...] += part.reshape(dx_away.shape)

    def add_dx_home(g, h):
        part = dx_part(lambda i, at: grad[g, h, 0:2, i, :, at:at + CHUNK], 2 * half, g)
        dx_home[h] += part.reshape(dx_home.shape[1:])

    def form_hidden(g):
        for s in (0, 1):
            c = 2 * g + s
            link_ab(c).wait_recv()
            total = ab_keep[1, c] + ab_got[1, c] + ab_recv[c]
            ab_keep[1, c] = total
            a, b = total[0], total[1]
            hid[g, :, FAR, :, s * CHUNK:(s + 1) * CHUNK] = (a * jax.nn.sigmoid(a) * b).astype(BF16)
        hid_far(g).start()
        hid_sib(g).start()

    def away_y(g):
        hid_sib(g).wait_recv()
        add_y(1, g)

    def form_grads(g):
        for s in (0, 1):
            c = 2 * g + s
            link_g(c).wait_recv()
            v = g_keep[1, c] + g_got[1, c] + g_recv[c]
            a, b = ab_keep[1, c, 0], ab_keep[1, c, 1]
            sig = jax.nn.sigmoid(a)
            grad[g, :, FAR, 0, :, s * CHUNK:(s + 1) * CHUNK] = (v * b * sig * (1.0 + a * (1.0 - sig))).astype(BF16)
            grad[g, :, FAR, 1, :, s * CHUNK:(s + 1) * CHUNK] = (v * (a * sig)).astype(BF16)
        grad_far(g, 0).start()
        grad_sib(g).start()

    def tp_copy(acc, peer, k):
        return remote(acc.at[1 - tp], peer, S_TP + k, tp_rs.at[k], tp=1 - tp)

    y_tp = [tp_copy(y_acc.at[q], y_peer.at[q], q) for q in (0, 1)]
    dx_tp = tp_copy(dx_away, dx_peer, 2)

    def row_home(p, r):
        device = {} if p == OWN else {'dp': sib}
        if r:
            device['tp'] = 1 - tp
        return remote(y_sum.at[p], y_stage.at[p, r], S_ROW_HOME, home_rs.at[2 if p == OWN else r], **device)

    home_rows = ((OWN, 1), (SIB, 0), (SIB, 1))

    def y_away(p):
        return remote(y_sum.at[p], y_stage.at[p, 0], S_ROW_AWAY, away_row_rs.at[0], dp=peers[p])

    def y_away_all():
        return remote(y_sum.at[2:4], y_stage.at[2:4, 0], S_ROW_AWAY, away_row_rs.at[0], dp=far)

    def y_away_fwd():
        return remote(y_stage.at[2:4, 0], y_stage.at[2:4, 1], S_ROW_FWD, away_row_rs.at[1], tp=1 - tp)

    def dx_row(p, r):
        device = {'dp': peers[p]}
        if r:
            device['tp'] = 1 - tp
        return remote(dx_sum.at[p - 2], dx_stage.at[r, p - 2], S_ROW_AWAY + 1, away_row_rs.at[2 + r], **device)

    def dx_row_all(r):
        return remote(dx_sum, dx_stage.at[r], S_ROW_AWAY + 1, away_row_rs.at[2 + r], dp=far)

    def finish_y(q):
        y_tp[q].wait()
        y_sum[2 * q:2 * q + 2] = (xc[tp, 2 * q:2 * q + 2].astype(F32) + (y_acc[q, tp] + y_peer[q])).astype(BF16)
        if q == 0:
            y_stage[OWN, 0] = y_sum[OWN]
            for p, r in home_rows:
                row_home(p, r).start()
        else:
            for p in (FAR, DIAG):
                y_away(p).start()

    def tail(h):
        return (remote(dx_home.at[h, 0], here_in.at[h], S_TAIL, tail_rs.at[h, 0], tp=1 - tp),
                remote(dx_home.at[h, 1], near_in.at[h, 1], S_TAIL + 1, tail_rs.at[h, 1], dp=sib, tp=1 - tp),
                remote(dx_home.at[h, 1], near_in.at[h, 0], S_TAIL + 2, tail_rs.at[h, 2], dp=sib))

    def finish_dx_home(h):
        for copy in tail(h):
            copy.wait_recv()
        dx_rows[h, :, cols(dp)] = (dyc[h, OWN].astype(F32) + (dx_home[h, 0] + here_in[h])).astype(BF16)
        dx_rows[h, :, cols(sib)] = (dy_own[h, :, cols(sib)].astype(F32) + (near_in[h, 0] + near_in[h, 1])).astype(BF16)

    remote(ab_give.at[1], ab_got.at[1], S_CORE_AB + 1, away_rs.at[0], dp=sib).wait()
    behind(form_hidden, away_y)
    y_tp[1].start()
    remote(g_give.at[1], g_got.at[1], S_CORE_G + 1, away_rs.at[1], dp=sib).wait()
    each(form_grads)
    finish_y(1)
    each(lambda g: grad_far(g, 1).start())

    def take_hidden(g):
        hid_far(g).wait_recv()
        hid_fwd(g).start()

    def home_y(g):
        hid_fwd(g).wait_recv()
        add_y(0, g)
        add_dx_away(g)

    remote(grad.at[:, :, FAR], grad.at[:, :, DIAG], S_GRAD_SIB, grad_sib_rs, dp=sib).wait()
    behind(take_hidden, home_y)
    y_tp[0].start()
    dx_tp.start()

    def take_grad(h):
        def body(g):
            grad_far(g, h).wait_recv()
            grad_fwd(g, h).start()
        return body

    def home_dx(h):
        def body(g):
            grad_fwd(g, h).wait_recv()
            add_dx_home(g, h)
        return body

    behind(take_grad(0), home_dx(0))
    for copy in tail(0):
        copy.start()
    finish_y(0)
    y_away_all().wait_recv()
    y_away_fwd().start()
    dx_tp.wait()
    dx_sum[...] = (dyc[tp, 2:4].astype(F32) + (dx_away[tp] + dx_peer[...])).astype(BF16)

    each_home = home_dx(1)

    def last_grads(g):
        take_grad(1)(g)

        @pl.when(g == groups - 1)
        def _():
            for p in (FAR, DIAG):
                for r in (1, 0):
                    dx_row(p, r).start()

    behind(last_grads, each_home)
    for copy in tail(1):
        copy.start()

    finish_dx_home(0)
    for p, r in home_rows:
        row_home(p, r).wait_recv()
    y_away_fwd().wait_recv()
    owner = {OWN: dp, SIB: sib, FAR: far, DIAG: diag}
    for p in range(SHARDS):
        y_rows[tp, :, cols(owner[p])] = y_stage[p, 0]
        y_rows[1 - tp, :, cols(owner[p])] = y_stage[p, 1]

    for i in (0, 1):
        slots = tokens[i][1]
        remote(slots.at[:, 0:2], slots.at[:, 0:2], S_TOK + i, tok_rs.at[i, 0], dp=sib).wait_send()
        token_fwd(i).wait_send()
    remote(ab_give.at[0], ab_got.at[0], S_CORE_AB, core_rs.at[0, 0], dp=sib).wait_send()
    remote(g_give.at[0], g_got.at[0], S_CORE_G, core_rs.at[0, 0], dp=sib).wait_send()
    remote(ab_keep.at[0], ab_recv, S_LINK_AB, link_rs.at[0, 0], dp=far).wait_send()
    remote(g_keep.at[0], g_recv, S_LINK_G, link_rs.at[0, 0], dp=far).wait_send()
    for kind in (S_HID_FAR, S_HID_SIB, S_HID_FWD):
        remote(hid.at[:, :, OWN], hid.at[:, :, SIB], kind, hid_rs.at[0, 0], dp=sib).wait_send()
    for kind in (S_GRAD_FAR, S_GRAD_FWD):
        remote(grad.at[:, :, OWN], grad.at[:, :, SIB], kind, grad_sib_rs, dp=sib).wait_send()
    remote(y_sum.at[0:3], y_sum.at[0:3], S_ROW_HOME, home_rs.at[0], dp=sib).wait_send()
    y_away_all().wait_send()
    y_away_fwd().wait_send()
    remote(dx_stage, dx_stage, S_ROW_AWAY + 1, away_row_rs.at[2], dp=far).wait_send()

    for r in (0, 1):
        dx_row_all(r).wait_recv()
    for p in (FAR, DIAG):
        dx_rows[tp, :, cols(owner[p])] = dx_stage[0, p - 2]
        dx_rows[1 - tp, :, cols(owner[p])] = dx_stage[1, p - 2]
    finish_dx_home(1)
    for k in range(3):
        remote(dx_home.at[:, 0], here_in, S_TAIL + k, tail_rs.at[0, 0], dp=sib).wait_send()


def gradient_kernel(x_t, dyc, hid, grad, y_rows, dx_rows, y_out, dx_out, dgate_out, dup_out, ddown_out,
                    dgate, dup, ddown, row_sem, tile_sem):
    groups = hid.shape[0]
    tokens = x_t.shape[1]
    width = dyc.shape[-1]
    per_group = GROUP // TILE
    rows_out = [pltpu.make_async_copy(y_rows, y_out, row_sem.at[0]), pltpu.make_async_copy(dx_rows, dx_out, row_sem.at[1])]

    def write(n, slot, k):
        at = pl.ds(pl.multiple_of(n * TILE, TILE), TILE)
        out = ddown_out.at[at] if k == 2 else (dgate_out, dup_out)[k].at[:, at]
        return pltpu.make_async_copy((dgate, dup, ddown)[k].at[slot], out, tile_sem.at[k, slot])

    def body(g, carry):
        for s in range(per_group):
            n = g * per_group + s
            slot = lax.rem(n, RING)

            def take(k):
                @pl.when(n >= RING)
                def _():
                    write(n - RING, slot, k).wait()

            at = slice(s * TILE, (s + 1) * TILE)
            for k, buf in enumerate((dgate, dup)):
                take(k)
                buf[slot] = _dot(x_t[...], grad[g, :, :, k, :, at].reshape(tokens, TILE), 1, 0)
                write(n, slot, k).start()
            take(2)
            ddown[slot] = _dot(hid[g, :, :, :, at].reshape(tokens, TILE), dyc[...].reshape(tokens, width), 0, 0)
            write(n, slot, 2).start()
        return carry

    lax.fori_loop(0, groups, body, 0)
    for copy in rows_out:
        copy.start()
    for n in range(groups * per_group - RING, groups * per_group):
        for k in range(3):
            write(n, n % RING, k).wait()
    for copy in rows_out:
        copy.wait()


def solution(mesh):
    def device_pass(x_rows, gate_blk, up_blk, down_blk, dy_rows):
        rows, model = x_rows.shape
        width, hidden = gate_blk.shape
        chunks, groups = hidden // CHUNK, hidden // GROUP
        half = rows // 2
        tokens = SHARDS * rows
        hbm = pl.BlockSpec(memory_space=pl.ANY)
        vmem = pl.BlockSpec(memory_space=pltpu.VMEM)
        sds = jax.ShapeDtypeStruct
        dma = pltpu.SemaphoreType.DMA
        tok = (2, SHARDS, half, width)
        block = (2, half, width)
        own = (2, half, model)
        x_t, dyc, hid, grad, y_own, dx_own = pl.pallas_call(
            exchange_kernel,
            name='exchange',
            out_shape=(sds((width, tokens), BF16), sds(tok, BF16), sds((groups, 2, SHARDS, half, GROUP), BF16),
                       sds((groups, 2, SHARDS, 2, half, GROUP), BF16), sds(own, BF16), sds(own, BF16)),
            in_specs=[vmem, hbm, hbm, hbm, vmem],
            out_specs=[vmem] * 6,
            scratch_shapes=[
                pltpu.VMEM(tok, BF16),
                pltpu.VMEM((groups, 2, 2, width, CHUNK), BF16), pltpu.VMEM((groups, GROUP, width), BF16),
                pltpu.VMEM((2, chunks, 2, 2, half, CHUNK), F32), pltpu.VMEM((2, chunks, 2, 2, half, CHUNK), F32),
                pltpu.VMEM((2, chunks, 2, 2, half, CHUNK), F32),
                pltpu.VMEM((2, chunks, 2, half, CHUNK), F32), pltpu.VMEM((2, chunks, 2, half, CHUNK), F32),
                pltpu.VMEM((2, chunks, 2, half, CHUNK), F32),
                pltpu.VMEM((chunks, 2, 2, half, CHUNK), F32), pltpu.VMEM((chunks, 2, half, CHUNK), F32),
                pltpu.VMEM((2, 2) + block, F32), pltpu.VMEM((2,) + block, F32), pltpu.VMEM((2,) + block, F32),
                pltpu.VMEM((2,) + block, F32), pltpu.VMEM(block, F32),
                pltpu.VMEM((SHARDS, half, width), BF16), pltpu.VMEM(block, BF16),
                pltpu.VMEM((SHARDS, 2, half, width), BF16), pltpu.VMEM((2,) + block, BF16),
                pltpu.VMEM(block, F32), pltpu.VMEM((2,) + block, F32),
                dma((SENDS,)), dma((chunks,)), dma((groups,)), dma((2, 3)), dma((2, chunks)), dma((2,)),
                dma((2, chunks)), dma((3, groups)), dma((2, 2, groups)), dma(()), dma((3,)), dma((3,)), dma((4,)), dma((2, 3)),
            ],
            compiler_params=pltpu.CompilerParams(collective_id=0, has_side_effects=True,
                                                 vmem_limit_bytes=44 * 1024 * 1024),
        )(x_rows.reshape(own), gate_blk, up_blk, down_blk, dy_rows.reshape(own))

        y_new, dx_new, dw_gate, dw_up, dw_down = pl.pallas_call(
            gradient_kernel,
            name='gradients',
            out_shape=(sds(own, BF16), sds(own, BF16), sds((width, hidden), F32), sds((width, hidden), F32),
                       sds((hidden, width), F32)),
            in_specs=[vmem] * 6,
            out_specs=[hbm] * 5,
            scratch_shapes=[pltpu.VMEM((RING, width, TILE), F32), pltpu.VMEM((RING, width, TILE), F32),
                            pltpu.VMEM((RING, TILE, width), F32), dma((2,)), dma((3, RING))],
            compiler_params=pltpu.CompilerParams(vmem_limit_bytes=44 * 1024 * 1024),
        )(x_t, dyc, hid, grad, y_own, dx_own)
        return y_new.reshape(rows, model), dx_new.reshape(rows, model), dw_gate, dw_up, dw_down

    row_spec = P('dp', None)
    weight_spec = P('dp', 'tp')
    down_spec = P('tp', 'dp')
    return jax.shard_map(device_pass, mesh=mesh,
                         in_specs=(row_spec, weight_spec, weight_spec, down_spec, row_spec),
                         out_specs=(row_spec, row_spec, weight_spec, weight_spec, down_spec),
                         check_vma=False)
```

```python
import jax
import jax.numpy as jnp
from jax import lax
from jax.experimental import pallas as pl
from jax.experimental.pallas import tpu as pltpu
from jax.sharding import PartitionSpec as P

MESH = pl.DeviceIdType.MESH
F32 = jnp.float32
BF16 = jnp.bfloat16
SHARDS = 4
CHUNK = 512
GROUP = 2 * CHUNK
TILE = 512
RING = 3
OWN, SIB, FAR, DIAG = 0, 1, 2, 3
(S_TOK, S_TOK_FWD, S_CORE_AB, S_CORE_G, S_LINK_AB, S_LINK_G, S_HID_FAR, S_HID_SIB, S_HID_FWD, S_GRAD_FAR, S_GRAD_SIB,
 S_GRAD_FWD, S_TP, S_ROW_HOME, S_ROW_AWAY, S_ROW_FWD, S_TAIL) = (0, 2, 4, 6, 8, 9, 10, 11, 12, 13, 14, 15, 16, 19, 20, 22, 23)
SENDS = 26


def _dot(lhs, rhs, lhs_dim, rhs_dim):
    return lax.dot_general(lhs, rhs, (((lhs_dim,), (rhs_dim,)), ((), ())), preferred_element_type=F32)


def exchange_kernel(token_rows, gate_hbm, up_hbm, down_hbm,
                    x_t, dyc, hid, grad, y_rows, dx_rows,
                    xc, gate_up, down,
                    ab_keep, ab_give, ab_got, g_keep, g_give, g_got, ab_recv, g_recv,
                    y_acc, dx_away, dx_home, y_peer, dx_peer, y_sum, dx_sum, y_stage, dx_stage, here_in, near_in,
                    send, gate_up_sem, down_sem, tok_rs, core_rs, away_rs, link_rs,
                    hid_rs, grad_rs, grad_sib_rs, tp_rs, home_rs, away_row_rs, tail_rs):
    tp = lax.axis_index('tp')
    dp = lax.axis_index('dp')
    sib = dp + 1 - 2 * lax.rem(dp, 2)
    far = lax.rem(dp + 2, SHARDS)
    diag = lax.rem(sib + 2, SHARDS)
    peers = {SIB: sib, FAR: far, DIAG: diag}
    half, width = xc.shape[-2:]
    groups = hid.shape[0]

    def remote(src, dst, ss, rs, **device):
        return pltpu.make_async_remote_copy(src_ref=src, dst_ref=dst, send_sem=send.at[ss], recv_sem=rs,
                                            device_id=device, device_id_type=MESH)

    def cols(i):
        return pl.ds(pl.multiple_of(i * width, width), width)

    def chunk_of(g, s):
        return pl.ds(pl.multiple_of(g * GROUP, GROUP) + s * CHUNK, CHUNK)

    def load_gate_up(g, s):
        sem = gate_up_sem.at[2 * g + s]
        return (pltpu.make_async_copy(gate_hbm.at[:, chunk_of(g, s)], gate_up.at[g, s, 0], sem),
                pltpu.make_async_copy(up_hbm.at[:, chunk_of(g, s)], gate_up.at[g, s, 1], sem))

    def load_down(g):
        return pltpu.make_async_copy(down_hbm.at[pl.ds(pl.multiple_of(g * GROUP, GROUP), GROUP)], down.at[g], down_sem.at[g])

    tokens = ((token_rows.at[0], xc), (token_rows.at[1], dyc))
    dy_own = token_rows.at[1]
    barrier = pltpu.get_barrier_semaphore()
    for p in (FAR, SIB, DIAG):
        pl.semaphore_signal(barrier, inc=1, device_id={'dp': peers[p]}, device_id_type=MESH)
        pl.semaphore_signal(barrier, inc=1, device_id={'dp': peers[p], 'tp': 1 - tp}, device_id_type=MESH)
    pl.semaphore_signal(barrier, inc=1, device_id={'tp': 1 - tp}, device_id_type=MESH)
    for g in range(groups):
        for s in (0, 1):
            for copy in load_gate_up(g, s):
                copy.start()
    for g in range(groups):
        load_down(g).start()
    for own, slots in tokens:
        slots[:, OWN] = own[:, :, cols(dp)]
    pl.semaphore_wait(barrier, 2 * SHARDS - 1)

    def token(p, i):
        own, slots = tokens[i]
        if p == SIB:
            return remote(own.at[:, :, cols(sib)], slots.at[:, SIB], S_TOK + i, tok_rs.at[i, 0], dp=sib)
        return remote(own.at[tp, :, cols(peers[p])], slots.at[tp, p], S_TOK + i, tok_rs.at[i, 1], dp=peers[p])

    def token_fwd(i):
        part = tokens[i][1].at[tp, 2:4]
        return remote(part, part, S_TOK_FWD + i, tok_rs.at[i, 2], tp=1 - tp)

    def tokens_far(i):
        part = tokens[i][1].at[tp, 2:4]
        return remote(part, part, S_TOK + i, tok_rs.at[i, 1], dp=far)

    for i in (0, 1):
        for p in (SIB, FAR, DIAG):
            token(p, i).start()

    def core_ab(q, c, i):
        rs = core_rs.at[i, c] if q == 0 else away_rs.at[0]
        return remote(ab_give.at[q, c, i], ab_got.at[q, c, i], S_CORE_AB + q, rs, dp=sib)

    def core_g(q, c):
        rs = core_rs.at[2, c] if q == 0 else away_rs.at[1]
        return remote(g_give.at[q, c], g_got.at[q, c], S_CORE_G + q, rs, dp=sib)

    def link_ab(c, i):
        return remote(ab_keep.at[0, c, i], ab_recv.at[c, i], S_LINK_AB, link_rs.at[i, c], dp=far)

    def link_g(c):
        return remote(g_keep.at[0, c], g_recv.at[c], S_LINK_G, link_rs.at[2, c], dp=far)

    def send_ab(c, i):
        core_ab(0, c, i).wait_recv()
        ab_keep[0, c, i] += ab_got[0, c, i]
        link_ab(c, i).start()

    def send_g(c):
        core_g(0, c).wait_recv()
        g_keep[0, c] += g_got[0, c]
        link_g(c).start()

    def pair_rows(slots, q):
        return slots[:, 2 * q:2 * q + 2].reshape(4 * half, slots.shape[-1])

    def split(part):
        part = part.reshape(2, 2, half, part.shape[-1])
        return part[:, 0], part[:, 1]

    def part_ab(q, g, s, i):
        c = 2 * g + s
        if q == 0 and i == 0:
            pltpu.make_async_copy(gate_up.at[g, s], gate_up.at[g, s], gate_up_sem.at[c]).wait()
        ab_keep[q, c, i], ab_give[q, c, i] = split(_dot(pair_rows(xc, q), gate_up[g, s, i], 1, 0))
        core_ab(q, c, i).start()

    def part_g(q, g, s):
        c = 2 * g + s
        if q == 0 and s == 0:
            load_down(g).wait()
        g_keep[q, c], g_give[q, c] = split(_dot(pair_rows(dyc, q), down[g, s * CHUNK:(s + 1) * CHUNK], 1, 1))
        core_g(q, c).start()

    def each(body):
        lax.fori_loop(0, groups, lambda g, carry: (body(g), carry)[1], 0)

    def behind(first, second):
        def body(g):
            first(g)

            @pl.when(g > 0)
            def _():
                second(g - 1)

        each(body)
        second(groups - 1)

    def home_parts(part, send_on, kinds):
        steps = [(s,) + kind for s in (0, 1) for kind in kinds]

        def body(g):
            for n, (s, *kind) in enumerate(steps):
                part(0, g, s, *kind)
                before_s, *before = steps[n - 1]
                if n == 0:
                    pl.when(g > 0)(lambda: send_on(2 * g - 1, *before))
                else:
                    send_on(2 * g + before_s, *before)

        each(body)
        send_on(2 * groups - 1, *kinds[-1])

    token(SIB, 0).wait_recv()
    home_parts(part_ab, send_ab, ((0,), (1,)))
    for i in (0, 1):
        tokens_far(i).wait_recv()
        token_fwd(i).start()
    token(SIB, 1).wait_recv()
    home_parts(part_g, send_g, ((),))
    token_fwd(0).wait_recv()
    each(lambda g: [part_ab(1, g, s, i) for s in (0, 1) for i in (0, 1)])
    token_fwd(1).wait_recv()
    each(lambda g: [part_g(1, g, s) for s in (0, 1)])
    x_t[...] = xc[...].reshape(2 * SHARDS * half, width).T

    def hid_far(g):
        return remote(hid.at[g, :, FAR], hid.at[g, :, OWN], S_HID_FAR, hid_rs.at[0, g], dp=far)

    def hid_sib(g):
        return remote(hid.at[g, :, FAR], hid.at[g, :, DIAG], S_HID_SIB, hid_rs.at[1, g], dp=sib)

    def hid_fwd(g):
        return remote(hid.at[g, :, OWN], hid.at[g, :, SIB], S_HID_FWD, hid_rs.at[2, g], dp=sib)

    def grad_far(g, h):
        return remote(grad.at[g, h, FAR], grad.at[g, h, OWN], S_GRAD_FAR, grad_rs.at[0, h, g], dp=far)

    def grad_sib(g):
        return remote(grad.at[g, :, FAR], grad.at[g, :, DIAG], S_GRAD_SIB, grad_sib_rs, dp=sib)

    def grad_fwd(g, h):
        return remote(grad.at[g, h, OWN], grad.at[g, h, SIB], S_GRAD_FWD, grad_rs.at[1, h, g], dp=sib)

    y_acc[...] = jnp.zeros_like(y_acc)
    dx_away[...] = jnp.zeros_like(dx_away)
    dx_home[...] = jnp.zeros_like(dx_home)

    def add_y(q, g):
        part = _dot(hid[g, :, 2 * q:2 * q + 2].reshape(4 * half, GROUP), down[g], 1, 0)
        y_acc[q] += part.reshape(y_acc.shape[1:])

    def dx_part(take, count, g):
        part = None
        for s in (0, 1):
            for i in (0, 1):
                lhs = take(i, s * CHUNK).reshape(count, CHUNK)
                term = _dot(lhs, gate_up[g, s, i], 1, 1)
                part = term if part is None else part + term
        return part

    def add_dx_away(g):
        part = dx_part(lambda i, at: grad[g, :, 2:4, i, :, at:at + CHUNK], 4 * half, g)
        dx_away[...] += part.reshape(dx_away.shape)

    def add_dx_home(g, h):
        part = dx_part(lambda i, at: grad[g, h, 0:2, i, :, at:at + CHUNK], 2 * half, g)
        dx_home[h] += part.reshape(dx_home.shape[1:])

    def form_hidden(g):
        for s in (0, 1):
            c = 2 * g + s
            for i in (0, 1):
                link_ab(c, i).wait_recv()
            total = ab_keep[1, c] + ab_got[1, c] + ab_recv[c]
            ab_keep[1, c] = total
            a, b = total[0], total[1]
            hid[g, :, FAR, :, s * CHUNK:(s + 1) * CHUNK] = (a * jax.nn.sigmoid(a) * b).astype(BF16)
        hid_far(g).start()
        hid_sib(g).start()

    def away_y(g):
        hid_sib(g).wait_recv()
        add_y(1, g)

    def form_grads(g):
        for s in (0, 1):
            c = 2 * g + s
            link_g(c).wait_recv()
            v = g_keep[1, c] + g_got[1, c] + g_recv[c]
            a, b = ab_keep[1, c, 0], ab_keep[1, c, 1]
            sig = jax.nn.sigmoid(a)
            grad[g, :, FAR, 0, :, s * CHUNK:(s + 1) * CHUNK] = (v * b * sig * (1.0 + a * (1.0 - sig))).astype(BF16)
            grad[g, :, FAR, 1, :, s * CHUNK:(s + 1) * CHUNK] = (v * (a * sig)).astype(BF16)
        grad_far(g, 0).start()
        grad_sib(g).start()

    def tp_copy(acc, peer, k):
        return remote(acc.at[1 - tp], peer, S_TP + k, tp_rs.at[k], tp=1 - tp)

    y_tp = [tp_copy(y_acc.at[q], y_peer.at[q], q) for q in (0, 1)]
    dx_tp = tp_copy(dx_away, dx_peer, 2)

    def row_home(p, r):
        device = {} if p == OWN else {'dp': sib}
        if r:
            device['tp'] = 1 - tp
        return remote(y_sum.at[p], y_stage.at[p, r], S_ROW_HOME, home_rs.at[2 if p == OWN else r], **device)

    home_rows = ((OWN, 1), (SIB, 0), (SIB, 1))

    def y_away(p):
        return remote(y_sum.at[p], y_stage.at[p, 0], S_ROW_AWAY, away_row_rs.at[0], dp=peers[p])

    def y_away_all():
        return remote(y_sum.at[2:4], y_stage.at[2:4, 0], S_ROW_AWAY, away_row_rs.at[0], dp=far)

    def y_away_fwd():
        return remote(y_stage.at[2:4, 0], y_stage.at[2:4, 1], S_ROW_FWD, away_row_rs.at[1], tp=1 - tp)

    def dx_row(p, r):
        device = {'dp': peers[p]}
        if r:
            device['tp'] = 1 - tp
        return remote(dx_sum.at[p - 2], dx_stage.at[r, p - 2], S_ROW_AWAY + 1, away_row_rs.at[2 + r], **device)

    def dx_row_all(r):
        return remote(dx_sum, dx_stage.at[r], S_ROW_AWAY + 1, away_row_rs.at[2 + r], dp=far)

    def finish_y(q):
        y_tp[q].wait()
        y_sum[2 * q:2 * q + 2] = (xc[tp, 2 * q:2 * q + 2].astype(F32) + (y_acc[q, tp] + y_peer[q])).astype(BF16)
        if q == 0:
            y_stage[OWN, 0] = y_sum[OWN]
            for p, r in home_rows:
                row_home(p, r).start()
        else:
            for p in (FAR, DIAG):
                y_away(p).start()

    def tail(h):
        return (remote(dx_home.at[h, 0], here_in.at[h], S_TAIL, tail_rs.at[h, 0], tp=1 - tp),
                remote(dx_home.at[h, 1], near_in.at[h, 1], S_TAIL + 1, tail_rs.at[h, 1], dp=sib, tp=1 - tp),
                remote(dx_home.at[h, 1], near_in.at[h, 0], S_TAIL + 2, tail_rs.at[h, 2], dp=sib))

    def finish_dx_home(h):
        for copy in tail(h):
            copy.wait_recv()
        dx_rows[h, :, cols(dp)] = (dyc[h, OWN].astype(F32) + (dx_home[h, 0] + here_in[h])).astype(BF16)
        dx_rows[h, :, cols(sib)] = (dy_own[h, :, cols(sib)].astype(F32) + (near_in[h, 0] + near_in[h, 1])).astype(BF16)

    remote(ab_give.at[1], ab_got.at[1], S_CORE_AB + 1, away_rs.at[0], dp=sib).wait()
    behind(form_hidden, away_y)
    y_tp[1].start()
    remote(g_give.at[1], g_got.at[1], S_CORE_G + 1, away_rs.at[1], dp=sib).wait()
    each(form_grads)
    finish_y(1)
    each(lambda g: grad_far(g, 1).start())

    def take_hidden(g):
        hid_far(g).wait_recv()
        hid_fwd(g).start()

    def home_y(g):
        hid_fwd(g).wait_recv()
        add_y(0, g)
        add_dx_away(g)

    remote(grad.at[:, :, FAR], grad.at[:, :, DIAG], S_GRAD_SIB, grad_sib_rs, dp=sib).wait()
    behind(take_hidden, home_y)
    y_tp[0].start()
    dx_tp.start()

    def take_grad(h):
        def body(g):
            grad_far(g, h).wait_recv()
            grad_fwd(g, h).start()
        return body

    def home_dx(h):
        def body(g):
            grad_fwd(g, h).wait_recv()
            add_dx_home(g, h)
        return body

    behind(take_grad(0), home_dx(0))
    for copy in tail(0):
        copy.start()
    finish_y(0)
    y_away_all().wait_recv()
    y_away_fwd().start()
    dx_tp.wait()
    dx_sum[...] = (dyc[tp, 2:4].astype(F32) + (dx_away[tp] + dx_peer[...])).astype(BF16)

    each_home = home_dx(1)

    def last_grads(g):
        take_grad(1)(g)

        @pl.when(g == groups - 1)
        def _():
            for p in (FAR, DIAG):
                for r in (1, 0):
                    dx_row(p, r).start()

    behind(last_grads, each_home)
    for copy in tail(1):
        copy.start()

    finish_dx_home(0)
    for p, r in home_rows:
        row_home(p, r).wait_recv()
    y_away_fwd().wait_recv()
    owner = {OWN: dp, SIB: sib, FAR: far, DIAG: diag}
    for p in range(SHARDS):
        y_rows[tp, :, cols(owner[p])] = y_stage[p, 0]
        y_rows[1 - tp, :, cols(owner[p])] = y_stage[p, 1]

    for i in (0, 1):
        slots = tokens[i][1]
        remote(slots.at[:, 0:2], slots.at[:, 0:2], S_TOK + i, tok_rs.at[i, 0], dp=sib).wait_send()
        token_fwd(i).wait_send()
    remote(ab_give.at[0], ab_got.at[0], S_CORE_AB, core_rs.at[0, 0], dp=sib).wait_send()
    remote(g_give.at[0], g_got.at[0], S_CORE_G, core_rs.at[0, 0], dp=sib).wait_send()
    remote(ab_keep.at[0], ab_recv, S_LINK_AB, link_rs.at[0, 0], dp=far).wait_send()
    remote(g_keep.at[0], g_recv, S_LINK_G, link_rs.at[0, 0], dp=far).wait_send()
    for kind in (S_HID_FAR, S_HID_SIB, S_HID_FWD):
        remote(hid.at[:, :, OWN], hid.at[:, :, SIB], kind, hid_rs.at[0, 0], dp=sib).wait_send()
    for kind in (S_GRAD_FAR, S_GRAD_FWD):
        remote(grad.at[:, :, OWN], grad.at[:, :, SIB], kind, grad_sib_rs, dp=sib).wait_send()
    remote(y_sum.at[0:3], y_sum.at[0:3], S_ROW_HOME, home_rs.at[0], dp=sib).wait_send()
    y_away_all().wait_send()
    y_away_fwd().wait_send()
    remote(dx_stage, dx_stage, S_ROW_AWAY + 1, away_row_rs.at[2], dp=far).wait_send()

    for r in (0, 1):
        dx_row_all(r).wait_recv()
    for p in (FAR, DIAG):
        dx_rows[tp, :, cols(owner[p])] = dx_stage[0, p - 2]
        dx_rows[1 - tp, :, cols(owner[p])] = dx_stage[1, p - 2]
    finish_dx_home(1)
    for k in range(3):
        remote(dx_home.at[:, 0], here_in, S_TAIL + k, tail_rs.at[0, 0], dp=sib).wait_send()


def gradient_kernel(x_t, dyc, hid, grad, y_rows, dx_rows, y_out, dx_out, dgate_out, dup_out, ddown_out,
                    dgate, dup, ddown, row_sem, tile_sem):
    groups = hid.shape[0]
    tokens = x_t.shape[1]
    width = dyc.shape[-1]
    per_group = GROUP // TILE
    rows_out = [pltpu.make_async_copy(y_rows, y_out, row_sem.at[0]), pltpu.make_async_copy(dx_rows, dx_out, row_sem.at[1])]

    def write(n, slot, k):
        at = pl.ds(pl.multiple_of(n * TILE, TILE), TILE)
        out = ddown_out.at[at] if k == 2 else (dgate_out, dup_out)[k].at[:, at]
        return pltpu.make_async_copy((dgate, dup, ddown)[k].at[slot], out, tile_sem.at[k, slot])

    def body(g, carry):
        for s in range(per_group):
            n = g * per_group + s
            slot = lax.rem(n, RING)

            def take(k):
                @pl.when(n >= RING)
                def _():
                    write(n - RING, slot, k).wait()

            at = slice(s * TILE, (s + 1) * TILE)
            for k, buf in enumerate((dgate, dup)):
                take(k)
                buf[slot] = _dot(x_t[...], grad[g, :, :, k, :, at].reshape(tokens, TILE), 1, 0)
                write(n, slot, k).start()
            take(2)
            ddown[slot] = _dot(hid[g, :, :, :, at].reshape(tokens, TILE), dyc[...].reshape(tokens, width), 0, 0)
            write(n, slot, 2).start()
        return carry

    for copy in rows_out:
        copy.start()
    lax.fori_loop(0, groups, body, 0)
    for n in range(groups * per_group - RING, groups * per_group):
        for k in range(3):
            write(n, n % RING, k).wait()
    for copy in rows_out:
        copy.wait()


def solution(mesh):
    def device_pass(x_rows, gate_blk, up_blk, down_blk, dy_rows):
        rows, model = x_rows.shape
        width, hidden = gate_blk.shape
        chunks, groups = hidden // CHUNK, hidden // GROUP
        half = rows // 2
        tokens = SHARDS * rows
        hbm = pl.BlockSpec(memory_space=pl.ANY)
        vmem = pl.BlockSpec(memory_space=pltpu.VMEM)
        sds = jax.ShapeDtypeStruct
        dma = pltpu.SemaphoreType.DMA
        tok = (2, SHARDS, half, width)
        block = (2, half, width)
        own = (2, half, model)
        x_t, dyc, hid, grad, y_own, dx_own = pl.pallas_call(
            exchange_kernel,
            name='exchange',
            out_shape=(sds((width, tokens), BF16), sds(tok, BF16), sds((groups, 2, SHARDS, half, GROUP), BF16),
                       sds((groups, 2, SHARDS, 2, half, GROUP), BF16), sds(own, BF16), sds(own, BF16)),
            in_specs=[vmem, hbm, hbm, hbm],
            out_specs=[vmem] * 6,
            scratch_shapes=[
                pltpu.VMEM(tok, BF16),
                pltpu.VMEM((groups, 2, 2, width, CHUNK), BF16), pltpu.VMEM((groups, GROUP, width), BF16),
                pltpu.VMEM((2, chunks, 2, 2, half, CHUNK), F32), pltpu.VMEM((2, chunks, 2, 2, half, CHUNK), F32),
                pltpu.VMEM((2, chunks, 2, 2, half, CHUNK), F32),
                pltpu.VMEM((2, chunks, 2, half, CHUNK), F32), pltpu.VMEM((2, chunks, 2, half, CHUNK), F32),
                pltpu.VMEM((2, chunks, 2, half, CHUNK), F32),
                pltpu.VMEM((chunks, 2, 2, half, CHUNK), F32), pltpu.VMEM((chunks, 2, half, CHUNK), F32),
                pltpu.VMEM((2, 2) + block, F32), pltpu.VMEM((2,) + block, F32), pltpu.VMEM((2,) + block, F32),
                pltpu.VMEM((2,) + block, F32), pltpu.VMEM(block, F32),
                pltpu.VMEM((SHARDS, half, width), BF16), pltpu.VMEM(block, BF16),
                pltpu.VMEM((SHARDS, 2, half, width), BF16), pltpu.VMEM((2,) + block, BF16),
                pltpu.VMEM(block, F32), pltpu.VMEM((2,) + block, F32),
                dma((SENDS,)), dma((chunks,)), dma((groups,)), dma((2, 3)), dma((3, chunks)), dma((2,)),
                dma((3, chunks)), dma((3, groups)), dma((2, 2, groups)), dma(()), dma((3,)), dma((3,)), dma((4,)), dma((2, 3)),
            ],
            compiler_params=pltpu.CompilerParams(collective_id=0, has_side_effects=True,
                                                 vmem_limit_bytes=44 * 1024 * 1024),
        )(jnp.concatenate([x_rows, dy_rows]).reshape((2,) + own), gate_blk, up_blk, down_blk)

        y_new, dx_new, dw_gate, dw_up, dw_down = pl.pallas_call(
            gradient_kernel,
            name='gradients',
            out_shape=(sds(own, BF16), sds(own, BF16), sds((width, hidden), F32), sds((width, hidden), F32),
                       sds((hidden, width), F32)),
            in_specs=[vmem] * 6,
            out_specs=[hbm] * 5,
            scratch_shapes=[pltpu.VMEM((RING, width, TILE), F32), pltpu.VMEM((RING, width, TILE), F32),
                            pltpu.VMEM((RING, TILE, width), F32), dma((2,)), dma((3, RING))],
            compiler_params=pltpu.CompilerParams(vmem_limit_bytes=44 * 1024 * 1024),
        )(x_t, dyc, hid, grad, y_own, dx_own)
        return y_new.reshape(rows, model), dx_new.reshape(rows, model), dw_gate, dw_up, dw_down

    row_spec = P('dp', None)
    weight_spec = P('dp', 'tp')
    down_spec = P('tp', 'dp')
    return jax.shard_map(device_pass, mesh=mesh,
                         in_specs=(row_spec, weight_spec, weight_spec, down_spec, row_spec),
                         out_specs=(row_spec, row_spec, weight_spec, weight_spec, down_spec),
                         check_vma=False)
```

```python
import jax
import jax.numpy as jnp
from jax import lax
from jax.experimental import pallas as pl
from jax.experimental.pallas import tpu as pltpu
from jax.sharding import PartitionSpec as P

MESH = pl.DeviceIdType.MESH
F32 = jnp.float32
BF16 = jnp.bfloat16
SHARDS = 4
CHUNK = 512
GROUP = 2 * CHUNK
TILE = 512
RING = 3
OWN, SIB, FAR, DIAG = 0, 1, 2, 3
(S_TOK, S_TOK_FWD, S_CORE_AB, S_CORE_G, S_LINK_AB, S_LINK_G, S_HID_FAR, S_HID_SIB, S_HID_FWD, S_GRAD_FAR, S_GRAD_SIB,
 S_GRAD_FWD, S_TP, S_ROW_HOME, S_ROW_AWAY, S_ROW_FWD, S_TAIL) = (0, 2, 4, 6, 8, 9, 10, 11, 12, 13, 14, 15, 16, 19, 20, 22, 23)
SENDS = 27


def _dot(lhs, rhs, lhs_dim, rhs_dim):
    return lax.dot_general(lhs, rhs, (((lhs_dim,), (rhs_dim,)), ((), ())), preferred_element_type=F32)


def exchange_kernel(token_rows, gate_hbm, up_hbm, down_hbm,
                    x_t, dyc, hid, grad, y_rows, dx_first, dx_half,
                    xc, gate_up, down,
                    ab_keep, ab_give, ab_got, g_keep, g_give, g_got, ab_recv, g_recv,
                    y_acc, dx_away, dx_home, y_peer, dx_peer, y_sum, dx_sum, y_stage, dx_stage, here_in, near_in,
                    send, gate_up_sem, down_sem, tok_rs, core_rs, away_rs, link_rs,
                    hid_rs, grad_rs, grad_sib_rs, tp_rs, home_rs, away_row_rs, tail_rs):
    tp = lax.axis_index('tp')
    dp = lax.axis_index('dp')
    sib = dp + 1 - 2 * lax.rem(dp, 2)
    far = lax.rem(dp + 2, SHARDS)
    diag = lax.rem(sib + 2, SHARDS)
    peers = {SIB: sib, FAR: far, DIAG: diag}
    half, width = xc.shape[-2:]
    groups = hid.shape[0]

    def remote(src, dst, ss, rs, **device):
        return pltpu.make_async_remote_copy(src_ref=src, dst_ref=dst, send_sem=send.at[ss], recv_sem=rs,
                                            device_id=device, device_id_type=MESH)

    def cols(i):
        return pl.ds(pl.multiple_of(i * width, width), width)

    def chunk_of(g, s):
        return pl.ds(pl.multiple_of(g * GROUP, GROUP) + s * CHUNK, CHUNK)

    def load_gate_up(g, s):
        sem = gate_up_sem.at[2 * g + s]
        return (pltpu.make_async_copy(gate_hbm.at[:, chunk_of(g, s)], gate_up.at[g, s, 0], sem),
                pltpu.make_async_copy(up_hbm.at[:, chunk_of(g, s)], gate_up.at[g, s, 1], sem))

    def load_down(g):
        return pltpu.make_async_copy(down_hbm.at[pl.ds(pl.multiple_of(g * GROUP, GROUP), GROUP)], down.at[g], down_sem.at[g])

    tokens = ((token_rows.at[0], xc), (token_rows.at[1], dyc))
    dy_own = token_rows.at[1]
    barrier = pltpu.get_barrier_semaphore()
    for p in (FAR, SIB, DIAG):
        pl.semaphore_signal(barrier, inc=1, device_id={'dp': peers[p]}, device_id_type=MESH)
        pl.semaphore_signal(barrier, inc=1, device_id={'dp': peers[p], 'tp': 1 - tp}, device_id_type=MESH)
    pl.semaphore_signal(barrier, inc=1, device_id={'tp': 1 - tp}, device_id_type=MESH)
    for g in range(groups):
        for s in (0, 1):
            for copy in load_gate_up(g, s):
                copy.start()
    for g in range(groups):
        load_down(g).start()
    for own, slots in tokens:
        slots[:, OWN] = own[:, :, cols(dp)]
    pl.semaphore_wait(barrier, 2 * SHARDS - 1)

    def token(p, i):
        own, slots = tokens[i]
        if p == SIB:
            return remote(own.at[:, :, cols(sib)], slots.at[:, SIB], S_TOK + i, tok_rs.at[i, 0], dp=sib)
        return remote(own.at[tp, :, cols(peers[p])], slots.at[tp, p], S_TOK + i, tok_rs.at[i, 1], dp=peers[p])

    def token_fwd(i):
        part = tokens[i][1].at[tp, 2:4]
        return remote(part, part, S_TOK_FWD + i, tok_rs.at[i, 2], tp=1 - tp)

    def tokens_far(i):
        part = tokens[i][1].at[tp, 2:4]
        return remote(part, part, S_TOK + i, tok_rs.at[i, 1], dp=far)

    for i in (0, 1):
        for p in (SIB, FAR, DIAG):
            token(p, i).start()

    def core_ab(q, c, i):
        rs = core_rs.at[0, lax.rem(2 * c + i, 4)] if q == 0 else away_rs.at[0]
        return remote(ab_give.at[q, c, i], ab_got.at[q, c, i], S_CORE_AB + q, rs, dp=sib)

    def core_g(q, c):
        rs = core_rs.at[1, lax.rem(c, 4)] if q == 0 else away_rs.at[1]
        return remote(g_give.at[q, c], g_got.at[q, c], S_CORE_G + q, rs, dp=sib)

    def link_ab(c, i):
        return remote(ab_keep.at[0, c, i], ab_recv.at[c, i], S_LINK_AB, link_rs.at[0, c // 2], dp=far)

    def link_g(c):
        return remote(g_keep.at[0, c], g_recv.at[c], S_LINK_G, link_rs.at[1, c // 2], dp=far)

    def send_ab(c, i):
        core_ab(0, c, i).wait_recv()
        ab_keep[0, c, i] += ab_got[0, c, i]
        link_ab(c, i).start()

    def send_g(c):
        core_g(0, c).wait_recv()
        g_keep[0, c] += g_got[0, c]
        link_g(c).start()

    def pair_rows(slots, q):
        return slots[:, 2 * q:2 * q + 2].reshape(4 * half, slots.shape[-1])

    def split(part):
        part = part.reshape(2, 2, half, part.shape[-1])
        return part[:, 0], part[:, 1]

    def part_ab(q, g, s, i):
        c = 2 * g + s
        if q == 0 and i == 0:
            pltpu.make_async_copy(gate_up.at[g, s], gate_up.at[g, s], gate_up_sem.at[c]).wait()
        ab_keep[q, c, i], ab_give[q, c, i] = split(_dot(pair_rows(xc, q), gate_up[g, s, i], 1, 0))
        core_ab(q, c, i).start()

    def part_g(q, g, s):
        c = 2 * g + s
        if q == 0 and s == 0:
            load_down(g).wait()
        g_keep[q, c], g_give[q, c] = split(_dot(pair_rows(dyc, q), down[g, s * CHUNK:(s + 1) * CHUNK], 1, 1))
        core_g(q, c).start()

    def each(body):
        lax.fori_loop(0, groups, lambda g, carry: (body(g), carry)[1], 0)

    def behind(first, second):
        def body(g):
            first(g)

            @pl.when(g > 0)
            def _():
                second(g - 1)

        each(body)
        second(groups - 1)

    def home_parts(part, send_on, kinds):
        steps = [(s,) + kind for s in (0, 1) for kind in kinds]

        def body(g):
            for n, (s, *kind) in enumerate(steps):
                part(0, g, s, *kind)
                before_s, *before = steps[n - 1]
                if n == 0:
                    pl.when(g > 0)(lambda: send_on(2 * g - 1, *before))
                else:
                    send_on(2 * g + before_s, *before)

        each(body)
        send_on(2 * groups - 1, *kinds[-1])

    token(SIB, 0).wait_recv()
    home_parts(part_ab, send_ab, ((0,), (1,)))
    for i in (0, 1):
        tokens_far(i).wait_recv()
        token_fwd(i).start()
    token(SIB, 1).wait_recv()
    home_parts(part_g, send_g, ((),))
    token_fwd(0).wait_recv()
    each(lambda g: [part_ab(1, g, s, i) for s in (0, 1) for i in (0, 1)])
    token_fwd(1).wait_recv()
    each(lambda g: [part_g(1, g, s) for s in (0, 1)])
    x_t[...] = xc[...].reshape(2 * SHARDS * half, width).T

    def hid_far(g):
        return remote(hid.at[g, :, FAR], hid.at[g, :, OWN], S_HID_FAR, hid_rs.at[0, g], dp=far)

    def hid_sib(g):
        return remote(hid.at[g, :, FAR], hid.at[g, :, DIAG], S_HID_SIB, hid_rs.at[1, g], dp=sib)

    def hid_fwd(g):
        return remote(hid.at[g, :, OWN], hid.at[g, :, SIB], S_HID_FWD, hid_rs.at[2, g], dp=sib)

    def grad_far(g, h):
        return remote(grad.at[g, h, FAR], grad.at[g, h, OWN], S_GRAD_FAR, grad_rs.at[0, h, g], dp=far)

    def grad_sib(g):
        return remote(grad.at[g, :, FAR], grad.at[g, :, DIAG], S_GRAD_SIB, grad_sib_rs, dp=sib)

    def grad_fwd(g, h):
        return remote(grad.at[g, h, OWN], grad.at[g, h, SIB], S_GRAD_FWD, grad_rs.at[1, h, g], dp=sib)

    y_acc[...] = jnp.zeros_like(y_acc)
    dx_away[...] = jnp.zeros_like(dx_away)
    dx_home[...] = jnp.zeros_like(dx_home)

    def add_y(q, g):
        part = _dot(hid[g, :, 2 * q:2 * q + 2].reshape(4 * half, GROUP), down[g], 1, 0)
        y_acc[q] += part.reshape(y_acc.shape[1:])

    def dx_part(take, count, g):
        part = None
        for s in (0, 1):
            for i in (0, 1):
                lhs = take(i, s * CHUNK).reshape(count, CHUNK)
                term = _dot(lhs, gate_up[g, s, i], 1, 1)
                part = term if part is None else part + term
        return part

    def add_dx_away(g):
        part = dx_part(lambda i, at: grad[g, :, 2:4, i, :, at:at + CHUNK], 4 * half, g)
        dx_away[...] += part.reshape(dx_away.shape)

    def add_dx_home(g, h):
        part = dx_part(lambda i, at: grad[g, h, 0:2, i, :, at:at + CHUNK], 2 * half, g)
        dx_home[h] += part.reshape(dx_home.shape[1:])

    def form_hidden(g):
        both = pl.ds(2 * g, 2)
        remote(ab_recv.at[both], ab_recv.at[both], S_LINK_AB, link_rs.at[0, g], dp=far).wait_recv()
        for s in (0, 1):
            c = 2 * g + s
            total = ab_keep[1, c] + ab_got[1, c] + ab_recv[c]
            ab_keep[1, c] = total
            a, b = total[0], total[1]
            hid[g, :, FAR, :, s * CHUNK:(s + 1) * CHUNK] = (a * jax.nn.sigmoid(a) * b).astype(BF16)
        hid_far(g).start()
        hid_sib(g).start()

    def away_y(g):
        hid_sib(g).wait_recv()
        add_y(1, g)

    def form_grads(g):
        both = pl.ds(2 * g, 2)
        remote(g_recv.at[both], g_recv.at[both], S_LINK_G, link_rs.at[1, g], dp=far).wait_recv()
        for s in (0, 1):
            c = 2 * g + s
            v = g_keep[1, c] + g_got[1, c] + g_recv[c]
            a, b = ab_keep[1, c, 0], ab_keep[1, c, 1]
            sig = jax.nn.sigmoid(a)
            grad[g, :, FAR, 0, :, s * CHUNK:(s + 1) * CHUNK] = (v * b * sig * (1.0 + a * (1.0 - sig))).astype(BF16)
            grad[g, :, FAR, 1, :, s * CHUNK:(s + 1) * CHUNK] = (v * (a * sig)).astype(BF16)
        grad_far(g, 0).start()
        grad_sib(g).start()

    def tp_copy(acc, peer, k):
        return remote(acc.at[1 - tp], peer, S_TP + k, tp_rs.at[k], tp=1 - tp)

    y_tp = [tp_copy(y_acc.at[q], y_peer.at[q], q) for q in (0, 1)]
    dx_tp = tp_copy(dx_away, dx_peer, 2)

    def row_home(p, r):
        device = {} if p == OWN else {'dp': sib}
        if r:
            device['tp'] = 1 - tp
        return remote(y_sum.at[p], y_stage.at[p, r], S_ROW_HOME, home_rs.at[2 if p == OWN else r], **device)

    home_rows = ((OWN, 1), (SIB, 0), (SIB, 1))

    def y_away(p):
        return remote(y_sum.at[p], y_stage.at[p, 0], S_ROW_AWAY, away_row_rs.at[0], dp=peers[p])

    def y_away_all():
        return remote(y_sum.at[2:4], y_stage.at[2:4, 0], S_ROW_AWAY, away_row_rs.at[0], dp=far)

    def y_away_fwd():
        return remote(y_stage.at[2:4, 0], y_stage.at[2:4, 1], S_ROW_FWD, away_row_rs.at[1], tp=1 - tp)

    def dx_row(p):
        return remote(dx_sum.at[p - 2], dx_stage.at[p - 2], S_ROW_AWAY + 1, away_row_rs.at[2], dp=peers[p])

    def dx_row_all():
        return remote(dx_sum, dx_stage, S_ROW_AWAY + 1, away_row_rs.at[2], dp=far)

    def finish_y(q):
        y_tp[q].wait()
        y_sum[2 * q:2 * q + 2] = (xc[tp, 2 * q:2 * q + 2].astype(F32) + (y_acc[q, tp] + y_peer[q])).astype(BF16)
        if q == 0:
            y_stage[OWN, 0] = y_sum[OWN]
            for p, r in home_rows:
                row_home(p, r).start()
        else:
            for p in (FAR, DIAG):
                y_away(p).start()

    def tail():
        return (remote(dx_home.at[0, 0], here_in, S_TAIL, tail_rs.at[0], tp=1 - tp),
                remote(dx_home.at[0, 1], near_in.at[1], S_TAIL + 1, tail_rs.at[1], dp=sib, tp=1 - tp),
                remote(dx_home.at[0, 1], near_in.at[0], S_TAIL + 2, tail_rs.at[2], dp=sib))

    def swap():
        return remote(dx_home.at[1, 1], dx_half.at[SIB], S_TAIL + 3, tail_rs.at[3], dp=sib)

    def finish_dx_first():
        for copy in tail():
            copy.wait()
        dx_first[0] = (dyc[0, OWN].astype(F32) + (dx_home[0, 0] + here_in[...])).astype(BF16)
        dx_first[1] = (dy_own[0, :, cols(sib)].astype(F32) + (near_in[0] + near_in[1])).astype(BF16)

    remote(ab_give.at[1], ab_got.at[1], S_CORE_AB + 1, away_rs.at[0], dp=sib).wait()
    behind(form_hidden, away_y)
    y_tp[1].start()
    remote(g_give.at[1], g_got.at[1], S_CORE_G + 1, away_rs.at[1], dp=sib).wait()
    each(form_grads)
    finish_y(1)
    each(lambda g: grad_far(g, 1).start())

    def take_hidden(g):
        hid_far(g).wait_recv()
        hid_fwd(g).start()

    def home_y(g):
        hid_fwd(g).wait_recv()
        add_y(0, g)
        add_dx_away(g)

    remote(grad.at[:, :, FAR], grad.at[:, :, DIAG], S_GRAD_SIB, grad_sib_rs, dp=sib).wait()
    behind(take_hidden, home_y)
    y_tp[0].start()
    dx_tp.start()

    def take_grad(h):
        def body(g):
            grad_far(g, h).wait_recv()
            grad_fwd(g, h).start()
        return body

    def home_dx(h):
        def body(g):
            grad_fwd(g, h).wait_recv()
            add_dx_home(g, h)
        return body

    behind(take_grad(0), home_dx(0))
    for copy in tail():
        copy.start()
    finish_y(0)
    y_away_all().wait_recv()
    y_away_fwd().start()
    dx_tp.wait()
    dx_sum[...] = (dyc[tp, 2:4].astype(F32) + (dx_away[tp] + dx_peer[...])).astype(BF16)

    each_home = home_dx(1)

    def last_grads(g):
        take_grad(1)(g)

        @pl.when(g == groups - 1)
        def _():
            for p in (FAR, DIAG):
                dx_row(p).start()

    behind(last_grads, each_home)
    swap().start()
    dx_half[OWN] = dx_home[1, 0]
    finish_dx_first()
    for p, r in home_rows:
        row_home(p, r).wait_recv()
    y_away_fwd().wait_recv()
    owner = {OWN: dp, SIB: sib, FAR: far, DIAG: diag}
    for p in range(SHARDS):
        y_rows[tp, :, cols(owner[p])] = y_stage[p, 0]
        y_rows[1 - tp, :, cols(owner[p])] = y_stage[p, 1]

    for i in (0, 1):
        slots = tokens[i][1]
        remote(slots.at[:, 0:2], slots.at[:, 0:2], S_TOK + i, tok_rs.at[i, 0], dp=sib).wait_send()
        token_fwd(i).wait_send()
    remote(ab_give.at[0], ab_got.at[0], S_CORE_AB, core_rs.at[0, 0], dp=sib).wait_send()
    remote(g_give.at[0], g_got.at[0], S_CORE_G, core_rs.at[0, 0], dp=sib).wait_send()
    remote(ab_keep.at[0], ab_recv, S_LINK_AB, link_rs.at[0, 0], dp=far).wait_send()
    remote(g_keep.at[0], g_recv, S_LINK_G, link_rs.at[0, 0], dp=far).wait_send()
    for kind in (S_HID_FAR, S_HID_SIB, S_HID_FWD):
        remote(hid.at[:, :, OWN], hid.at[:, :, SIB], kind, hid_rs.at[0, 0], dp=sib).wait_send()
    for kind in (S_GRAD_FAR, S_GRAD_FWD):
        remote(grad.at[:, :, OWN], grad.at[:, :, SIB], kind, grad_sib_rs, dp=sib).wait_send()
    remote(y_sum.at[0:3], y_sum.at[0:3], S_ROW_HOME, home_rs.at[0], dp=sib).wait_send()
    y_away_all().wait_send()
    y_away_fwd().wait_send()

    dx_row_all().wait()
    dx_half[2:4] = dx_stage[...].astype(F32)
    swap().wait()


def gradient_kernel(x_t, dyc, hid, grad, y_rows, y_out, dgate_out, dup_out, ddown_out,
                    dgate, dup, ddown, row_sem, tile_sem):
    groups = hid.shape[0]
    tokens = x_t.shape[1]
    width = dyc.shape[-1]
    per_group = GROUP // TILE
    rows_out = pltpu.make_async_copy(y_rows, y_out, row_sem)

    def write(n, slot, k):
        at = pl.ds(pl.multiple_of(n * TILE, TILE), TILE)
        out = ddown_out.at[at] if k == 2 else (dgate_out, dup_out)[k].at[:, at]
        return pltpu.make_async_copy((dgate, dup, ddown)[k].at[slot], out, tile_sem.at[k, slot])

    def body(g, carry):
        for s in range(per_group):
            n = g * per_group + s
            slot = lax.rem(n, RING)

            def take(k):
                @pl.when(n >= RING)
                def _():
                    write(n - RING, slot, k).wait()

            at = slice(s * TILE, (s + 1) * TILE)
            for k, buf in enumerate((dgate, dup)):
                take(k)
                buf[slot] = _dot(x_t[...], grad[g, :, :, k, :, at].reshape(tokens, TILE), 1, 0)
                write(n, slot, k).start()
            take(2)
            ddown[slot] = _dot(hid[g, :, :, :, at].reshape(tokens, TILE), dyc[...].reshape(tokens, width), 0, 0)
            write(n, slot, 2).start()
        return carry

    rows_out.start()
    lax.fori_loop(0, groups, body, 0)
    for n in range(groups * per_group - RING, groups * per_group):
        for k in range(3):
            write(n, n % RING, k).wait()
    rows_out.wait()


def place_kernel(token_rows, dx_first, mine, theirs, dx_out):
    tp = lax.axis_index('tp')
    dp = lax.axis_index('dp')
    sib = dp + 1 - 2 * lax.rem(dp, 2)
    width = mine.shape[-1]

    def cols(i):
        return pl.ds(pl.multiple_of(i * width, width), width)

    for p, owner in ((OWN, dp), (SIB, sib)):
        dx_out[0, :, cols(owner)] = dx_first[p]
        dx_out[1, :, cols(owner)] = (token_rows[1, 1, :, cols(owner)].astype(F32) + (mine[p] + theirs[p])).astype(BF16)
    for p, owner in ((FAR, lax.rem(dp + 2, SHARDS)), (DIAG, lax.rem(sib + 2, SHARDS))):
        dx_out[tp, :, cols(owner)] = mine[p].astype(BF16)
        dx_out[1 - tp, :, cols(owner)] = theirs[p].astype(BF16)


def solution(mesh):
    def device_pass(x_rows, gate_blk, up_blk, down_blk, dy_rows):
        rows, model = x_rows.shape
        width, hidden = gate_blk.shape
        chunks, groups = hidden // CHUNK, hidden // GROUP
        half = rows // 2
        tokens = SHARDS * rows
        hbm = pl.BlockSpec(memory_space=pl.ANY)
        vmem = pl.BlockSpec(memory_space=pltpu.VMEM)
        sds = jax.ShapeDtypeStruct
        dma = pltpu.SemaphoreType.DMA
        tok = (2, SHARDS, half, width)
        block = (2, half, width)
        own = (2, half, model)
        token_rows = jnp.concatenate([x_rows, dy_rows]).reshape((2,) + own)
        x_t, dyc, hid, grad, y_own, dx_first, dx_half = pl.pallas_call(
            exchange_kernel,
            name='exchange',
            out_shape=(sds((width, tokens), BF16), sds(tok, BF16), sds((groups, 2, SHARDS, half, GROUP), BF16),
                       sds((groups, 2, SHARDS, 2, half, GROUP), BF16), sds(own, BF16), sds(block, BF16),
                       sds((SHARDS, half, width), F32)),
            in_specs=[vmem, hbm, hbm, hbm],
            out_specs=[vmem] * 7,
            scratch_shapes=[
                pltpu.VMEM(tok, BF16),
                pltpu.VMEM((groups, 2, 2, width, CHUNK), BF16), pltpu.VMEM((groups, GROUP, width), BF16),
                pltpu.VMEM((2, chunks, 2, 2, half, CHUNK), F32), pltpu.VMEM((2, chunks, 2, 2, half, CHUNK), F32),
                pltpu.VMEM((2, chunks, 2, 2, half, CHUNK), F32),
                pltpu.VMEM((2, chunks, 2, half, CHUNK), F32), pltpu.VMEM((2, chunks, 2, half, CHUNK), F32),
                pltpu.VMEM((2, chunks, 2, half, CHUNK), F32),
                pltpu.VMEM((chunks, 2, 2, half, CHUNK), F32), pltpu.VMEM((chunks, 2, half, CHUNK), F32),
                pltpu.VMEM((2, 2) + block, F32), pltpu.VMEM((2,) + block, F32), pltpu.VMEM((2,) + block, F32),
                pltpu.VMEM((2,) + block, F32), pltpu.VMEM(block, F32),
                pltpu.VMEM((SHARDS, half, width), BF16), pltpu.VMEM(block, BF16),
                pltpu.VMEM((SHARDS, 2, half, width), BF16), pltpu.VMEM(block, BF16),
                pltpu.VMEM((half, width), F32), pltpu.VMEM(block, F32),
                dma((SENDS,)), dma((chunks,)), dma((groups,)), dma((2, 3)), dma((2, 4)), dma((2,)),
                dma((2, groups)), dma((3, groups)), dma((2, 2, groups)), dma(()), dma((3,)), dma((3,)), dma((3,)), dma((4,)),
            ],
            compiler_params=pltpu.CompilerParams(collective_id=0, has_side_effects=True,
                                                 vmem_limit_bytes=44 * 1024 * 1024),
        )(token_rows, gate_blk, up_blk, down_blk)
        dx_other = lax.ppermute(dx_half, 'tp', [(0, 1), (1, 0)])

        y_new, dw_gate, dw_up, dw_down = pl.pallas_call(
            gradient_kernel,
            name='gradients',
            out_shape=(sds(own, BF16), sds((width, hidden), F32), sds((width, hidden), F32), sds((hidden, width), F32)),
            in_specs=[vmem] * 5,
            out_specs=[hbm] * 4,
            scratch_shapes=[pltpu.VMEM((RING, width, TILE), F32), pltpu.VMEM((RING, width, TILE), F32),
                            pltpu.VMEM((RING, TILE, width), F32), dma(()), dma((3, RING))],
            cost_estimate=pl.CostEstimate(flops=6 * tokens * width * hidden, bytes_accessed=12 * width * hidden,
                                          transcendentals=0),
            compiler_params=pltpu.CompilerParams(vmem_limit_bytes=44 * 1024 * 1024),
        )(x_t, dyc, hid, grad, y_own)
        dx_new = pl.pallas_call(
            place_kernel,
            name='place_dx',
            out_shape=sds(own, BF16),
            in_specs=[vmem] * 4,
            out_specs=vmem,
            compiler_params=pltpu.CompilerParams(vmem_limit_bytes=4 * 1024 * 1024),
        )(token_rows, dx_first, dx_half, dx_other)
        return y_new.reshape(rows, model), dx_new.reshape(rows, model), dw_gate, dw_up, dw_down

    row_spec = P('dp', None)
    weight_spec = P('dp', 'tp')
    down_spec = P('tp', 'dp')
    return jax.shard_map(device_pass, mesh=mesh,
                         in_specs=(row_spec, weight_spec, weight_spec, down_spec, row_spec),
                         out_specs=(row_spec, row_spec, weight_spec, weight_spec, down_spec),
                         check_vma=False)
```

```python
import jax
import jax.numpy as jnp
from jax import lax
from jax.experimental import pallas as pl
from jax.experimental.pallas import tpu as pltpu
from jax.sharding import PartitionSpec as P

MESH = pl.DeviceIdType.MESH
F32 = jnp.float32
BF16 = jnp.bfloat16
SHARDS = 4
CHUNK = 512
GROUP = 2 * CHUNK
TILE = CHUNK
RING = 3
OWN, SIB, FAR, DIAG = 0, 1, 2, 3
(S_TOK, S_TOK_FWD, S_CORE_AB, S_CORE_G, S_LINK_AB, S_LINK_G, S_HID_FAR, S_HID_SIB, S_HID_FWD, S_GRAD_FAR, S_GRAD_SIB,
 S_GRAD_FWD, S_TP, S_ROW_HOME, S_ROW_AWAY, S_SWAP) = (0, 2, 4, 6, 8, 9, 10, 11, 12, 13, 14, 15, 16, 19, 20, 22)
SENDS = 23


def _dot(lhs, rhs, lhs_dim, rhs_dim):
    return lax.dot_general(lhs, rhs, (((lhs_dim,), (rhs_dim,)), ((), ())), preferred_element_type=F32)


def exchange_kernel(token_rows, gate_hbm, up_hbm, down_hbm,
                    x_t, dyc, hid, grad, y_home, half_rows,
                    xc, gate_up, down,
                    ab_keep, ab_give, ab_got, g_keep, g_give, g_got, ab_recv, g_recv,
                    y_acc, dx_away, dx_home, y_peer, dx_peer, y_sum, dx_sum, y_far, dx_far,
                    send, gate_up_sem, down_sem, tok_rs, core_rs, away_rs, link_rs,
                    hid_rs, grad_rs, grad_sib_rs, tp_rs, home_rs, away_row_rs, swap_rs):
    tp = lax.axis_index('tp')
    dp = lax.axis_index('dp')
    sib = dp + 1 - 2 * lax.rem(dp, 2)
    far = lax.rem(dp + 2, SHARDS)
    diag = lax.rem(sib + 2, SHARDS)
    peers = {SIB: sib, FAR: far, DIAG: diag}
    half, width = xc.shape[-2:]
    groups = hid.shape[0]

    def remote(src, dst, ss, rs, **device):
        return pltpu.make_async_remote_copy(src_ref=src, dst_ref=dst, send_sem=send.at[ss], recv_sem=rs,
                                            device_id=device, device_id_type=MESH)

    def cols(i):
        return pl.ds(pl.multiple_of(i * width, width), width)

    def chunk_of(g, s):
        return pl.ds(pl.multiple_of(g * GROUP, GROUP) + s * CHUNK, CHUNK)

    def load_gate_up(g, s):
        sem = gate_up_sem.at[2 * g + s]
        return (pltpu.make_async_copy(gate_hbm.at[:, chunk_of(g, s)], gate_up.at[g, s, 0], sem),
                pltpu.make_async_copy(up_hbm.at[:, chunk_of(g, s)], gate_up.at[g, s, 1], sem))

    def load_down(g):
        return pltpu.make_async_copy(down_hbm.at[pl.ds(pl.multiple_of(g * GROUP, GROUP), GROUP)], down.at[g], down_sem.at[g])

    tokens = ((token_rows.at[0], xc), (token_rows.at[1], dyc))
    dy_own = token_rows.at[1]
    barrier = pltpu.get_barrier_semaphore()
    for p in (FAR, SIB, DIAG):
        pl.semaphore_signal(barrier, inc=1, device_id={'dp': peers[p]}, device_id_type=MESH)
        pl.semaphore_signal(barrier, inc=1, device_id={'dp': peers[p], 'tp': 1 - tp}, device_id_type=MESH)
    pl.semaphore_signal(barrier, inc=1, device_id={'tp': 1 - tp}, device_id_type=MESH)
    for g in range(groups):
        for s in (0, 1):
            for copy in load_gate_up(g, s):
                copy.start()
    for g in range(groups):
        load_down(g).start()
    for own, slots in tokens:
        slots[:, OWN] = own[:, :, cols(dp)]
    pl.semaphore_wait(barrier, 2 * SHARDS - 1)

    def token(p, i):
        own, slots = tokens[i]
        if p == SIB:
            return remote(own.at[:, :, cols(sib)], slots.at[:, SIB], S_TOK + i, tok_rs.at[i, 0], dp=sib)
        return remote(own.at[tp, :, cols(peers[p])], slots.at[tp, p], S_TOK + i, tok_rs.at[i, 1], dp=peers[p])

    def token_fwd(i):
        part = tokens[i][1].at[tp, 2:4]
        return remote(part, part, S_TOK_FWD + i, tok_rs.at[i, 2], tp=1 - tp)

    def tokens_far(i):
        part = tokens[i][1].at[tp, 2:4]
        return remote(part, part, S_TOK + i, tok_rs.at[i, 1], dp=far)

    for i in (0, 1):
        for p in (SIB, FAR, DIAG):
            token(p, i).start()

    def core_ab(q, c, i):
        rs = core_rs.at[0, lax.rem(2 * c + i, 4)] if q == 0 else away_rs.at[0]
        return remote(ab_give.at[q, c, i], ab_got.at[q, c, i], S_CORE_AB + q, rs, dp=sib)

    def core_g(q, c):
        rs = core_rs.at[1, lax.rem(c, 4)] if q == 0 else away_rs.at[1]
        return remote(g_give.at[q, c], g_got.at[q, c], S_CORE_G + q, rs, dp=sib)

    def link_ab(c, i):
        return remote(ab_keep.at[0, c, i], ab_recv.at[c, i], S_LINK_AB, link_rs.at[0, c // 2], dp=far)

    def link_g(c):
        return remote(g_keep.at[0, c], g_recv.at[c], S_LINK_G, link_rs.at[1, c // 2], dp=far)

    def send_ab(c, i):
        core_ab(0, c, i).wait_recv()
        ab_keep[0, c, i] += ab_got[0, c, i]
        link_ab(c, i).start()

    def send_g(c):
        core_g(0, c).wait_recv()
        g_keep[0, c] += g_got[0, c]
        link_g(c).start()

    def pair_rows(slots, q):
        return slots[:, 2 * q:2 * q + 2].reshape(4 * half, slots.shape[-1])

    def split(part):
        part = part.reshape(2, 2, half, part.shape[-1])
        return part[:, 0], part[:, 1]

    def part_ab(q, g, s, i):
        c = 2 * g + s
        if q == 0 and i == 0:
            pltpu.make_async_copy(gate_up.at[g, s], gate_up.at[g, s], gate_up_sem.at[c]).wait()
        ab_keep[q, c, i], ab_give[q, c, i] = split(_dot(pair_rows(xc, q), gate_up[g, s, i], 1, 0))
        core_ab(q, c, i).start()

    def part_g(q, g, s):
        c = 2 * g + s
        if q == 0 and s == 0:
            load_down(g).wait()
        g_keep[q, c], g_give[q, c] = split(_dot(pair_rows(dyc, q), down[g, s * CHUNK:(s + 1) * CHUNK], 1, 1))
        core_g(q, c).start()

    def each(body):
        lax.fori_loop(0, groups, lambda g, carry: (body(g), carry)[1], 0)

    def behind(first, second):
        def body(g):
            first(g)

            @pl.when(g > 0)
            def _():
                second(g - 1)

        each(body)
        second(groups - 1)

    def home_parts(part, send_on, kinds):
        steps = [(s,) + kind for s in (0, 1) for kind in kinds]

        def body(g):
            for n, (s, *kind) in enumerate(steps):
                part(0, g, s, *kind)
                before_s, *before = steps[n - 1]
                if n == 0:
                    pl.when(g > 0)(lambda: send_on(2 * g - 1, *before))
                else:
                    send_on(2 * g + before_s, *before)

        each(body)
        send_on(2 * groups - 1, *kinds[-1])

    token(SIB, 0).wait_recv()
    home_parts(part_ab, send_ab, ((0,), (1,)))
    for i in (0, 1):
        tokens_far(i).wait_recv()
        token_fwd(i).start()
    token(SIB, 1).wait_recv()
    home_parts(part_g, send_g, ((),))
    token_fwd(0).wait_recv()
    each(lambda g: [part_ab(1, g, s, i) for s in (0, 1) for i in (0, 1)])
    token_fwd(1).wait_recv()
    each(lambda g: [part_g(1, g, s) for s in (0, 1)])
    x_t[...] = xc[...].reshape(2 * SHARDS * half, width).T

    def hid_far(g):
        return remote(hid.at[g, :, FAR], hid.at[g, :, OWN], S_HID_FAR, hid_rs.at[0, g], dp=far)

    def hid_sib(g):
        return remote(hid.at[g, :, FAR], hid.at[g, :, DIAG], S_HID_SIB, hid_rs.at[1, g], dp=sib)

    def hid_fwd(g):
        return remote(hid.at[g, :, OWN], hid.at[g, :, SIB], S_HID_FWD, hid_rs.at[2, g], dp=sib)

    def grad_far(c):
        return remote(grad.at[c, :, FAR], grad.at[c, :, OWN], S_GRAD_FAR, grad_rs.at[0, c], dp=far)

    def grad_sib(c):
        return remote(grad.at[c, :, FAR], grad.at[c, :, DIAG], S_GRAD_SIB, grad_sib_rs, dp=sib)

    def grad_fwd(c):
        return remote(grad.at[c, :, OWN], grad.at[c, :, SIB], S_GRAD_FWD, grad_rs.at[1, c], dp=sib)

    y_acc[...] = jnp.zeros_like(y_acc)
    dx_away[...] = jnp.zeros_like(dx_away)
    dx_home[...] = jnp.zeros_like(dx_home)

    def add_y(q, g):
        part = _dot(hid[g, :, 2 * q:2 * q + 2].reshape(4 * half, GROUP), down[g], 1, 0)
        y_acc[q] += part.reshape(y_acc.shape[1:])

    def add_dx(acc, q, g, s):
        part = None
        for i in (0, 1):
            lhs = grad[2 * g + s, :, 2 * q:2 * q + 2, i].reshape(4 * half, CHUNK)
            term = _dot(lhs, gate_up[g, s, i], 1, 1)
            part = term if part is None else part + term
        acc[...] += part.reshape(acc.shape)

    def form_hidden(g):
        both = pl.ds(2 * g, 2)
        remote(ab_recv.at[both], ab_recv.at[both], S_LINK_AB, link_rs.at[0, g], dp=far).wait_recv()
        for s in (0, 1):
            c = 2 * g + s
            total = ab_keep[1, c] + ab_got[1, c] + ab_recv[c]
            ab_keep[1, c] = total
            a, b = total[0], total[1]
            hid[g, :, FAR, :, s * CHUNK:(s + 1) * CHUNK] = (a * jax.nn.sigmoid(a) * b).astype(BF16)
        hid_far(g).start()
        hid_sib(g).start()

    def away_y(g):
        hid_sib(g).wait_recv()
        add_y(1, g)

    def form_grads(g):
        both = pl.ds(2 * g, 2)
        remote(g_recv.at[both], g_recv.at[both], S_LINK_G, link_rs.at[1, g], dp=far).wait_recv()
        for s in (0, 1):
            c = 2 * g + s
            v = g_keep[1, c] + g_got[1, c] + g_recv[c]
            a, b = ab_keep[1, c, 0], ab_keep[1, c, 1]
            sig = jax.nn.sigmoid(a)
            grad[c, :, FAR, 0] = (v * b * sig * (1.0 + a * (1.0 - sig))).astype(BF16)
            grad[c, :, FAR, 1] = (v * (a * sig)).astype(BF16)
            grad_far(c).start()
            grad_sib(c).start()

    def tp_copy(acc, peer, k):
        return remote(acc.at[1 - tp], peer, S_TP + k, tp_rs.at[k], tp=1 - tp)

    y_tp = [tp_copy(y_acc.at[q], y_peer.at[q], q) for q in (0, 1)]
    dx_tp = tp_copy(dx_away, dx_peer, 2)

    def row_home(p, r):
        device = {} if p == OWN else {'dp': sib}
        if r:
            device['tp'] = 1 - tp
        return remote(y_sum.at[p], y_home.at[p, r], S_ROW_HOME, home_rs.at[2 if p == OWN else r], **device)

    home_rows = ((OWN, 1), (SIB, 0), (SIB, 1))

    def far_row(i, p):
        total = y_sum.at[p] if i == 0 else dx_sum.at[p - 2]
        return remote(total, (y_far, dx_far)[i].at[p - 2], S_ROW_AWAY + i, away_row_rs.at[i], dp=peers[p])

    def far_rows(i):
        rows_in = (y_far, dx_far)[i]
        return remote(rows_in, rows_in, S_ROW_AWAY + i, away_row_rs.at[i], dp=far)

    def finish_y(q):
        y_tp[q].wait()
        y_sum[2 * q:2 * q + 2] = (xc[tp, 2 * q:2 * q + 2].astype(F32) + (y_acc[q, tp] + y_peer[q])).astype(BF16)
        if q == 0:
            y_home[OWN, 0] = y_sum[OWN]
            for p, r in home_rows:
                row_home(p, r).start()

    def swap():
        return remote(dx_home.at[:, 1], half_rows.at[2:4], S_SWAP, swap_rs, dp=sib)

    remote(ab_give.at[1], ab_got.at[1], S_CORE_AB + 1, away_rs.at[0], dp=sib).wait()
    behind(form_hidden, away_y)
    y_tp[1].start()
    remote(g_give.at[1], g_got.at[1], S_CORE_G + 1, away_rs.at[1], dp=sib).wait()
    each(form_grads)
    finish_y(1)

    def take_hidden(g):
        hid_far(g).wait_recv()
        hid_fwd(g).start()

    def home_y(g):
        hid_fwd(g).wait_recv()
        add_y(0, g)
        for s in (0, 1):
            add_dx(dx_away, 1, g, s)

    remote(grad.at[:, :, FAR], grad.at[:, :, DIAG], S_GRAD_SIB, grad_sib_rs, dp=sib).wait()
    behind(take_hidden, home_y)
    y_tp[0].start()
    dx_tp.start()

    def take_grad(c):
        grad_far(c).wait_recv()
        grad_fwd(c).start()

    def home_dx(g, s):
        grad_fwd(2 * g + s).wait_recv()
        add_dx(dx_home, 0, g, s)

    def take_grads(g):
        take_grad(2 * g)

        @pl.when(g > 0)
        def _():
            home_dx(g - 1, 1)

        @pl.when(g == 2)
        def _():
            dx_tp.wait()
            dx_sum[...] = (dyc[tp, 2:4].astype(F32) + (dx_away[tp] + dx_peer[...])).astype(BF16)
            for i in (0, 1):
                for p in (FAR, DIAG):
                    far_row(i, p).start()
            finish_y(0)

        take_grad(2 * g + 1)
        home_dx(g, 0)

    each(take_grads)
    home_dx(groups - 1, 1)
    swap().start()
    half_rows[0:2] = dx_home[:, 0]
    for p, r in home_rows:
        row_home(p, r).wait_recv()

    for i in (0, 1):
        slots = tokens[i][1]
        remote(slots.at[:, 0:2], slots.at[:, 0:2], S_TOK + i, tok_rs.at[i, 0], dp=sib).wait_send()
        token_fwd(i).wait_send()
    remote(ab_give.at[0], ab_got.at[0], S_CORE_AB, core_rs.at[0, 0], dp=sib).wait_send()
    remote(g_give.at[0], g_got.at[0], S_CORE_G, core_rs.at[0, 0], dp=sib).wait_send()
    remote(ab_keep.at[0], ab_recv, S_LINK_AB, link_rs.at[0, 0], dp=far).wait_send()
    remote(g_keep.at[0], g_recv, S_LINK_G, link_rs.at[0, 0], dp=far).wait_send()
    for kind in (S_HID_FAR, S_HID_SIB, S_HID_FWD):
        remote(hid.at[:, :, OWN], hid.at[:, :, SIB], kind, hid_rs.at[0, 0], dp=sib).wait_send()
    for kind in (S_GRAD_FAR, S_GRAD_FWD):
        remote(grad.at[:, :, OWN], grad.at[:, :, SIB], kind, grad_sib_rs, dp=sib).wait_send()
    remote(y_sum.at[0:3], y_sum.at[0:3], S_ROW_HOME, home_rs.at[0], dp=sib).wait_send()

    for i, rows_in in enumerate((y_far, dx_far)):
        far_rows(i).wait()
        half_rows[4 + 2 * i:6 + 2 * i] = rows_in[...].astype(F32)
    swap().wait()


def gradient_kernel(x_t, dyc, hid, grad, dgate_out, dup_out, ddown_out, dgate, dup, ddown, tile_sem):
    groups = hid.shape[0]
    tokens = x_t.shape[1]
    width = dyc.shape[-1]
    per_group = GROUP // TILE

    def write(n, slot, k):
        at = pl.ds(pl.multiple_of(n * TILE, TILE), TILE)
        out = ddown_out.at[at] if k == 2 else (dgate_out, dup_out)[k].at[:, at]
        return pltpu.make_async_copy((dgate, dup, ddown)[k].at[slot], out, tile_sem.at[k, slot])

    def body(g, carry):
        for s in range(per_group):
            n = g * per_group + s
            slot = lax.rem(n, RING)

            def take(k):
                @pl.when(n >= RING)
                def _():
                    write(n - RING, slot, k).wait()

            at = slice(s * TILE, (s + 1) * TILE)
            for k, buf in enumerate((dgate, dup)):
                take(k)
                buf[slot] = _dot(x_t[...], grad[n, :, :, k].reshape(tokens, TILE), 1, 0)
                write(n, slot, k).start()
            take(2)
            ddown[slot] = _dot(hid[g, :, :, :, at].reshape(tokens, TILE), dyc[...].reshape(tokens, width), 0, 0)
            write(n, slot, 2).start()
        return carry

    lax.fori_loop(0, groups, body, 0)
    for n in range(groups * per_group - RING, groups * per_group):
        for k in range(3):
            write(n, n % RING, k).wait()


def place_kernel(token_rows, y_home, mine, theirs, y_out, dx_out):
    tp = lax.axis_index('tp')
    dp = lax.axis_index('dp')
    sib = dp + 1 - 2 * lax.rem(dp, 2)
    width = mine.shape[-1]

    def cols(i):
        return pl.ds(pl.multiple_of(i * width, width), width)

    for p, owner in ((OWN, dp), (SIB, sib)):
        y_out[tp, :, cols(owner)] = y_home[p, 0]
        y_out[1 - tp, :, cols(owner)] = y_home[p, 1]
        at = pl.ds(2 * p, 2)
        dx_out[:, :, cols(owner)] = (token_rows[1, :, :, cols(owner)].astype(F32) + (mine[at] + theirs[at])).astype(BF16)
    for p, owner in ((FAR, lax.rem(dp + 2, SHARDS)), (DIAG, lax.rem(sib + 2, SHARDS))):
        for out, at in ((y_out, p + 2), (dx_out, p + 4)):
            out[tp, :, cols(owner)] = mine[at].astype(BF16)
            out[1 - tp, :, cols(owner)] = theirs[at].astype(BF16)


def solution(mesh):
    def device_pass(x_rows, gate_blk, up_blk, down_blk, dy_rows):
        rows, model = x_rows.shape
        width, hidden = gate_blk.shape
        chunks, groups = hidden // CHUNK, hidden // GROUP
        half = rows // 2
        tokens = SHARDS * rows
        hbm = pl.BlockSpec(memory_space=pl.ANY)
        vmem = pl.BlockSpec(memory_space=pltpu.VMEM)
        sds = jax.ShapeDtypeStruct
        dma = pltpu.SemaphoreType.DMA
        tok = (2, SHARDS, half, width)
        block = (2, half, width)
        own = (2, half, model)
        token_rows = jnp.concatenate([x_rows, dy_rows]).reshape((2,) + own)
        x_t, dyc, hid, grad, y_home, half_rows = pl.pallas_call(
            exchange_kernel,
            name='exchange',
            out_shape=(sds((width, tokens), BF16), sds(tok, BF16), sds((groups, 2, SHARDS, half, GROUP), BF16),
                       sds((chunks, 2, SHARDS, 2, half, CHUNK), BF16), sds((2,) + block, BF16),
                       sds((8, half, width), F32)),
            in_specs=[vmem, hbm, hbm, hbm],
            out_specs=[vmem] * 6,
            scratch_shapes=[
                pltpu.VMEM(tok, BF16),
                pltpu.VMEM((groups, 2, 2, width, CHUNK), BF16), pltpu.VMEM((groups, GROUP, width), BF16),
                pltpu.VMEM((2, chunks, 2, 2, half, CHUNK), F32), pltpu.VMEM((2, chunks, 2, 2, half, CHUNK), F32),
                pltpu.VMEM((2, chunks, 2, 2, half, CHUNK), F32),
                pltpu.VMEM((2, chunks, 2, half, CHUNK), F32), pltpu.VMEM((2, chunks, 2, half, CHUNK), F32),
                pltpu.VMEM((2, chunks, 2, half, CHUNK), F32),
                pltpu.VMEM((chunks, 2, 2, half, CHUNK), F32), pltpu.VMEM((chunks, 2, half, CHUNK), F32),
                pltpu.VMEM((2, 2) + block, F32), pltpu.VMEM((2,) + block, F32), pltpu.VMEM((2,) + block, F32),
                pltpu.VMEM((2,) + block, F32), pltpu.VMEM(block, F32),
                pltpu.VMEM((SHARDS, half, width), BF16), pltpu.VMEM(block, BF16),
                pltpu.VMEM(block, BF16), pltpu.VMEM(block, BF16),
                dma((SENDS,)), dma((chunks,)), dma((groups,)), dma((2, 3)), dma((2, 4)), dma((2,)),
                dma((2, groups)), dma((3, groups)), dma((2, chunks)), dma(()), dma((3,)), dma((3,)), dma((2,)), dma(()),
            ],
            compiler_params=pltpu.CompilerParams(collective_id=0, has_side_effects=True,
                                                 vmem_limit_bytes=44 * 1024 * 1024),
        )(token_rows, gate_blk, up_blk, down_blk)
        other_rows = lax.ppermute(half_rows, 'tp', [(0, 1), (1, 0)])

        dw_gate, dw_up, dw_down = pl.pallas_call(
            gradient_kernel,
            name='gradients',
            out_shape=(sds((width, hidden), F32), sds((width, hidden), F32), sds((hidden, width), F32)),
            in_specs=[vmem] * 4,
            out_specs=[hbm] * 3,
            scratch_shapes=[pltpu.VMEM((RING, width, TILE), F32), pltpu.VMEM((RING, width, TILE), F32),
                            pltpu.VMEM((RING, TILE, width), F32), dma((3, RING))],
            cost_estimate=pl.CostEstimate(flops=6 * tokens * width * hidden, bytes_accessed=12 * width * hidden,
                                          transcendentals=0),
            compiler_params=pltpu.CompilerParams(vmem_limit_bytes=44 * 1024 * 1024),
        )(x_t, dyc, hid, grad)
        y_new, dx_new = pl.pallas_call(
            place_kernel,
            name='place_rows',
            out_shape=(sds(own, BF16), sds(own, BF16)),
            in_specs=[vmem] * 4,
            out_specs=[vmem] * 2,
            compiler_params=pltpu.CompilerParams(vmem_limit_bytes=4 * 1024 * 1024),
        )(token_rows, y_home, half_rows, other_rows)
        return y_new.reshape(rows, model), dx_new.reshape(rows, model), dw_gate, dw_up, dw_down

    row_spec = P('dp', None)
    weight_spec = P('dp', 'tp')
    down_spec = P('tp', 'dp')
    return jax.shard_map(device_pass, mesh=mesh,
                         in_specs=(row_spec, weight_spec, weight_spec, down_spec, row_spec),
                         out_specs=(row_spec, row_spec, weight_spec, weight_spec, down_spec),
                         check_vma=False)
```

```python
import jax
import jax.numpy as jnp
from jax import lax
from jax.experimental import pallas as pl
from jax.experimental.pallas import tpu as pltpu
from jax.sharding import PartitionSpec as P

MESH = pl.DeviceIdType.MESH
F32 = jnp.float32
BF16 = jnp.bfloat16
SHARDS = 4
CHUNK = 512
GROUP = 2 * CHUNK
TILE = CHUNK
RING = 3
OWN, SIB, FAR, DIAG = 0, 1, 2, 3
(S_TOK, S_TOK_FWD, S_CORE_AB, S_CORE_G, S_LINK_AB, S_LINK_G, S_HID_FAR, S_HID_SIB, S_HID_FWD, S_GRAD_FAR, S_GRAD_SIB,
 S_GRAD_FWD, S_TP, S_ROW_HOME, S_ROW_AWAY, S_SWAP) = (0, 2, 4, 6, 8, 9, 10, 11, 12, 13, 14, 15, 16, 19, 20, 22)
SENDS = 23


def _dot(lhs, rhs, lhs_dim, rhs_dim):
    return lax.dot_general(lhs, rhs, (((lhs_dim,), (rhs_dim,)), ((), ())), preferred_element_type=F32)


def exchange_kernel(token_rows, gate_hbm, up_hbm, down_hbm,
                    x_t, dyc, hid, grad, y_home, half_rows,
                    xc, gate_up, down, last_t,
                    ab_keep, ab_give, ab_got, g_keep, g_give, g_got, ab_recv, g_recv,
                    y_acc, dx_away, dx_home, y_peer, dx_peer, y_sum, dx_sum, y_far, dx_far,
                    send, gate_up_sem, down_sem, tok_rs, core_rs, away_rs, link_rs,
                    hid_rs, grad_rs, grad_sib_rs, tp_rs, home_rs, away_row_rs, swap_rs):
    tp = lax.axis_index('tp')
    dp = lax.axis_index('dp')
    sib = dp + 1 - 2 * lax.rem(dp, 2)
    far = lax.rem(dp + 2, SHARDS)
    diag = lax.rem(sib + 2, SHARDS)
    peers = {SIB: sib, FAR: far, DIAG: diag}
    half, width = xc.shape[-2:]
    groups = hid.shape[0]

    def remote(src, dst, ss, rs, **device):
        return pltpu.make_async_remote_copy(src_ref=src, dst_ref=dst, send_sem=send.at[ss], recv_sem=rs,
                                            device_id=device, device_id_type=MESH)

    def cols(i):
        return pl.ds(pl.multiple_of(i * width, width), width)

    def chunk_of(g, s):
        return pl.ds(pl.multiple_of(g * GROUP, GROUP) + s * CHUNK, CHUNK)

    def load_gate_up(g, s):
        sem = gate_up_sem.at[2 * g + s]
        return (pltpu.make_async_copy(gate_hbm.at[:, chunk_of(g, s)], gate_up.at[g, s, 0], sem),
                pltpu.make_async_copy(up_hbm.at[:, chunk_of(g, s)], gate_up.at[g, s, 1], sem))

    def load_down(g):
        return pltpu.make_async_copy(down_hbm.at[pl.ds(pl.multiple_of(g * GROUP, GROUP), GROUP)], down.at[g], down_sem.at[g])

    tokens = ((token_rows.at[0], xc), (token_rows.at[1], dyc))
    dy_own = token_rows.at[1]
    barrier = pltpu.get_barrier_semaphore()
    for device in ({'dp': far}, {'dp': diag}, {'dp': sib}, {'tp': 1 - tp}, {'dp': sib, 'tp': 1 - tp}):
        pl.semaphore_signal(barrier, inc=1, device_id=device, device_id_type=MESH)
    for g in range(groups):
        for s in (0, 1):
            for copy in load_gate_up(g, s):
                copy.start()
    for g in range(groups):
        load_down(g).start()
    for own, slots in tokens:
        slots[:, OWN] = own[:, :, cols(dp)]
    pl.semaphore_wait(barrier, 5)

    def token(p, i):
        own, slots = tokens[i]
        if p == SIB:
            return remote(own.at[:, :, cols(sib)], slots.at[:, SIB], S_TOK + i, tok_rs.at[i, 0], dp=sib)
        return remote(own.at[tp, :, cols(peers[p])], slots.at[tp, p], S_TOK + i, tok_rs.at[i, 1], dp=peers[p])

    def token_fwd(i):
        part = tokens[i][1].at[tp, 2:4]
        return remote(part, part, S_TOK_FWD + i, tok_rs.at[i, 2], tp=1 - tp)

    def tokens_far(i):
        part = tokens[i][1].at[tp, 2:4]
        return remote(part, part, S_TOK + i, tok_rs.at[i, 1], dp=far)

    for i in (0, 1):
        for p in (SIB, FAR, DIAG):
            token(p, i).start()

    def core_ab(q, c, i):
        rs = core_rs.at[0, lax.rem(2 * c + i, 4)] if q == 0 else away_rs.at[0]
        return remote(ab_give.at[q, c, i], ab_got.at[q, c, i], S_CORE_AB + q, rs, dp=sib)

    def core_g(q, c):
        rs = core_rs.at[1, lax.rem(c, 4)] if q == 0 else away_rs.at[1]
        return remote(g_give.at[q, c], g_got.at[q, c], S_CORE_G + q, rs, dp=sib)

    def link_ab(c, i):
        return remote(ab_keep.at[0, c, i], ab_recv.at[c, i], S_LINK_AB, link_rs.at[0, c // 2], dp=far)

    def link_g(c):
        return remote(g_keep.at[0, c], g_recv.at[c], S_LINK_G, link_rs.at[1, c // 2], dp=far)

    def send_ab(c, i):
        core_ab(0, c, i).wait_recv()
        ab_keep[0, c, i] += ab_got[0, c, i]
        link_ab(c, i).start()

    def send_g(c):
        core_g(0, c).wait_recv()
        g_keep[0, c] += g_got[0, c]
        link_g(c).start()

    def pair_rows(slots, q):
        return slots[:, 2 * q:2 * q + 2].reshape(4 * half, slots.shape[-1])

    def split(part):
        part = part.reshape(2, 2, half, part.shape[-1])
        return part[:, 0], part[:, 1]

    def part_ab(q, g, s, i):
        c = 2 * g + s
        if q == 0 and i == 0:
            pltpu.make_async_copy(gate_up.at[g, s], gate_up.at[g, s], gate_up_sem.at[c]).wait()
        ab_keep[q, c, i], ab_give[q, c, i] = split(_dot(pair_rows(xc, q), gate_up[g, s, i], 1, 0))
        core_ab(q, c, i).start()

    def part_g(q, g, s):
        c = 2 * g + s
        if q == 0 and s == 0:
            load_down(g).wait()
        g_keep[q, c], g_give[q, c] = split(_dot(pair_rows(dyc, q), down[g, s * CHUNK:(s + 1) * CHUNK], 1, 1))
        core_g(q, c).start()

    def each(body):
        lax.fori_loop(0, groups, lambda g, carry: (body(g), carry)[1], 0)

    def behind(first, second):
        def body(g):
            first(g)

            @pl.when(g > 0)
            def _():
                second(g - 1)

        each(body)
        second(groups - 1)

    def home_parts(part, send_on, kinds):
        steps = [(s,) + kind for s in (0, 1) for kind in kinds]

        def body(g):
            for n, (s, *kind) in enumerate(steps):
                part(0, g, s, *kind)
                before_s, *before = steps[n - 1]
                if n == 0:
                    pl.when(g > 0)(lambda: send_on(2 * g - 1, *before))
                else:
                    send_on(2 * g + before_s, *before)

        each(body)
        send_on(2 * groups - 1, *kinds[-1])

    token(SIB, 0).wait_recv()
    home_parts(part_ab, send_ab, ((0,), (1,)))
    for i in (0, 1):
        tokens_far(i).wait_recv()
        token_fwd(i).start()
    token(SIB, 1).wait_recv()
    home_parts(part_g, send_g, ((),))
    token_fwd(0).wait_recv()
    each(lambda g: [part_ab(1, g, s, i) for s in (0, 1) for i in (0, 1)])
    token_fwd(1).wait_recv()
    each(lambda g: [part_g(1, g, s) for s in (0, 1)])
    x_t[...] = xc[...].reshape(2 * SHARDS * half, width).T
    for i in (0, 1):
        last_t[i] = gate_up[groups - 1, 1, i].T

    def hid_far(g):
        return remote(hid.at[g, :, FAR], hid.at[g, :, OWN], S_HID_FAR, hid_rs.at[0, g], dp=far)

    def hid_sib(g):
        return remote(hid.at[g, :, FAR], hid.at[g, :, DIAG], S_HID_SIB, hid_rs.at[1, g], dp=sib)

    def hid_fwd(g):
        return remote(hid.at[g, :, OWN], hid.at[g, :, SIB], S_HID_FWD, hid_rs.at[2, g], dp=sib)

    def grad_far(c):
        return remote(grad.at[c, :, FAR], grad.at[c, :, OWN], S_GRAD_FAR, grad_rs.at[0, c], dp=far)

    def grad_sib(c):
        return remote(grad.at[c, :, FAR], grad.at[c, :, DIAG], S_GRAD_SIB, grad_sib_rs, dp=sib)

    def grad_fwd(c):
        return remote(grad.at[c, :, OWN], grad.at[c, :, SIB], S_GRAD_FWD, grad_rs.at[1, c], dp=sib)

    y_acc[...] = jnp.zeros_like(y_acc)
    dx_away[...] = jnp.zeros_like(dx_away)
    dx_home[...] = jnp.zeros_like(dx_home)

    def add_y(q, g):
        part = _dot(hid[g, :, 2 * q:2 * q + 2].reshape(4 * half, GROUP), down[g], 1, 0)
        y_acc[q] += part.reshape(y_acc.shape[1:])

    def add_dx(acc, q, g, s, last=False):
        part = None
        for i in (0, 1):
            lhs = grad[2 * g + s, :, 2 * q:2 * q + 2, i].reshape(4 * half, CHUNK)
            term = _dot(lhs, last_t[i], 1, 0) if last else _dot(lhs, gate_up[g, s, i], 1, 1)
            part = term if part is None else part + term
        acc[...] += part.reshape(acc.shape)

    def form_hidden(g):
        both = pl.ds(2 * g, 2)
        remote(ab_recv.at[both], ab_recv.at[both], S_LINK_AB, link_rs.at[0, g], dp=far).wait_recv()
        for s in (0, 1):
            c = 2 * g + s
            total = ab_keep[1, c] + ab_got[1, c] + ab_recv[c]
            ab_keep[1, c] = total
            a, b = total[0], total[1]
            hid[g, :, FAR, :, s * CHUNK:(s + 1) * CHUNK] = (a * jax.nn.sigmoid(a) * b).astype(BF16)
        hid_far(g).start()
        hid_sib(g).start()

    def away_y(g):
        hid_sib(g).wait_recv()
        add_y(1, g)

    def form_grads(g):
        both = pl.ds(2 * g, 2)
        remote(g_recv.at[both], g_recv.at[both], S_LINK_G, link_rs.at[1, g], dp=far).wait_recv()
        for s in (0, 1):
            c = 2 * g + s
            v = g_keep[1, c] + g_got[1, c] + g_recv[c]
            a, b = ab_keep[1, c, 0], ab_keep[1, c, 1]
            sig = jax.nn.sigmoid(a)
            grad[c, :, FAR, 0] = (v * b * sig * (1.0 + a * (1.0 - sig))).astype(BF16)
            grad[c, :, FAR, 1] = (v * (a * sig)).astype(BF16)
            grad_far(c).start()
            grad_sib(c).start()

    def tp_copy(acc, peer, k):
        return remote(acc.at[1 - tp], peer, S_TP + k, tp_rs.at[k], tp=1 - tp)

    y_tp = [tp_copy(y_acc.at[q], y_peer.at[q], q) for q in (0, 1)]
    dx_tp = tp_copy(dx_away, dx_peer, 2)

    def row_home(p, r):
        device = {} if p == OWN else {'dp': sib}
        if r:
            device['tp'] = 1 - tp
        return remote(y_sum.at[p], y_home.at[p, r], S_ROW_HOME, home_rs.at[2 if p == OWN else r], **device)

    home_rows = ((OWN, 1), (SIB, 0), (SIB, 1))

    def far_row(i, p):
        total = y_sum.at[p] if i == 0 else dx_sum.at[p - 2]
        return remote(total, (y_far, dx_far)[i].at[p - 2], S_ROW_AWAY + i, away_row_rs.at[i], dp=peers[p])

    def far_rows(i):
        rows_in = (y_far, dx_far)[i]
        return remote(rows_in, rows_in, S_ROW_AWAY + i, away_row_rs.at[i], dp=far)

    def finish_y(q):
        y_tp[q].wait()
        y_sum[2 * q:2 * q + 2] = (xc[tp, 2 * q:2 * q + 2].astype(F32) + (y_acc[q, tp] + y_peer[q])).astype(BF16)
        if q == 0:
            y_home[OWN, 0] = y_sum[OWN]
            for p, r in home_rows:
                row_home(p, r).start()

    def swap():
        return remote(dx_home.at[:, 1], half_rows.at[2:4], S_SWAP, swap_rs, dp=sib)

    remote(ab_give.at[1], ab_got.at[1], S_CORE_AB + 1, away_rs.at[0], dp=sib).wait()
    behind(form_hidden, away_y)
    y_tp[1].start()
    remote(g_give.at[1], g_got.at[1], S_CORE_G + 1, away_rs.at[1], dp=sib).wait()
    each(form_grads)
    finish_y(1)

    def take_hidden(g):
        hid_far(g).wait_recv()
        hid_fwd(g).start()

    def home_y(g):
        hid_fwd(g).wait_recv()
        add_y(0, g)
        for s in (0, 1):
            add_dx(dx_away, 1, g, s)

    remote(grad.at[:, :, FAR], grad.at[:, :, DIAG], S_GRAD_SIB, grad_sib_rs, dp=sib).wait()
    behind(take_hidden, home_y)
    y_tp[0].start()
    dx_tp.start()

    def take_grad(c):
        grad_far(c).wait_recv()
        grad_fwd(c).start()

    def home_dx(g, s, last=False):
        grad_fwd(2 * g + s).wait_recv()
        add_dx(dx_home, 0, g, s, last)

    def take_grads(g):
        take_grad(2 * g)

        @pl.when(g > 0)
        def _():
            home_dx(g - 1, 1)

        take_grad(2 * g + 1)
        home_dx(g, 0)

        @pl.when(g == 2)
        def _():
            dx_tp.wait()
            dx_sum[...] = (dyc[tp, 2:4].astype(F32) + (dx_away[tp] + dx_peer[...])).astype(BF16)
            for i in (0, 1):
                for p in (FAR, DIAG):
                    far_row(i, p).start()
            finish_y(0)

    each(take_grads)
    home_dx(groups - 1, 1, last=True)
    swap().start()
    half_rows[0:2] = dx_home[:, 0]
    for p, r in home_rows:
        row_home(p, r).wait_recv()

    for i in (0, 1):
        slots = tokens[i][1]
        remote(slots.at[:, 0:2], slots.at[:, 0:2], S_TOK + i, tok_rs.at[i, 0], dp=sib).wait_send()
        token_fwd(i).wait_send()
    remote(ab_give.at[0], ab_got.at[0], S_CORE_AB, core_rs.at[0, 0], dp=sib).wait_send()
    remote(g_give.at[0], g_got.at[0], S_CORE_G, core_rs.at[0, 0], dp=sib).wait_send()
    remote(ab_keep.at[0], ab_recv, S_LINK_AB, link_rs.at[0, 0], dp=far).wait_send()
    remote(g_keep.at[0], g_recv, S_LINK_G, link_rs.at[0, 0], dp=far).wait_send()
    for kind in (S_HID_FAR, S_HID_SIB, S_HID_FWD):
        remote(hid.at[:, :, OWN], hid.at[:, :, SIB], kind, hid_rs.at[0, 0], dp=sib).wait_send()
    for kind in (S_GRAD_FAR, S_GRAD_FWD):
        remote(grad.at[:, :, OWN], grad.at[:, :, SIB], kind, grad_sib_rs, dp=sib).wait_send()
    remote(y_sum.at[0:3], y_sum.at[0:3], S_ROW_HOME, home_rs.at[0], dp=sib).wait_send()

    for i, rows_in in enumerate((y_far, dx_far)):
        far_rows(i).wait()
        half_rows[4 + 2 * i:6 + 2 * i] = rows_in[...].astype(F32)
    swap().wait()


def gradient_kernel(x_t, dyc, hid, grad, dgate_out, dup_out, ddown_out, dgate, dup, ddown, tile_sem):
    groups = hid.shape[0]
    tokens = x_t.shape[1]
    width = dyc.shape[-1]
    per_group = GROUP // TILE

    def write(n, slot, k):
        at = pl.ds(pl.multiple_of(n * TILE, TILE), TILE)
        out = ddown_out.at[at] if k == 2 else (dgate_out, dup_out)[k].at[:, at]
        return pltpu.make_async_copy((dgate, dup, ddown)[k].at[slot], out, tile_sem.at[k, slot])

    def body(g, carry):
        for s in range(per_group):
            n = g * per_group + s
            slot = lax.rem(n, RING)

            def take(k):
                @pl.when(n >= RING)
                def _():
                    write(n - RING, slot, k).wait()

            at = slice(s * TILE, (s + 1) * TILE)
            for k, buf in enumerate((dgate, dup)):
                take(k)
                buf[slot] = _dot(x_t[...], grad[n, :, :, k].reshape(tokens, TILE), 1, 0)
                write(n, slot, k).start()
            take(2)
            ddown[slot] = _dot(hid[g, :, :, :, at].reshape(tokens, TILE), dyc[...].reshape(tokens, width), 0, 0)
            write(n, slot, 2).start()
        return carry

    lax.fori_loop(0, groups, body, 0)
    for n in range(groups * per_group - RING, groups * per_group):
        for k in range(3):
            write(n, n % RING, k).wait()


def place_kernel(token_rows, y_home, mine, theirs, y_out, dx_out):
    tp = lax.axis_index('tp')
    dp = lax.axis_index('dp')
    sib = dp + 1 - 2 * lax.rem(dp, 2)
    width = mine.shape[-1]

    def cols(i):
        return pl.ds(pl.multiple_of(i * width, width), width)

    for p, owner in ((OWN, dp), (SIB, sib)):
        y_out[tp, :, cols(owner)] = y_home[p, 0]
        y_out[1 - tp, :, cols(owner)] = y_home[p, 1]
        at = pl.ds(2 * p, 2)
        dx_out[:, :, cols(owner)] = (token_rows[1, :, :, cols(owner)].astype(F32) + (mine[at] + theirs[at])).astype(BF16)
    for p, owner in ((FAR, lax.rem(dp + 2, SHARDS)), (DIAG, lax.rem(sib + 2, SHARDS))):
        for out, at in ((y_out, p + 2), (dx_out, p + 4)):
            out[tp, :, cols(owner)] = mine[at].astype(BF16)
            out[1 - tp, :, cols(owner)] = theirs[at].astype(BF16)


def solution(mesh):
    def device_pass(x_rows, gate_blk, up_blk, down_blk, dy_rows):
        rows, model = x_rows.shape
        width, hidden = gate_blk.shape
        chunks, groups = hidden // CHUNK, hidden // GROUP
        half = rows // 2
        tokens = SHARDS * rows
        hbm = pl.BlockSpec(memory_space=pl.ANY)
        vmem = pl.BlockSpec(memory_space=pltpu.VMEM)
        sds = jax.ShapeDtypeStruct
        dma = pltpu.SemaphoreType.DMA
        tok = (2, SHARDS, half, width)
        block = (2, half, width)
        own = (2, half, model)
        token_rows = jnp.concatenate([x_rows, dy_rows]).reshape((2,) + own)
        x_t, dyc, hid, grad, y_home, half_rows = pl.pallas_call(
            exchange_kernel,
            name='exchange',
            out_shape=(sds((width, tokens), BF16), sds(tok, BF16), sds((groups, 2, SHARDS, half, GROUP), BF16),
                       sds((chunks, 2, SHARDS, 2, half, CHUNK), BF16), sds((2,) + block, BF16),
                       sds((8, half, width), F32)),
            in_specs=[vmem, hbm, hbm, hbm],
            out_specs=[vmem] * 6,
            scratch_shapes=[
                pltpu.VMEM(tok, BF16),
                pltpu.VMEM((groups, 2, 2, width, CHUNK), BF16), pltpu.VMEM((groups, GROUP, width), BF16),
                pltpu.VMEM((2, CHUNK, width), BF16),
                pltpu.VMEM((2, chunks, 2, 2, half, CHUNK), F32), pltpu.VMEM((2, chunks, 2, 2, half, CHUNK), F32),
                pltpu.VMEM((2, chunks, 2, 2, half, CHUNK), F32),
                pltpu.VMEM((2, chunks, 2, half, CHUNK), F32), pltpu.VMEM((2, chunks, 2, half, CHUNK), F32),
                pltpu.VMEM((2, chunks, 2, half, CHUNK), F32),
                pltpu.VMEM((chunks, 2, 2, half, CHUNK), F32), pltpu.VMEM((chunks, 2, half, CHUNK), F32),
                pltpu.VMEM((2, 2) + block, F32), pltpu.VMEM((2,) + block, F32), pltpu.VMEM((2,) + block, F32),
                pltpu.VMEM((2,) + block, F32), pltpu.VMEM(block, F32),
                pltpu.VMEM((SHARDS, half, width), BF16), pltpu.VMEM(block, BF16),
                pltpu.VMEM(block, BF16), pltpu.VMEM(block, BF16),
                dma((SENDS,)), dma((chunks,)), dma((groups,)), dma((2, 3)), dma((2, 4)), dma((2,)),
                dma((2, groups)), dma((3, groups)), dma((2, chunks)), dma(()), dma((3,)), dma((3,)), dma((2,)), dma(()),
            ],
            compiler_params=pltpu.CompilerParams(collective_id=0, has_side_effects=True,
                                                 vmem_limit_bytes=44 * 1024 * 1024),
        )(token_rows, gate_blk, up_blk, down_blk)
        other_rows = lax.ppermute(half_rows, 'tp', [(0, 1), (1, 0)])

        dw_gate, dw_up, dw_down = pl.pallas_call(
            gradient_kernel,
            name='gradients',
            out_shape=(sds((width, hidden), F32), sds((width, hidden), F32), sds((hidden, width), F32)),
            in_specs=[vmem] * 4,
            out_specs=[hbm] * 3,
            scratch_shapes=[pltpu.VMEM((RING, width, TILE), F32), pltpu.VMEM((RING, width, TILE), F32),
                            pltpu.VMEM((RING, TILE, width), F32), dma((3, RING))],
            cost_estimate=pl.CostEstimate(flops=6 * tokens * width * hidden, bytes_accessed=12 * width * hidden,
                                          transcendentals=0),
            compiler_params=pltpu.CompilerParams(vmem_limit_bytes=44 * 1024 * 1024),
        )(x_t, dyc, hid, grad)
        y_new, dx_new = pl.pallas_call(
            place_kernel,
            name='place_rows',
            out_shape=(sds(own, BF16), sds(own, BF16)),
            in_specs=[vmem] * 4,
            out_specs=[vmem] * 2,
            compiler_params=pltpu.CompilerParams(vmem_limit_bytes=4 * 1024 * 1024),
        )(token_rows, y_home, half_rows, other_rows)
        return y_new.reshape(rows, model), dx_new.reshape(rows, model), dw_gate, dw_up, dw_down

    row_spec = P('dp', None)
    weight_spec = P('dp', 'tp')
    down_spec = P('tp', 'dp')
    return jax.shard_map(device_pass, mesh=mesh,
                         in_specs=(row_spec, weight_spec, weight_spec, down_spec, row_spec),
                         out_specs=(row_spec, row_spec, weight_spec, weight_spec, down_spec),
                         check_vma=False)
```

```python
import jax
import jax.numpy as jnp
from jax import lax
from jax.experimental import pallas as pl
from jax.experimental.pallas import tpu as pltpu
from jax.sharding import PartitionSpec as P

MESH = pl.DeviceIdType.MESH
F32 = jnp.float32
BF16 = jnp.bfloat16
SHARDS = 4
CHUNK = 512
GROUP = 2 * CHUNK
TILE = CHUNK
RING = 3
OWN, SIB, FAR, DIAG = 0, 1, 2, 3
(S_TOK, S_TOK_FWD, S_CORE_AB, S_CORE_G, S_LINK_AB, S_LINK_G, S_HID_FAR, S_HID_SIB, S_HID_FWD, S_GRAD_FAR, S_GRAD_SIB,
 S_GRAD_FWD, S_TP, S_ROW_HOME, S_ROW_AWAY, S_SWAP) = (0, 2, 4, 6, 8, 9, 10, 11, 12, 13, 14, 15, 16, 19, 20, 22)
SEND_SLOT = (0, 0, 0, 0, 0, 1, 0, 2, 0, 0, 0, 0, 0, 0, 3, 0, 4, 5, 6, 0, 7, 8, 9)
SENDS = 10


def _dot(lhs, rhs, lhs_dim, rhs_dim):
    return lax.dot_general(lhs, rhs, (((lhs_dim,), (rhs_dim,)), ((), ())), preferred_element_type=F32)


def exchange_kernel(token_rows, gate_hbm, up_hbm, down_hbm,
                    x_t, dyc, hid, grad, y_home, half_rows,
                    xc, gate_up, down, last_t,
                    ab_keep, ab_give, ab_got, g_keep, g_give, g_got, ab_recv, g_recv,
                    y_acc, dx_away, dx_home, y_peer, dx_peer, y_sum, dx_sum, y_far, dx_far,
                    send, gate_up_sem, down_sem, tok_rs, core_rs, away_rs, link_rs,
                    hid_rs, grad_rs, grad_sib_rs, tp_rs, home_rs, away_row_rs, swap_rs):
    tp = lax.axis_index('tp')
    dp = lax.axis_index('dp')
    sib = dp + 1 - 2 * lax.rem(dp, 2)
    far = lax.rem(dp + 2, SHARDS)
    diag = lax.rem(sib + 2, SHARDS)
    peers = {SIB: sib, FAR: far, DIAG: diag}
    half, width = xc.shape[-2:]
    groups = hid.shape[0]

    def remote(src, dst, ss, rs, **device):
        return pltpu.make_async_remote_copy(src_ref=src, dst_ref=dst, send_sem=send.at[SEND_SLOT[ss]], recv_sem=rs,
                                            device_id=device, device_id_type=MESH)

    def cols(i):
        return pl.ds(pl.multiple_of(i * width, width), width)

    def chunk_of(g, s):
        return pl.ds(pl.multiple_of(g * GROUP, GROUP) + s * CHUNK, CHUNK)

    def load_gate_up(g, s):
        sem = gate_up_sem.at[2 * g + s]
        return (pltpu.make_async_copy(gate_hbm.at[:, chunk_of(g, s)], gate_up.at[g, s, 0], sem),
                pltpu.make_async_copy(up_hbm.at[:, chunk_of(g, s)], gate_up.at[g, s, 1], sem))

    def load_down(g):
        return pltpu.make_async_copy(down_hbm.at[pl.ds(pl.multiple_of(g * GROUP, GROUP), GROUP)], down.at[g], down_sem.at[g])

    tokens = ((token_rows.at[0], xc), (token_rows.at[1], dyc))
    dy_own = token_rows.at[1]
    barrier = pltpu.get_barrier_semaphore()
    for device in ({'dp': far}, {'dp': diag}, {'dp': sib}, {'tp': 1 - tp}, {'dp': sib, 'tp': 1 - tp}):
        pl.semaphore_signal(barrier, inc=1, device_id=device, device_id_type=MESH)
    for g in range(groups):
        for s in (0, 1):
            for copy in load_gate_up(g, s):
                copy.start()
    for g in range(groups):
        load_down(g).start()
    for own, slots in tokens:
        slots[:, OWN] = own[:, :, cols(dp)]
    pl.semaphore_wait(barrier, 5)

    def token(p, i):
        own, slots = tokens[i]
        if p == SIB:
            return remote(own.at[:, :, cols(sib)], slots.at[:, SIB], S_TOK + i, tok_rs.at[i, 0], dp=sib)
        return remote(own.at[tp, :, cols(peers[p])], slots.at[tp, p], S_TOK + i, tok_rs.at[i, 1], dp=peers[p])

    def token_fwd(i):
        part = tokens[i][1].at[tp, 2:4]
        return remote(part, part, S_TOK_FWD + i, tok_rs.at[i, 2], tp=1 - tp)

    def tokens_far(i):
        part = tokens[i][1].at[tp, 2:4]
        return remote(part, part, S_TOK + i, tok_rs.at[i, 1], dp=far)

    for i in (0, 1):
        for p in (SIB, FAR, DIAG):
            token(p, i).start()

    def core_ab(q, c, i):
        rs = core_rs.at[0, lax.rem(2 * c + i, 4)] if q == 0 else away_rs.at[0]
        return remote(ab_give.at[q, c, i], ab_got.at[q, c, i], S_CORE_AB + q, rs, dp=sib)

    def core_g(q, c):
        rs = core_rs.at[1, lax.rem(c, 4)] if q == 0 else away_rs.at[1]
        return remote(g_give.at[q, c], g_got.at[q, c], S_CORE_G + q, rs, dp=sib)

    def link_ab(c, i):
        return remote(ab_keep.at[0, c, i], ab_recv.at[c, i], S_LINK_AB, link_rs.at[0, c // 2], dp=far)

    def link_g(c):
        return remote(g_keep.at[0, c], g_recv.at[c], S_LINK_G, link_rs.at[1, c // 2], dp=far)

    def send_ab(c, i):
        core_ab(0, c, i).wait_recv()
        ab_keep[0, c, i] += ab_got[0, c, i]
        link_ab(c, i).start()

    def send_g(c):
        core_g(0, c).wait_recv()
        g_keep[0, c] += g_got[0, c]
        link_g(c).start()

    def pair_rows(slots, q):
        return slots[:, 2 * q:2 * q + 2].reshape(4 * half, slots.shape[-1])

    def split(part):
        part = part.reshape(2, 2, half, part.shape[-1])
        return part[:, 0], part[:, 1]

    def part_ab(q, g, s, i):
        c = 2 * g + s
        if q == 0 and i == 0:
            pltpu.make_async_copy(gate_up.at[g, s], gate_up.at[g, s], gate_up_sem.at[c]).wait()
        ab_keep[q, c, i], ab_give[q, c, i] = split(_dot(pair_rows(xc, q), gate_up[g, s, i], 1, 0))
        core_ab(q, c, i).start()

    def part_g(q, g, s):
        c = 2 * g + s
        if q == 0 and s == 0:
            load_down(g).wait()
        g_keep[q, c], g_give[q, c] = split(_dot(pair_rows(dyc, q), down[g, s * CHUNK:(s + 1) * CHUNK], 1, 1))
        core_g(q, c).start()

    def each(body):
        lax.fori_loop(0, groups, lambda g, carry: (body(g), carry)[1], 0)

    def behind(first, second):
        def body(g):
            first(g)

            @pl.when(g > 0)
            def _():
                second(g - 1)

        each(body)
        second(groups - 1)

    def home_parts(part, send_on, kinds):
        steps = [(s,) + kind for s in (0, 1) for kind in kinds]

        def body(g):
            for n, (s, *kind) in enumerate(steps):
                part(0, g, s, *kind)
                before_s, *before = steps[n - 1]
                if n == 0:
                    pl.when(g > 0)(lambda: send_on(2 * g - 1, *before))
                else:
                    send_on(2 * g + before_s, *before)

        each(body)
        send_on(2 * groups - 1, *kinds[-1])

    token(SIB, 0).wait_recv()
    home_parts(part_ab, send_ab, ((0,), (1,)))
    for i in (0, 1):
        tokens_far(i).wait_recv()
        token_fwd(i).start()
    token(SIB, 1).wait_recv()
    home_parts(part_g, send_g, ((),))
    token_fwd(0).wait_recv()
    each(lambda g: [part_ab(1, g, s, i) for s in (0, 1) for i in (0, 1)])
    token_fwd(1).wait_recv()
    each(lambda g: [part_g(1, g, s) for s in (0, 1)])
    x_t[...] = xc[...].reshape(2 * SHARDS * half, width).T
    for i in (0, 1):
        last_t[i] = gate_up[groups - 1, 1, i].T

    def hid_far(g):
        return remote(hid.at[g, :, FAR], hid.at[g, :, OWN], S_HID_FAR, hid_rs.at[0, g], dp=far)

    def hid_sib(g):
        return remote(hid.at[g, :, FAR], hid.at[g, :, DIAG], S_HID_SIB, hid_rs.at[1, g], dp=sib)

    def hid_fwd(g):
        return remote(hid.at[g, :, OWN], hid.at[g, :, SIB], S_HID_FWD, hid_rs.at[2, g], dp=sib)

    def grad_far(c):
        return remote(grad.at[c, :, FAR], grad.at[c, :, OWN], S_GRAD_FAR, grad_rs.at[0, c], dp=far)

    def grad_sib(c):
        return remote(grad.at[c, :, FAR], grad.at[c, :, DIAG], S_GRAD_SIB, grad_sib_rs, dp=sib)

    def grad_fwd(c):
        return remote(grad.at[c, :, OWN], grad.at[c, :, SIB], S_GRAD_FWD, grad_rs.at[1, c], dp=sib)

    y_acc[...] = jnp.zeros_like(y_acc)
    dx_away[...] = jnp.zeros_like(dx_away)
    dx_home[...] = jnp.zeros_like(dx_home)

    def add_y(q, g):
        part = _dot(hid[g, :, 2 * q:2 * q + 2].reshape(4 * half, GROUP), down[g], 1, 0)
        y_acc[q] += part.reshape(y_acc.shape[1:])

    def add_dx(acc, q, g, s, last=False):
        part = None
        for i in (0, 1):
            lhs = grad[2 * g + s, :, 2 * q:2 * q + 2, i].reshape(4 * half, CHUNK)
            term = _dot(lhs, last_t[i], 1, 0) if last else _dot(lhs, gate_up[g, s, i], 1, 1)
            part = term if part is None else part + term
        acc[...] += part.reshape(acc.shape)

    def form_hidden(g):
        both = pl.ds(2 * g, 2)
        remote(ab_recv.at[both], ab_recv.at[both], S_LINK_AB, link_rs.at[0, g], dp=far).wait_recv()
        for s in (0, 1):
            c = 2 * g + s
            total = ab_keep[1, c] + ab_got[1, c] + ab_recv[c]
            ab_keep[1, c] = total
            a, b = total[0], total[1]
            hid[g, :, FAR, :, s * CHUNK:(s + 1) * CHUNK] = (a * jax.nn.sigmoid(a) * b).astype(BF16)
        hid_far(g).start()
        hid_sib(g).start()

    def away_y(g):
        hid_sib(g).wait_recv()
        add_y(1, g)

    def form_grads(g):
        both = pl.ds(2 * g, 2)
        remote(g_recv.at[both], g_recv.at[both], S_LINK_G, link_rs.at[1, g], dp=far).wait_recv()
        for s in (0, 1):
            c = 2 * g + s
            v = g_keep[1, c] + g_got[1, c] + g_recv[c]
            a, b = ab_keep[1, c, 0], ab_keep[1, c, 1]
            sig = jax.nn.sigmoid(a)
            grad[c, :, FAR, 0] = (v * b * sig * (1.0 + a * (1.0 - sig))).astype(BF16)
            grad[c, :, FAR, 1] = (v * (a * sig)).astype(BF16)
            grad_far(c).start()
            grad_sib(c).start()

    def tp_copy(acc, peer, k):
        return remote(acc.at[1 - tp], peer, S_TP + k, tp_rs.at[k], tp=1 - tp)

    y_tp = [tp_copy(y_acc.at[q], y_peer.at[q], q) for q in (0, 1)]
    dx_tp = tp_copy(dx_away, dx_peer, 2)

    def row_home(p, r):
        device = {} if p == OWN else {'dp': sib}
        if r:
            device['tp'] = 1 - tp
        return remote(y_sum.at[p], y_home.at[p, r], S_ROW_HOME, home_rs.at[2 if p == OWN else r], **device)

    home_rows = ((OWN, 1), (SIB, 0), (SIB, 1))

    def far_row(i, p):
        total = y_sum.at[p] if i == 0 else dx_sum.at[p - 2]
        return remote(total, (y_far, dx_far)[i].at[p - 2], S_ROW_AWAY + i, away_row_rs.at[i], dp=peers[p])

    def far_rows(i):
        rows_in = (y_far, dx_far)[i]
        return remote(rows_in, rows_in, S_ROW_AWAY + i, away_row_rs.at[i], dp=far)

    def finish_y(q):
        y_tp[q].wait()
        y_sum[2 * q:2 * q + 2] = (xc[tp, 2 * q:2 * q + 2].astype(F32) + (y_acc[q, tp] + y_peer[q])).astype(BF16)
        if q == 0:
            y_home[OWN, 0] = y_sum[OWN]
            for p, r in home_rows:
                row_home(p, r).start()

    def swap():
        return remote(dx_home.at[:, 1], half_rows.at[2:4], S_SWAP, swap_rs, dp=sib)

    remote(ab_give.at[1], ab_got.at[1], S_CORE_AB + 1, away_rs.at[0], dp=sib).wait()
    behind(form_hidden, away_y)
    y_tp[1].start()
    remote(g_give.at[1], g_got.at[1], S_CORE_G + 1, away_rs.at[1], dp=sib).wait()
    each(form_grads)
    finish_y(1)

    def take_hidden(g):
        hid_far(g).wait_recv()
        hid_fwd(g).start()

    def home_y(g):
        hid_fwd(g).wait_recv()
        add_y(0, g)
        for s in (0, 1):
            add_dx(dx_away, 1, g, s)

    remote(grad.at[:, :, FAR], grad.at[:, :, DIAG], S_GRAD_SIB, grad_sib_rs, dp=sib).wait()
    behind(take_hidden, home_y)
    y_tp[0].start()
    dx_tp.start()

    def take_grad(c):
        grad_far(c).wait_recv()
        grad_fwd(c).start()

    def home_dx(g, s, last=False):
        grad_fwd(2 * g + s).wait_recv()
        add_dx(dx_home, 0, g, s, last)

    def take_grads(g):
        take_grad(2 * g)

        @pl.when(g > 0)
        def _():
            home_dx(g - 1, 1)

        take_grad(2 * g + 1)
        home_dx(g, 0)

        @pl.when(g == 2)
        def _():
            dx_tp.wait()
            dx_sum[...] = (dyc[tp, 2:4].astype(F32) + (dx_away[tp] + dx_peer[...])).astype(BF16)
            for i in (0, 1):
                for p in (FAR, DIAG):
                    far_row(i, p).start()
            finish_y(0)

    each(take_grads)
    home_dx(groups - 1, 1, last=True)
    swap().start()
    half_rows[0:2] = dx_home[:, 0]
    for p, r in home_rows:
        row_home(p, r).wait_recv()

    for i in (0, 1):
        slots = tokens[i][1]
        remote(slots.at[:, 0:2], slots.at[:, 0:2], S_TOK + i, tok_rs.at[i, 0], dp=sib).wait_send()
        token_fwd(i).wait_send()
    remote(ab_give.at[0], ab_got.at[0], S_CORE_AB, core_rs.at[0, 0], dp=sib).wait_send()
    remote(g_give.at[0], g_got.at[0], S_CORE_G, core_rs.at[0, 0], dp=sib).wait_send()
    remote(ab_keep.at[0], ab_recv, S_LINK_AB, link_rs.at[0, 0], dp=far).wait_send()
    remote(g_keep.at[0], g_recv, S_LINK_G, link_rs.at[0, 0], dp=far).wait_send()
    for kind in (S_HID_FAR, S_HID_SIB, S_HID_FWD):
        remote(hid.at[:, :, OWN], hid.at[:, :, SIB], kind, hid_rs.at[0, 0], dp=sib).wait_send()
    for kind in (S_GRAD_FAR, S_GRAD_FWD):
        remote(grad.at[:, :, OWN], grad.at[:, :, SIB], kind, grad_sib_rs, dp=sib).wait_send()
    remote(y_sum.at[0:3], y_sum.at[0:3], S_ROW_HOME, home_rs.at[0], dp=sib).wait_send()

    for i, rows_in in enumerate((y_far, dx_far)):
        far_rows(i).wait()
        half_rows[4 + 2 * i:6 + 2 * i] = rows_in[...].astype(F32)
    swap().wait()


def gradient_kernel(x_t, dyc, hid, grad, dgate_out, dup_out, ddown_out, dgate, dup, ddown, tile_sem):
    groups = hid.shape[0]
    tokens = x_t.shape[1]
    width = dyc.shape[-1]
    per_group = GROUP // TILE

    def write(n, slot, k):
        at = pl.ds(pl.multiple_of(n * TILE, TILE), TILE)
        out = ddown_out.at[at] if k == 2 else (dgate_out, dup_out)[k].at[:, at]
        return pltpu.make_async_copy((dgate, dup, ddown)[k].at[slot], out, tile_sem.at[k, slot])

    def body(g, carry):
        for s in range(per_group):
            n = g * per_group + s
            slot = lax.rem(n, RING)

            def take(k):
                @pl.when(n >= RING)
                def _():
                    write(n - RING, slot, k).wait()

            at = slice(s * TILE, (s + 1) * TILE)
            for k, buf in enumerate((dgate, dup)):
                take(k)
                buf[slot] = _dot(x_t[...], grad[n, :, :, k].reshape(tokens, TILE), 1, 0)
                write(n, slot, k).start()
            take(2)
            ddown[slot] = _dot(hid[g, :, :, :, at].reshape(tokens, TILE), dyc[...].reshape(tokens, width), 0, 0)
            write(n, slot, 2).start()
        return carry

    lax.fori_loop(0, groups, body, 0)
    for n in range(groups * per_group - RING, groups * per_group):
        for k in range(3):
            write(n, n % RING, k).wait()


def place_kernel(token_rows, y_home, mine, theirs, y_out, dx_out):
    tp = lax.axis_index('tp')
    dp = lax.axis_index('dp')
    sib = dp + 1 - 2 * lax.rem(dp, 2)
    width = mine.shape[-1]

    def cols(i):
        return pl.ds(pl.multiple_of(i * width, width), width)

    for p, owner in ((OWN, dp), (SIB, sib)):
        y_out[tp, :, cols(owner)] = y_home[p, 0]
        y_out[1 - tp, :, cols(owner)] = y_home[p, 1]
        at = pl.ds(2 * p, 2)
        dx_out[:, :, cols(owner)] = (token_rows[1, :, :, cols(owner)].astype(F32) + (mine[at] + theirs[at])).astype(BF16)
    for p, owner in ((FAR, lax.rem(dp + 2, SHARDS)), (DIAG, lax.rem(sib + 2, SHARDS))):
        for out, at in ((y_out, p + 2), (dx_out, p + 4)):
            out[tp, :, cols(owner)] = mine[at].astype(BF16)
            out[1 - tp, :, cols(owner)] = theirs[at].astype(BF16)


def solution(mesh):
    def device_pass(x_rows, gate_blk, up_blk, down_blk, dy_rows):
        rows, model = x_rows.shape
        width, hidden = gate_blk.shape
        chunks, groups = hidden // CHUNK, hidden // GROUP
        half = rows // 2
        tokens = SHARDS * rows
        hbm = pl.BlockSpec(memory_space=pl.ANY)
        vmem = pl.BlockSpec(memory_space=pltpu.VMEM)
        sds = jax.ShapeDtypeStruct
        dma = pltpu.SemaphoreType.DMA
        tok = (2, SHARDS, half, width)
        block = (2, half, width)
        own = (2, half, model)
        token_rows = jnp.concatenate([x_rows, dy_rows]).reshape((2,) + own)
        x_t, dyc, hid, grad, y_home, half_rows = pl.pallas_call(
            exchange_kernel,
            name='exchange',
            out_shape=(sds((width, tokens), BF16), sds(tok, BF16), sds((groups, 2, SHARDS, half, GROUP), BF16),
                       sds((chunks, 2, SHARDS, 2, half, CHUNK), BF16), sds((2,) + block, BF16),
                       sds((8, half, width), F32)),
            in_specs=[vmem, hbm, hbm, hbm],
            out_specs=[vmem] * 6,
            scratch_shapes=[
                pltpu.VMEM(tok, BF16),
                pltpu.VMEM((groups, 2, 2, width, CHUNK), BF16), pltpu.VMEM((groups, GROUP, width), BF16),
                pltpu.VMEM((2, CHUNK, width), BF16),
                pltpu.VMEM((2, chunks, 2, 2, half, CHUNK), F32), pltpu.VMEM((2, chunks, 2, 2, half, CHUNK), F32),
                pltpu.VMEM((2, chunks, 2, 2, half, CHUNK), F32),
                pltpu.VMEM((2, chunks, 2, half, CHUNK), F32), pltpu.VMEM((2, chunks, 2, half, CHUNK), F32),
                pltpu.VMEM((2, chunks, 2, half, CHUNK), F32),
                pltpu.VMEM((chunks, 2, 2, half, CHUNK), F32), pltpu.VMEM((chunks, 2, half, CHUNK), F32),
                pltpu.VMEM((2, 2) + block, F32), pltpu.VMEM((2,) + block, F32), pltpu.VMEM((2,) + block, F32),
                pltpu.VMEM((2,) + block, F32), pltpu.VMEM(block, F32),
                pltpu.VMEM((SHARDS, half, width), BF16), pltpu.VMEM(block, BF16),
                pltpu.VMEM(block, BF16), pltpu.VMEM(block, BF16),
                dma((SENDS,)), dma((chunks,)), dma((groups,)), dma((2, 3)), dma((2, 4)), dma((2,)),
                dma((2, groups)), dma((3, groups)), dma((2, chunks)), dma(()), dma((3,)), dma((3,)), dma((2,)), dma(()),
            ],
            compiler_params=pltpu.CompilerParams(collective_id=0, has_side_effects=True,
                                                 vmem_limit_bytes=44 * 1024 * 1024),
        )(token_rows, gate_blk, up_blk, down_blk)
        other_rows = lax.ppermute(half_rows, 'tp', [(0, 1), (1, 0)])

        dw_gate, dw_up, dw_down = pl.pallas_call(
            gradient_kernel,
            name='gradients',
            out_shape=(sds((width, hidden), F32), sds((width, hidden), F32), sds((hidden, width), F32)),
            in_specs=[vmem] * 4,
            out_specs=[hbm] * 3,
            scratch_shapes=[pltpu.VMEM((RING, width, TILE), F32), pltpu.VMEM((RING, width, TILE), F32),
                            pltpu.VMEM((RING, TILE, width), F32), dma((3, RING))],
            cost_estimate=pl.CostEstimate(flops=6 * tokens * width * hidden, bytes_accessed=12 * width * hidden,
                                          transcendentals=0),
            compiler_params=pltpu.CompilerParams(vmem_limit_bytes=44 * 1024 * 1024),
        )(x_t, dyc, hid, grad)
        y_new, dx_new = pl.pallas_call(
            place_kernel,
            name='place_rows',
            out_shape=(sds(own, BF16), sds(own, BF16)),
            in_specs=[vmem] * 4,
            out_specs=[vmem] * 2,
            compiler_params=pltpu.CompilerParams(vmem_limit_bytes=4 * 1024 * 1024),
        )(token_rows, y_home, half_rows, other_rows)
        return y_new.reshape(rows, model), dx_new.reshape(rows, model), dw_gate, dw_up, dw_down

    row_spec = P('dp', None)
    weight_spec = P('dp', 'tp')
    down_spec = P('tp', 'dp')
    return jax.shard_map(device_pass, mesh=mesh,
                         in_specs=(row_spec, weight_spec, weight_spec, down_spec, row_spec),
                         out_specs=(row_spec, row_spec, weight_spec, weight_spec, down_spec),
                         check_vma=False)
```

```python
import jax
import jax.numpy as jnp
from jax import lax
from jax.experimental import pallas as pl
from jax.experimental.pallas import tpu as pltpu
from jax.sharding import PartitionSpec as P

MESH = pl.DeviceIdType.MESH
F32 = jnp.float32
BF16 = jnp.bfloat16
SHARDS = 4
CHUNK = 512
GROUP = 2 * CHUNK
TILE = CHUNK
RING = 3
OWN, SIB, FAR, DIAG = 0, 1, 2, 3
(S_TOK, S_TOK_FWD, S_CORE_AB, S_CORE_G, S_LINK_AB, S_LINK_G, S_HID_FAR, S_HID_SIB, S_HID_FWD, S_GRAD_FAR, S_GRAD_SIB,
 S_GRAD_FWD, S_TP, S_ROW_HOME, S_ROW_AWAY, S_SWAP) = (0, 2, 4, 6, 8, 9, 10, 11, 12, 13, 14, 15, 16, 19, 20, 22)
SEND_SLOT = (0, 0, 0, 0, 0, 1, 0, 2, 0, 0, 0, 0, 0, 0, 3, 0, 4, 5, 6, 0, 7, 8, 9)
SENDS = 10


def _dot(lhs, rhs, lhs_dim, rhs_dim):
    return lax.dot_general(lhs, rhs, (((lhs_dim,), (rhs_dim,)), ((), ())), preferred_element_type=F32)


def exchange_kernel(token_rows, gate_hbm, up_hbm, down_hbm,
                    x_t, dyc, hid, grad, y_home, half_rows,
                    xc, gate_up, down, last_t,
                    ab_keep, ab_give, ab_got, g_keep, g_give, g_got, ab_recv, g_recv,
                    y_acc, dx_away, dx_home, y_peer, dx_peer, y_sum, dx_sum, y_far, dx_far,
                    send, gate_up_sem, down_sem, tok_rs, core_rs, away_rs, link_rs,
                    hid_rs, grad_rs, grad_sib_rs, tp_rs, home_rs, away_row_rs, swap_rs):
    tp = lax.axis_index('tp')
    dp = lax.axis_index('dp')
    sib = dp + 1 - 2 * lax.rem(dp, 2)
    far = lax.rem(dp + 2, SHARDS)
    diag = lax.rem(sib + 2, SHARDS)
    peers = {SIB: sib, FAR: far, DIAG: diag}
    half, width = xc.shape[-2:]
    groups = hid.shape[0]

    def remote(src, dst, ss, rs, **device):
        return pltpu.make_async_remote_copy(src_ref=src, dst_ref=dst, send_sem=send.at[SEND_SLOT[ss]], recv_sem=rs,
                                            device_id=device, device_id_type=MESH)

    def cols(i):
        return pl.ds(pl.multiple_of(i * width, width), width)

    def chunk_of(g, s):
        return pl.ds(pl.multiple_of(g * GROUP, GROUP) + s * CHUNK, CHUNK)

    def load_gate_up(g, s):
        sem = gate_up_sem.at[2 * g + s]
        return (pltpu.make_async_copy(gate_hbm.at[:, chunk_of(g, s)], gate_up.at[g, s, 0], sem),
                pltpu.make_async_copy(up_hbm.at[:, chunk_of(g, s)], gate_up.at[g, s, 1], sem))

    def load_down(g):
        return pltpu.make_async_copy(down_hbm.at[pl.ds(pl.multiple_of(g * GROUP, GROUP), GROUP)], down.at[g], down_sem)

    tokens = ((token_rows.at[0], xc), (token_rows.at[1], dyc))
    dy_own = token_rows.at[1]
    barrier = pltpu.get_barrier_semaphore()
    for device in ({'dp': far}, {'dp': diag}, {'dp': sib}, {'tp': 1 - tp}, {'dp': sib, 'tp': 1 - tp}):
        pl.semaphore_signal(barrier, inc=1, device_id=device, device_id_type=MESH)
    for g in range(groups):
        for s in (0, 1):
            for copy in load_gate_up(g, s):
                copy.start()
    for g in range(groups):
        load_down(g).start()
    for own, slots in tokens:
        slots[:, OWN] = own[:, :, cols(dp)]
    pl.semaphore_wait(barrier, 5)

    def token(p, i):
        own, slots = tokens[i]
        if p == SIB:
            return remote(own.at[:, :, cols(sib)], slots.at[:, SIB], S_TOK + i, tok_rs.at[i, 0], dp=sib)
        return remote(own.at[tp, :, cols(peers[p])], slots.at[tp, p], S_TOK + i, tok_rs.at[i, 1], dp=peers[p])

    def token_fwd(i):
        part = tokens[i][1].at[tp, 2:4]
        return remote(part, part, S_TOK_FWD + i, tok_rs.at[i, 2], tp=1 - tp)

    def tokens_far(i):
        part = tokens[i][1].at[tp, 2:4]
        return remote(part, part, S_TOK + i, tok_rs.at[i, 1], dp=far)

    for i in (0, 1):
        for p in (SIB, FAR, DIAG):
            token(p, i).start()

    def core_ab(q, c, i):
        rs = core_rs.at[0, lax.rem(2 * c + i, 4)] if q == 0 else away_rs.at[0]
        return remote(ab_give.at[q, c, i], ab_got.at[q, c, i], S_CORE_AB + q, rs, dp=sib)

    def core_g(q, c):
        rs = core_rs.at[1, lax.rem(c, 4)] if q == 0 else away_rs.at[1]
        return remote(g_give.at[q, c], g_got.at[q, c], S_CORE_G + q, rs, dp=sib)

    def link_ab(c, i):
        return remote(ab_keep.at[0, c, i], ab_recv.at[c, i], S_LINK_AB, link_rs.at[0, c // 2], dp=far)

    def link_g(c):
        return remote(g_keep.at[0, c], g_recv.at[c], S_LINK_G, link_rs.at[1, c // 2], dp=far)

    def send_ab(c, i):
        core_ab(0, c, i).wait_recv()
        ab_keep[0, c, i] += ab_got[0, c, i]
        link_ab(c, i).start()

    def send_g(c):
        core_g(0, c).wait_recv()
        g_keep[0, c] += g_got[0, c]
        link_g(c).start()

    def pair_rows(slots, q):
        return slots[:, 2 * q:2 * q + 2].reshape(4 * half, slots.shape[-1])

    def split(part):
        part = part.reshape(2, 2, half, part.shape[-1])
        return part[:, 0], part[:, 1]

    def part_ab(q, g, s, i):
        c = 2 * g + s
        if q == 0 and i == 0:
            pltpu.make_async_copy(gate_up.at[g, s], gate_up.at[g, s], gate_up_sem.at[c]).wait()
        ab_keep[q, c, i], ab_give[q, c, i] = split(_dot(pair_rows(xc, q), gate_up[g, s, i], 1, 0))
        core_ab(q, c, i).start()

    def part_g(q, g, s):
        c = 2 * g + s
        g_keep[q, c], g_give[q, c] = split(_dot(pair_rows(dyc, q), down[g, s * CHUNK:(s + 1) * CHUNK], 1, 1))
        core_g(q, c).start()

    def each(body):
        lax.fori_loop(0, groups, lambda g, carry: (body(g), carry)[1], 0)

    def behind(first, second):
        def body(g):
            first(g)

            @pl.when(g > 0)
            def _():
                second(g - 1)

        each(body)
        second(groups - 1)

    def home_parts(part, send_on, kinds):
        steps = [(s,) + kind for s in (0, 1) for kind in kinds]

        def body(g):
            for n, (s, *kind) in enumerate(steps):
                part(0, g, s, *kind)
                before_s, *before = steps[n - 1]
                if n == 0:
                    pl.when(g > 0)(lambda: send_on(2 * g - 1, *before))
                else:
                    send_on(2 * g + before_s, *before)

        each(body)
        send_on(2 * groups - 1, *kinds[-1])

    token(SIB, 0).wait_recv()
    home_parts(part_ab, send_ab, ((0,), (1,)))
    for i in (0, 1):
        tokens_far(i).wait_recv()
        token_fwd(i).start()
    token(SIB, 1).wait_recv()
    pltpu.make_async_copy(down, down, down_sem).wait()
    home_parts(part_g, send_g, ((),))
    token_fwd(0).wait_recv()
    each(lambda g: [part_ab(1, g, s, i) for s in (0, 1) for i in (0, 1)])
    token_fwd(1).wait_recv()
    each(lambda g: [part_g(1, g, s) for s in (0, 1)])
    x_t[...] = xc[...].reshape(2 * SHARDS * half, width).T
    for i in (0, 1):
        last_t[i] = gate_up[groups - 1, 1, i].T

    def hid_far(g):
        return remote(hid.at[g, :, FAR], hid.at[g, :, OWN], S_HID_FAR, hid_rs.at[0, g], dp=far)

    def hid_sib(g):
        return remote(hid.at[g, :, FAR], hid.at[g, :, DIAG], S_HID_SIB, hid_rs.at[1, g], dp=sib)

    def hid_fwd(g):
        return remote(hid.at[g, :, OWN], hid.at[g, :, SIB], S_HID_FWD, hid_rs.at[2, g], dp=sib)

    def grad_far(c):
        return remote(grad.at[c, :, FAR], grad.at[c, :, OWN], S_GRAD_FAR, grad_rs.at[0, c], dp=far)

    def grad_sib(c):
        return remote(grad.at[c, :, FAR], grad.at[c, :, DIAG], S_GRAD_SIB, grad_sib_rs, dp=sib)

    def grad_fwd(c):
        return remote(grad.at[c, :, OWN], grad.at[c, :, SIB], S_GRAD_FWD, grad_rs.at[1, c], dp=sib)

    y_acc[...] = jnp.zeros_like(y_acc)
    dx_away[...] = jnp.zeros_like(dx_away)
    dx_home[...] = jnp.zeros_like(dx_home)

    def add_y(q, g):
        part = _dot(hid[g, :, 2 * q:2 * q + 2].reshape(4 * half, GROUP), down[g], 1, 0)
        y_acc[q] += part.reshape(y_acc.shape[1:])

    def add_dx(acc, q, g, s, last=False):
        part = None
        for i in (0, 1):
            lhs = grad[2 * g + s, :, 2 * q:2 * q + 2, i].reshape(4 * half, CHUNK)
            term = _dot(lhs, last_t[i], 1, 0) if last else _dot(lhs, gate_up[g, s, i], 1, 1)
            part = term if part is None else part + term
        acc[...] += part.reshape(acc.shape)

    def form_hidden(g):
        both = pl.ds(2 * g, 2)
        remote(ab_recv.at[both], ab_recv.at[both], S_LINK_AB, link_rs.at[0, g], dp=far).wait_recv()
        for s in (0, 1):
            c = 2 * g + s
            total = ab_keep[1, c] + ab_got[1, c] + ab_recv[c]
            ab_keep[1, c] = total
            a, b = total[0], total[1]
            hid[g, :, FAR, :, s * CHUNK:(s + 1) * CHUNK] = (a * jax.nn.sigmoid(a) * b).astype(BF16)
        hid_far(g).start()
        hid_sib(g).start()

    def away_y(g):
        hid_sib(g).wait_recv()
        add_y(1, g)

    def form_grads(g):
        both = pl.ds(2 * g, 2)
        remote(g_recv.at[both], g_recv.at[both], S_LINK_G, link_rs.at[1, g], dp=far).wait_recv()
        for s in (0, 1):
            c = 2 * g + s
            v = g_keep[1, c] + g_got[1, c] + g_recv[c]
            a, b = ab_keep[1, c, 0], ab_keep[1, c, 1]
            sig = jax.nn.sigmoid(a)
            grad[c, :, FAR, 0] = (v * b * sig * (1.0 + a * (1.0 - sig))).astype(BF16)
            grad[c, :, FAR, 1] = (v * (a * sig)).astype(BF16)
            grad_far(c).start()
            grad_sib(c).start()

    def tp_copy(acc, peer, k):
        return remote(acc.at[1 - tp], peer, S_TP + k, tp_rs.at[k], tp=1 - tp)

    y_tp = [tp_copy(y_acc.at[q], y_peer.at[q], q) for q in (0, 1)]
    dx_tp = tp_copy(dx_away, dx_peer, 2)

    def row_home(p, r):
        device = {} if p == OWN else {'dp': sib}
        if r:
            device['tp'] = 1 - tp
        return remote(y_sum.at[p], y_home.at[p, r], S_ROW_HOME, home_rs, **device)

    home_rows = ((OWN, 1), (SIB, 0), (SIB, 1))

    def far_row(i, p):
        total = y_sum.at[p] if i == 0 else dx_sum.at[p - 2]
        return remote(total, (y_far, dx_far)[i].at[p - 2], S_ROW_AWAY + i, away_row_rs.at[i], dp=peers[p])

    def far_rows(i):
        rows_in = (y_far, dx_far)[i]
        return remote(rows_in, rows_in, S_ROW_AWAY + i, away_row_rs.at[i], dp=far)

    def finish_y(q):
        y_tp[q].wait()
        y_sum[2 * q:2 * q + 2] = (xc[tp, 2 * q:2 * q + 2].astype(F32) + (y_acc[q, tp] + y_peer[q])).astype(BF16)
        if q == 0:
            y_home[OWN, 0] = y_sum[OWN]
            for p, r in home_rows:
                row_home(p, r).start()

    def swap():
        return remote(dx_home.at[:, 1], half_rows.at[2:4], S_SWAP, swap_rs, dp=sib)

    remote(ab_give.at[1], ab_got.at[1], S_CORE_AB + 1, away_rs.at[0], dp=sib).wait()
    behind(form_hidden, away_y)
    y_tp[1].start()
    remote(g_give.at[1], g_got.at[1], S_CORE_G + 1, away_rs.at[1], dp=sib).wait()
    each(form_grads)
    finish_y(1)

    def take_hidden(g):
        hid_far(g).wait_recv()
        hid_fwd(g).start()

    def home_y(g):
        hid_fwd(g).wait_recv()
        add_y(0, g)
        for s in (0, 1):
            add_dx(dx_away, 1, g, s)

    remote(grad.at[:, :, FAR], grad.at[:, :, DIAG], S_GRAD_SIB, grad_sib_rs, dp=sib).wait()
    behind(take_hidden, home_y)
    y_tp[0].start()
    dx_tp.start()

    def take_grad(c):
        grad_far(c).wait_recv()
        grad_fwd(c).start()

    def home_dx(g, s, last=False):
        grad_fwd(2 * g + s).wait_recv()
        add_dx(dx_home, 0, g, s, last)

    def take_grads(g):
        take_grad(2 * g)

        @pl.when(g > 0)
        def _():
            home_dx(g - 1, 1)

        take_grad(2 * g + 1)
        home_dx(g, 0)

        @pl.when(g == 2)
        def _():
            dx_tp.wait()
            dx_sum[...] = (dyc[tp, 2:4].astype(F32) + (dx_away[tp] + dx_peer[...])).astype(BF16)
            for i in (0, 1):
                for p in (FAR, DIAG):
                    far_row(i, p).start()
            finish_y(0)

    each(take_grads)
    home_dx(groups - 1, 1, last=True)
    swap().start()
    half_rows[0:2] = dx_home[:, 0]
    remote(y_sum.at[0:3], y_sum.at[0:3], S_ROW_HOME, home_rs, dp=sib).wait_recv()

    for i in (0, 1):
        slots = tokens[i][1]
        remote(slots.at[:, 0:2], slots.at[:, 0:2], S_TOK + i, tok_rs.at[i, 0], dp=sib).wait_send()
        token_fwd(i).wait_send()
    remote(ab_give.at[0], ab_got.at[0], S_CORE_AB, core_rs.at[0, 0], dp=sib).wait_send()
    remote(g_give.at[0], g_got.at[0], S_CORE_G, core_rs.at[0, 0], dp=sib).wait_send()
    remote(ab_keep.at[0], ab_recv, S_LINK_AB, link_rs.at[0, 0], dp=far).wait_send()
    remote(g_keep.at[0], g_recv, S_LINK_G, link_rs.at[0, 0], dp=far).wait_send()
    for kind in (S_HID_FAR, S_HID_SIB, S_HID_FWD):
        remote(hid.at[:, :, OWN], hid.at[:, :, SIB], kind, hid_rs.at[0, 0], dp=sib).wait_send()
    for kind in (S_GRAD_FAR, S_GRAD_FWD):
        remote(grad.at[:, :, OWN], grad.at[:, :, SIB], kind, grad_sib_rs, dp=sib).wait_send()
    remote(y_sum.at[0:3], y_sum.at[0:3], S_ROW_HOME, home_rs, dp=sib).wait_send()

    for i, rows_in in enumerate((y_far, dx_far)):
        far_rows(i).wait()
        half_rows[4 + 2 * i:6 + 2 * i] = rows_in[...].astype(F32)
    swap().wait()


def gradient_kernel(x_t, dyc, hid, grad, dgate_out, dup_out, ddown_out, dgate, dup, ddown, tile_sem):
    groups = hid.shape[0]
    tokens = x_t.shape[1]
    width = dyc.shape[-1]
    per_group = GROUP // TILE

    def write(n, slot, k):
        at = pl.ds(pl.multiple_of(n * TILE, TILE), TILE)
        out = ddown_out.at[at] if k == 2 else (dgate_out, dup_out)[k].at[:, at]
        return pltpu.make_async_copy((dgate, dup, ddown)[k].at[slot], out, tile_sem.at[k, slot])

    def body(g, carry):
        for s in range(per_group):
            n = g * per_group + s
            slot = lax.rem(n, RING)

            def take(k):
                @pl.when(n >= RING)
                def _():
                    write(n - RING, slot, k).wait()

            at = slice(s * TILE, (s + 1) * TILE)
            for k, buf in enumerate((dgate, dup)):
                take(k)
                buf[slot] = _dot(x_t[...], grad[n, :, :, k].reshape(tokens, TILE), 1, 0)
                write(n, slot, k).start()
            take(2)
            ddown[slot] = _dot(hid[g, :, :, :, at].reshape(tokens, TILE), dyc[...].reshape(tokens, width), 0, 0)
            write(n, slot, 2).start()
        return carry

    lax.fori_loop(0, groups, body, 0)
    for n in range(groups * per_group - RING, groups * per_group):
        for k in range(3):
            write(n, n % RING, k).wait()


def place_kernel(token_rows, y_home, mine, theirs, y_out, dx_out):
    tp = lax.axis_index('tp')
    dp = lax.axis_index('dp')
    sib = dp + 1 - 2 * lax.rem(dp, 2)
    width = mine.shape[-1]

    def cols(i):
        return pl.ds(pl.multiple_of(i * width, width), width)

    for p, owner in ((OWN, dp), (SIB, sib)):
        y_out[tp, :, cols(owner)] = y_home[p, 0]
        y_out[1 - tp, :, cols(owner)] = y_home[p, 1]
        at = pl.ds(2 * p, 2)
        dx_out[:, :, cols(owner)] = (token_rows[1, :, :, cols(owner)].astype(F32) + (mine[at] + theirs[at])).astype(BF16)
    for p, owner in ((FAR, lax.rem(dp + 2, SHARDS)), (DIAG, lax.rem(sib + 2, SHARDS))):
        for out, at in ((y_out, p + 2), (dx_out, p + 4)):
            out[tp, :, cols(owner)] = mine[at].astype(BF16)
            out[1 - tp, :, cols(owner)] = theirs[at].astype(BF16)


def solution(mesh):
    def device_pass(x_rows, gate_blk, up_blk, down_blk, dy_rows):
        rows, model = x_rows.shape
        width, hidden = gate_blk.shape
        chunks, groups = hidden // CHUNK, hidden // GROUP
        half = rows // 2
        tokens = SHARDS * rows
        hbm = pl.BlockSpec(memory_space=pl.ANY)
        vmem = pl.BlockSpec(memory_space=pltpu.VMEM)
        sds = jax.ShapeDtypeStruct
        dma = pltpu.SemaphoreType.DMA
        tok = (2, SHARDS, half, width)
        block = (2, half, width)
        own = (2, half, model)
        token_rows = jnp.concatenate([x_rows, dy_rows]).reshape((2,) + own)
        x_t, dyc, hid, grad, y_home, half_rows = pl.pallas_call(
            exchange_kernel,
            name='exchange',
            out_shape=(sds((width, tokens), BF16), sds(tok, BF16), sds((groups, 2, SHARDS, half, GROUP), BF16),
                       sds((chunks, 2, SHARDS, 2, half, CHUNK), BF16), sds((2,) + block, BF16),
                       sds((8, half, width), F32)),
            in_specs=[vmem, hbm, hbm, hbm],
            out_specs=[vmem] * 6,
            scratch_shapes=[
                pltpu.VMEM(tok, BF16),
                pltpu.VMEM((groups, 2, 2, width, CHUNK), BF16), pltpu.VMEM((groups, GROUP, width), BF16),
                pltpu.VMEM((2, CHUNK, width), BF16),
                pltpu.VMEM((2, chunks, 2, 2, half, CHUNK), F32), pltpu.VMEM((2, chunks, 2, 2, half, CHUNK), F32),
                pltpu.VMEM((2, chunks, 2, 2, half, CHUNK), F32),
                pltpu.VMEM((2, chunks, 2, half, CHUNK), F32), pltpu.VMEM((2, chunks, 2, half, CHUNK), F32),
                pltpu.VMEM((2, chunks, 2, half, CHUNK), F32),
                pltpu.VMEM((chunks, 2, 2, half, CHUNK), F32), pltpu.VMEM((chunks, 2, half, CHUNK), F32),
                pltpu.VMEM((2, 2) + block, F32), pltpu.VMEM((2,) + block, F32), pltpu.VMEM((2,) + block, F32),
                pltpu.VMEM((2,) + block, F32), pltpu.VMEM(block, F32),
                pltpu.VMEM((SHARDS, half, width), BF16), pltpu.VMEM(block, BF16),
                pltpu.VMEM(block, BF16), pltpu.VMEM(block, BF16),
                dma((SENDS,)), dma((chunks,)), dma(()), dma((2, 3)), dma((2, 4)), dma((2,)),
                dma((2, groups)), dma((3, groups)), dma((2, chunks)), dma(()), dma((3,)), dma(()), dma((2,)), dma(()),
            ],
            compiler_params=pltpu.CompilerParams(collective_id=0, has_side_effects=True,
                                                 vmem_limit_bytes=44 * 1024 * 1024),
        )(token_rows, gate_blk, up_blk, down_blk)
        other_rows = lax.ppermute(half_rows, 'tp', [(0, 1), (1, 0)])

        dw_gate, dw_up, dw_down = pl.pallas_call(
            gradient_kernel,
            name='gradients',
            out_shape=(sds((width, hidden), F32), sds((width, hidden), F32), sds((hidden, width), F32)),
            in_specs=[vmem] * 4,
            out_specs=[hbm] * 3,
            scratch_shapes=[pltpu.VMEM((RING, width, TILE), F32), pltpu.VMEM((RING, width, TILE), F32),
                            pltpu.VMEM((RING, TILE, width), F32), dma((3, RING))],
            cost_estimate=pl.CostEstimate(flops=6 * tokens * width * hidden, bytes_accessed=12 * width * hidden,
                                          transcendentals=0),
            compiler_params=pltpu.CompilerParams(vmem_limit_bytes=44 * 1024 * 1024),
        )(x_t, dyc, hid, grad)
        y_new, dx_new = pl.pallas_call(
            place_kernel,
            name='place_rows',
            out_shape=(sds(own, BF16), sds(own, BF16)),
            in_specs=[vmem] * 4,
            out_specs=[vmem] * 2,
            compiler_params=pltpu.CompilerParams(vmem_limit_bytes=4 * 1024 * 1024),
        )(token_rows, y_home, half_rows, other_rows)
        return y_new.reshape(rows, model), dx_new.reshape(rows, model), dw_gate, dw_up, dw_down

    row_spec = P('dp', None)
    weight_spec = P('dp', 'tp')
    down_spec = P('tp', 'dp')
    return jax.shard_map(device_pass, mesh=mesh,
                         in_specs=(row_spec, weight_spec, weight_spec, down_spec, row_spec),
                         out_specs=(row_spec, row_spec, weight_spec, weight_spec, down_spec),
                         check_vma=False)
```
